256 devices in a mesh: ta: 32 (over z, y_lo, core), gz: 4 (over x), gy: 2 (over y_hi).
Axes of the slice: x: 4, y: 4 (y_hi: 2, y_lo: 2; y = y_hi * 2 + y_lo), z: 8, core: 2. Of those that a mesh axis runs over, the one named last changes fastest.
Arguments:
- right_side: float32 [256, 32, 32, 128], P('ta', 'gz', 'gy'), may hold values from -12 to 12, as said below
- mass_field: float32 [256, 32, 32, 128], P('ta', 'gz', 'gy'), may hold values from 0.05 to 0.8
Outputs:
- solution: float32 [256, 32, 32, 128], P('ta', 'gz', 'gy')
- residual: float32 [256, 32, 32, 128], P('ta', 'gz', 'gy')
The draws below stay inside these ranges and needn't reach their ends.
Inputs may be any that keep to these rules, and one draw needn't show every extreme that they name: right_side is twice a field constant on aligned blocks of 8 x 8 x 8 x 8 sites plus site-by-site noise, each part within -4 to 4.
All inputs are finite; a program needn't handle non-finite values.
Results may differ from the reference program's by a relative error of at most 0.0003.
Values sent between devices are 32-bit elements.
A program may use at most 128 MiB of HBM per device.

```python
import math
import jax
import jax.numpy as jnp

LEVELS = 4
PRE = 2
POST = 2
COARSE_STEPS = 4
NT = 256
NZ = 32
NY = 32
NX = 128


def draw_right_side(key, part):
    coarse_key = jax.random.fold_in(key, 11)
    detail_key = jax.random.fold_in(key, 23)
    coarse_shape = (NT // 8, NZ // 8, NY // 8, NX // 8)
    whole_shape = (NT, NZ, NY, NX)
    coarse = jnp.clip(jax.random.normal(coarse_key, coarse_shape, jnp.float32), -4.0, 4.0)
    detail = jnp.clip(jax.random.normal(detail_key, whole_shape, jnp.float32), -4.0, 4.0)
    filled = coarse
    for dimension in range(4):
        filled = jnp.repeat(filled, 8, axis=dimension)
    return (2.0 * filled + detail).astype(jnp.float32)


def shard_levels(key, extent, shards, low, top_value):
    loudness = 1.0
    for position, blocks in shards:
        steps = jax.random.uniform(jax.random.fold_in(jax.random.fold_in(key, 6), position), (blocks,), jnp.float32, low / len(shards), top_value / len(shards))
        loudness = loudness * jnp.repeat(jnp.exp(steps), extent[position] // blocks).reshape((-1,) + (1,) * (len(extent) - 1 - position))
    return loudness


def setup_inputs(seed: int = 0) -> dict:
    keys = jax.random.split(jax.random.key(seed), 3)
    return {
        "right_side": draw_right_side(jax.random.fold_in(keys[2], 71), 0),
        "mass_field": jnp.clip(jnp.exp(math.log(0.8) - 2.7725887 * jax.random.uniform(keys[1], (NT, NZ, NY, NX), jnp.float32) ** shard_levels(keys[1], (NT, NZ, NY, NX), ((0, 32), (1, 4), (2, 2)), -0.2, 0.2)), 0.05, 0.8),
    }


DAMPING = 0.7


def neighbours(values):
    summed = jnp.zeros_like(values)
    for dimension in range(4):
        summed = summed + jnp.roll(values, 1, dimension) + jnp.roll(values, -1, dimension)
    return summed


def operate(values, mass_level, coarse_level):
    factor = 0.5 ** coarse_level
    return factor * (8.0 * values - neighbours(values)) + mass_level * values


def coarsen(values):
    first, second, third, fourth = values.shape
    blocks = values.reshape(first // 2, 2, second // 2, 2, third // 2, 2, fourth // 2, 2)
    return jnp.mean(blocks, axis=(1, 3, 5, 7))


def refine(values):
    for dimension in range(4):
        values = jnp.repeat(values, 2, axis=dimension)
    return values


def sweeps(values, source, mass_level, coarse_level, count_steps):
    diagonal = 8.0 * (0.5 ** coarse_level) + mass_level
    for sweep_no in range(count_steps):
        values = values + DAMPING * (source - operate(values, mass_level, coarse_level)) / diagonal
    return values


def cycle(source, mass_level, coarse_level):
    diagonal = 8.0 * (0.5 ** coarse_level) + mass_level
    values = DAMPING * source / diagonal
    if coarse_level == LEVELS - 1:
        return sweeps(values, source, mass_level, coarse_level, COARSE_STEPS - 1)
    values = sweeps(values, source, mass_level, coarse_level, PRE - 1)
    remainder = source - operate(values, mass_level, coarse_level)
    correction = cycle(coarsen(remainder), coarsen(mass_level), coarse_level + 1)
    values = values + refine(correction)
    return sweeps(values, source, mass_level, coarse_level, POST)


def reference(right_side, mass_field):
    solution = cycle(right_side, mass_field, 0)
    residual = right_side - operate(solution, mass_field, 0)
    return solution, residual
```

```python
import jax
import jax.numpy as jnp
from jax import lax
from jax.experimental import pallas as pl
from jax.experimental.pallas import tpu as pltpu
from jax.sharding import PartitionSpec as P

LEVELS = 4
POST = 2
COARSE_STEPS = 4
DAMPING = 0.7
ROUNDS = 16
OFF = 8
MESH = pl.DeviceIdType.MESH


def dims(level):
    return 8 >> level, 8 >> level, 16 >> level


def padded_shape(level):
    nt, nz, ny = dims(level)
    return (nt + 2, nz + 2, 2 * OFF + max(ny, 8), 128)


def kernel(
    s_ref, m_ref, sol_ref, res_ref,
    v0, v1, v2, v3, s_1, s_2, s_3, m_1, m_2, m_3, tmp, send_sem, recv_sem,
):
    ta, gz, gy = lax.axis_index("ta"), lax.axis_index("gz"), lax.axis_index("gy")
    nta, ngz, ngy = lax.axis_size("ta"), lax.axis_size("gz"), lax.axis_size("gy")
    t_up, t_down = lax.rem(ta + 1, nta), lax.rem(ta + nta - 1, nta)
    z_up, z_down = lax.rem(gz + 1, ngz), lax.rem(gz + ngz - 1, ngz)
    y_other = lax.rem(gy + 1, ngy)

    barrier = pltpu.get_barrier_semaphore()
    peers = ({"ta": t_up}, {"ta": t_down}, {"gz": z_up}, {"gz": z_down}, {"gy": y_other})
    for peer in peers:
        pl.semaphore_signal(barrier, inc=1, device_id=peer, device_id_type=MESH)
    pl.semaphore_wait(barrier, len(peers))

    buffers = (v0, v1, v2, v3)
    sources, masses = (s_ref, s_1, s_2, s_3), (m_ref, m_1, m_2, m_3)
    sent = []

    def exchange(level, slot):
        nt, nz, ny = dims(level)
        buf = buffers[level].at[slot]
        number = len(sent) // 6
        t_all, z_all, y_all = pl.ds(1, nt), pl.ds(1, nz), pl.ds(OFF, ny)

        def box(dim, at):
            whole = [t_all, z_all, y_all]
            whole[dim] = pl.ds(at, 1)
            return buf.at[whole[0], whole[1], whole[2], :]

        plan = (
            ({"gy": y_other}, 2, OFF + ny - 1, OFF - 1),
            ({"gy": y_other}, 2, OFF, OFF + ny),
            ({"ta": t_up}, 0, nt, 0),
            ({"ta": t_down}, 0, 1, nt + 1),
            ({"gz": z_up}, 1, nz, 0),
            ({"gz": z_down}, 1, 1, nz + 1),
        )
        copies = []
        for i, (peer, dim, at, to) in enumerate(plan):
            copies.append(
                pltpu.make_async_remote_copy(
                    src_ref=box(dim, at),
                    dst_ref=box(dim, to),
                    send_sem=send_sem.at[number, i],
                    recv_sem=recv_sem.at[number, i],
                    device_id=peer,
                    device_id_type=MESH,
                )
            )
        for copy in copies:
            copy.start()
        for copy in copies:
            copy.wait_recv()
        sent.extend(copies)

    def around(buf, t, level):
        _, nz, ny = dims(level)
        rows = pl.ds(OFF, ny)
        mid = buf[t + 1, pl.ds(1, nz), rows, :]
        total = buf[t, pl.ds(1, nz), rows, :] + buf[t + 2, pl.ds(1, nz), rows, :]
        total += buf[t + 1, pl.ds(0, nz), rows, :] + buf[t + 1, pl.ds(2, nz), rows, :]
        total += buf[t + 1, pl.ds(1, nz), pl.ds(OFF - 1, ny), :]
        total += buf[t + 1, pl.ds(1, nz), pl.ds(OFF + 1, ny), :]
        step = 1 << level
        total += pltpu.roll(mid, step, 2) + pltpu.roll(mid, 128 - step, 2)
        return mid, total

    def planes(level, body):
        nt = dims(level)[0]
        if nt == 1:
            body(0)
        else:
            lax.fori_loop(0, nt, lambda t, c: (body(t), c)[1], 0)

    def own(buf, t, level):
        _, nz, ny = dims(level)
        return buf.at[t + 1, pl.ds(1, nz), pl.ds(OFF, ny), :]

    def diag(level, t):
        return 8.0 * 0.5**level + masses[level][t]

    def first(level, slot):
        def body(t):
            own(buffers[level].at[slot], t, level)[...] = (
                DAMPING * sources[level][t] / diag(level, t)
            )

        planes(level, body)

    def sweep(level, slot, out):
        def body(t):
            mid, total = around(buffers[level].at[slot], t, level)
            d = diag(level, t)
            image = d * mid - 0.5**level * total
            own(buffers[level].at[out], t, level)[...] = (
                mid + DAMPING * (sources[level][t] - image) / d
            )

        planes(level, body)

    def residual(level, slot, t):
        mid, total = around(buffers[level].at[slot], t, level)
        return sources[level][t] - (diag(level, t) * mid - 0.5**level * total)

    def coarsen(level, get, out):
        nt, nz, ny = dims(level)
        step = 1 << level

        def body(t):
            a = get(2 * t) + get(2 * t + 1)
            a = a.reshape(nz // 2, 2, ny, 128)
            a = a[:, 0] + a[:, 1]
            tmp[0 : nz // 2, 0:ny, :] = a
            b = tmp[0 : nz // 2, pl.ds(0, ny // 2, stride=2), :]
            b += tmp[0 : nz // 2, pl.ds(1, ny // 2, stride=2), :]
            lane = lax.broadcasted_iota(jnp.int32, b.shape, 2)
            low = jnp.bitwise_and(lane, step) == 0
            b += jnp.where(low, pltpu.roll(b, 128 - step, 2), pltpu.roll(b, step, 2))
            out[t] = b * (1.0 / 16.0)

        if nt == 2:
            body(0)
        else:
            lax.fori_loop(0, nt // 2, lambda t, c: (body(t), c)[1], 0)

    def correct(level, slot, out, coarse_slot):
        nt, nz, ny = dims(level)

        def body(t):
            e = own(buffers[level + 1].at[coarse_slot], t, level + 1)[...]
            tmp[0 : nz // 2, pl.ds(0, ny // 2, stride=2), :] = e
            tmp[0 : nz // 2, pl.ds(1, ny // 2, stride=2), :] = e
            e = tmp[0 : nz // 2, 0:ny, :]
            e = jnp.broadcast_to(e[:, None], (nz // 2, 2, ny, 128)).reshape(nz, ny, 128)
            for k in range(2):
                old = own(buffers[level].at[slot], 2 * t + k, level)[...]
                own(buffers[level].at[out], 2 * t + k, level)[...] = old + e

        if nt == 2:
            body(0)
        else:
            lax.fori_loop(0, nt // 2, lambda t, c: (body(t), c)[1], 0)

    for level in range(LEVELS - 1):
        coarsen(level, lambda t, level=level: masses[level][t], masses[level + 1])

    for level in range(LEVELS - 1):
        first(level, 0)
        exchange(level, 0)
        sweep(level, 0, 1)
        exchange(level, 1)
        coarsen(level, lambda t, level=level: residual(level, 1, t), sources[level + 1])
    level = LEVELS - 1
    first(level, 0)
    for step in range(COARSE_STEPS - 1):
        exchange(level, step)
        sweep(level, step, step + 1)
    last = COARSE_STEPS - 1
    for level in reversed(range(LEVELS - 1)):
        correct(level, 1, 2, last)
        for slot in range(2, 2 + POST):
            exchange(level, slot)
            sweep(level, slot, slot + 1)
        last = 2 + POST
    exchange(0, last)

    def finish(t):
        res_ref[t] = residual(0, last, t)
        sol_ref[t] = own(buffers[0].at[last], t, 0)[...]

    planes(0, finish)
    for copy in sent:
        copy.wait_send()


def per_device(right_side, mass_field):
    f32 = jnp.float32
    block = jax.ShapeDtypeStruct(right_side.shape, f32)
    vmem = pl.BlockSpec(memory_space=pltpu.VMEM)
    slots = [5, 5, 5, COARSE_STEPS]
    scratch = [pltpu.VMEM((n,) + padded_shape(level), f32) for level, n in enumerate(slots)]
    for _ in range(2):
        for level in range(1, LEVELS):
            scratch.append(pltpu.VMEM(dims(level) + (128,), f32))
    scratch.append(pltpu.VMEM((8, 16, 128), f32))
    scratch += [pltpu.SemaphoreType.DMA((ROUNDS, 6))] * 2
    return pl.pallas_call(
        kernel,
        out_shape=(block, block),
        in_specs=[vmem, vmem],
        out_specs=(vmem, vmem),
        scratch_shapes=scratch,
        compiler_params=pltpu.CompilerParams(
            collective_id=0, has_side_effects=True, vmem_limit_bytes=48 * 1024 * 1024
        ),
    )(right_side, mass_field)


def solution(mesh):
    placed = (P("ta", "gz", "gy", None), P("ta", "gz", "gy", None))
    return jax.shard_map(
        per_device, mesh=mesh, in_specs=placed, out_specs=placed, check_vma=False
    )
```

```python
import jax
import jax.numpy as jnp
from jax import lax
from jax.experimental import pallas as pl
from jax.experimental.pallas import tpu as pltpu
from jax.sharding import PartitionSpec as P

DAMPING = 0.7
OFF = 8
COPIES = 160
MESH = pl.DeviceIdType.MESH


def lanes(like):
    return lax.broadcasted_iota(jnp.int32, like.shape, like.ndim - 1)


def rows(like):
    return lax.broadcasted_iota(jnp.int32, like.shape, like.ndim - 2)


def roll(x, shift, axis):
    return pltpu.roll(x, shift % x.shape[axis], axis)


def ring(x, shift, axis=0):
    shift %= x.shape[axis]
    return jnp.concatenate([x[-shift:], x[:-shift]], axis=axis)


def even(index, step):
    return jnp.bitwise_and(index, step) == 0


def partner(x, step, axis):
    index = lax.broadcasted_iota(jnp.int32, x.shape, axis)
    return jnp.where(even(index, step), roll(x, -step, axis), roll(x, step, axis))


def spread(x, step, axis):
    index = lax.broadcasted_iota(jnp.int32, x.shape, axis)
    low = even(index, step)
    return jnp.where(low, x, roll(x, step, axis)), jnp.where(low, roll(x, -step, axis), x)


def pack4(a, b, c, d):
    lane = lanes(a)
    return jnp.where(
        even(lane, 2), jnp.where(even(lane, 1), a, b), jnp.where(even(lane, 1), c, d)
    )


def unpack4(x):
    last = x.ndim - 1
    first, second = spread(x, 1, last)
    a, c = spread(first, 2, last)
    b, d = spread(second, 2, last)
    return a, b, c, d


def kernel(
    s_ref, m_ref, sol_ref, res_ref,
    v0, s1, m1, v1, p2, s2, m2, u2, v2, d2_own, d2_in, d3, s3, m3, v3, tmp, send_sem, recv_sem,
):
    ta, gz, gy = lax.axis_index("ta"), lax.axis_index("gz"), lax.axis_index("gy")
    nta, ngz, ngy = lax.axis_size("ta"), lax.axis_size("gz"), lax.axis_size("gy")

    def device(a, b, c):
        return (
            lax.rem(ta + (a + nta), nta),
            lax.rem(gz + (b + ngz), ngz),
            lax.rem(gy + c, ngy),
        )

    barrier = pltpu.get_barrier_semaphore()
    near = [(a, b, c) for a in (0, 1, -1) for b in range(4) for c in range(2)][1:]
    far = [(a, 0, 0) for k in range(2, 6) for a in (k, -k)]
    for offset in near + far:
        pl.semaphore_signal(barrier, inc=1, device_id=device(*offset), device_id_type=MESH)
    pl.semaphore_wait(barrier, len(near) + len(far))

    copies, started = [], []

    def send(src, dst, offset):
        i = len(started)
        copy = pltpu.make_async_remote_copy(
            src_ref=src,
            dst_ref=dst,
            send_sem=send_sem.at[i],
            recv_sem=recv_sem.at[i],
            device_id=device(*offset),
            device_id_type=MESH,
        )
        copies.append(copy)
        started.append(i)
        copy.start()
        return copy

    def arrived(some):
        for copy in some:
            copy.wait_recv()

    t_all, y_all = pl.ds(1, 8), pl.ds(OFF, 16)
    z_all = t_all

    def swap0(slot):
        buf = v0.at[slot]
        return [
            send(buf.at[t_all, z_all, pl.ds(OFF + 15, 1)], buf.at[t_all, z_all, pl.ds(OFF - 1, 1)], (0, 0, 1)),
            send(buf.at[t_all, z_all, pl.ds(OFF, 1)], buf.at[t_all, z_all, pl.ds(OFF + 16, 1)], (0, 0, 1)),
            send(buf.at[8, z_all, y_all], buf.at[0, z_all, y_all], (1, 0, 0)),
            send(buf.at[1, z_all, y_all], buf.at[9, z_all, y_all], (-1, 0, 0)),
            send(buf.at[t_all, 8, y_all], buf.at[t_all, 0, y_all], (0, 1, 0)),
            send(buf.at[t_all, 1, y_all], buf.at[t_all, 9, y_all], (0, -1, 0)),
        ]

    def around0(slot, t):
        buf = v0.at[slot]
        mid = buf[t + 1, z_all, y_all, :]
        total = buf[t, z_all, y_all, :] + buf[t + 2, z_all, y_all, :]
        total += buf[t + 1, pl.ds(0, 8), y_all, :] + buf[t + 1, pl.ds(2, 8), y_all, :]
        total += buf[t + 1, z_all, pl.ds(OFF - 1, 16), :] + buf[t + 1, z_all, pl.ds(OFF + 1, 16), :]
        return mid, total + roll(mid, 1, 2) + roll(mid, -1, 2)

    def loop(low, high, body):
        lax.fori_loop(low, high, lambda t, c: (body(t), c)[1], 0)

    def sweep0(slot, out):
        def body(t):
            mid, total = around0(slot, t)
            d = 8.0 + m_ref[t]
            v0[out, t + 1, z_all, y_all, :] = mid + DAMPING * (s_ref[t] - (d * mid - total)) / d

        loop(0, 8, body)

    def residual0(slot, t):
        mid, total = around0(slot, t)
        return s_ref[t] - ((8.0 + m_ref[t]) * mid - total)

    def coarsen_plane(a, step):
        nz, ny, _ = a.shape
        a = a.reshape(nz // 2, 2, ny, 128)
        tmp[0 : nz // 2, 0:ny, :] = a[:, 0] + a[:, 1]
        b = tmp[0 : nz // 2, pl.ds(0, ny // 2, stride=2), :]
        b += tmp[0 : nz // 2, pl.ds(1, ny // 2, stride=2), :]
        return (b + partner(b, step, 2)) * (1.0 / 16.0)

    def swap1(buf, radius):
        def span(k, side):
            if side == 0:
                return pl.ds(3, 4), pl.ds(3, 4)
            if side == 1:
                return pl.ds(7 - k, k), pl.ds(3 - k, k)
            return pl.ds(3, k), pl.ds(7, k)

        group = []
        for a in (0, 1, -1):
            for b in (0, 1, -1):
                for c in (0, 1, -1):
                    k = radius + 1 - abs(a) - abs(b) - abs(c)
                    if k < 1 or not (a or b or c):
                        continue
                    (t_src, t_dst), (z_src, z_dst) = span(k, a), span(k, b)
                    y = {0: pl.ds(0, 8), 1: pl.ds(8 - k, k), -1: pl.ds(0, k)}[c]
                    y_dst = y if c == 0 else pl.ds(y.start + 8, y.size)
                    group.append(
                        send(buf.at[t_src, z_src, y], buf.at[t_dst, z_dst, y_dst], (a, b, abs(c)))
                    )
        return group

    def around1(slot, t, radius):
        nz = 4 + 2 * radius
        z = 3 - radius
        buf = v1.at[slot]
        mid = buf[t, pl.ds(z, nz)]
        total = buf[t - 1, pl.ds(z, nz)] + buf[t + 1, pl.ds(z, nz)]
        total += buf[t, pl.ds(z - 1, nz)] + buf[t, pl.ds(z + 1, nz)]
        total += roll(mid, 1, 1) + roll(mid, -1, 1)
        return mid, total + roll(mid, 2, 2) + roll(mid, -2, 2)

    def sweep1(slot, out, radius):
        z = pl.ds(3 - radius, 4 + 2 * radius)

        def body(t):
            mid, total = around1(slot, t, radius)
            d = 4.0 + m1[t, z]
            v1[out, t, z] = mid + DAMPING * (s1[t, z] - (d * mid - 0.5 * total)) / d

        loop(3 - radius, 7 + radius, body)

    def gather2(buf, block):
        buf[1, 0, 0:4, :] = pack4(block[0, 0], block[0, 1], block[1, 0], block[1, 1])
        own = buf.at[1, 0, pl.ds(0, 4)]
        return [
            send(own, buf.at[1 - a, (4 - b) % 4, pl.ds(4 * c, 4)], (a, b, c)) for a, b, c in near
        ]

    def unpack2(x, into, at):
        a, b, c, d = unpack4(x)
        for z in range(4):
            into[at, 2 * z], into[at, 2 * z + 1] = a[z], b[z]
            into[at + 1, 2 * z], into[at + 1, 2 * z + 1] = c[z], d[z]

    def image(buf, t, level):
        mid = buf[t]
        total = buf[t - 1] + buf[t + 1] + ring(mid, 1) + ring(mid, -1)
        step = level - 1
        total += roll(mid, step, 1) + roll(mid, -step, 1)
        step = 1 << level
        return mid, total + roll(mid, step, 2) + roll(mid, -step, 2)

    def sweep_ring(buf, out, source, mass, low, high, level):
        factor = 0.5**level

        def body(t):
            mid, total = image(buf, t, level)
            d = 8.0 * factor + mass[t]
            out[t] = mid + DAMPING * (source[t] - (d * mid - factor * total)) / d

        loop(low, high, body)

    def coarsen_ring(first, second):
        a = (first + second).reshape(4, 2, 8, 128)
        a = a[:, 0] + a[:, 1]
        a += partner(a, 1, 1)
        return (a + partner(a, 4, 2)) * (1.0 / 16.0)

    def pack3(x):
        row, lane = rows(x[0]), lanes(x[0])
        return jnp.where(
            even(row, 1), jnp.where(even(lane, 1), x[0], x[2]), jnp.where(even(lane, 1), x[1], x[3])
        )

    def unpack3(x, into, t):
        first, second = spread(x, 1, 0)
        into[t, 0], into[t, 2] = spread(first, 1, 1)
        into[t, 1], into[t, 3] = spread(second, 1, 1)

    def first0(t):
        v0[0, t + 1, z_all, y_all, :] = DAMPING * s_ref[t] / (8.0 + m_ref[t])

    loop(0, 8, first0)
    waiting = swap0(0)

    def mass1(t):
        m1[t + 3, pl.ds(3, 4), 0:8, :] = coarsen_plane(m_ref[2 * t] + m_ref[2 * t + 1], 1)

    loop(0, 4, mass1)
    own1 = pl.ds(3, 4)
    for t in range(2):
        s2[4 + t, 0:2, 0:4, :] = coarsen_plane(
            m1[3 + 2 * t, own1, 0:8, :] + m1[4 + 2 * t, own1, 0:8, :], 2
        )
    mass2_in = gather2(p2.at[0], s2[4:6, 0:2, 0:4, :])
    mass1_in = swap1(m1, 2)

    arrived(waiting)
    sweep0(0, 1)
    arrived(swap0(1))

    def down0(t):
        a = residual0(1, 2 * t) + residual0(1, 2 * t + 1)
        s1[t + 3, own1, 0:8, :] = coarsen_plane(a, 1)

    loop(0, 4, down0)
    waiting = swap1(s1, 2)
    arrived(mass1_in)
    arrived(mass2_in)
    for t in range(3):
        unpack2(p2[0, t], m2, 2 + 2 * t)
    d2_own[1] = p2[0, 1]
    mass3 = coarsen_ring(m2[4], m2[5])
    arrived(waiting)

    z_two = pl.ds(1, 8)

    def first1(t):
        v1[0, t, z_two] = DAMPING * s1[t, z_two] / (4.0 + m1[t, z_two])

    loop(1, 9, first1)
    sweep1(0, 1, 1)

    residuals = []
    for t in range(4):
        mid, total = around1(1, 3 + t, 0)
        mid, total = mid[:, 0:8], total[:, 0:8]
        d = 4.0 + m1[3 + t, own1, 0:8, :]
        residuals.append(s1[3 + t, own1, 0:8, :] - (d * mid - 0.5 * total))
    for t in range(2):
        s2[4 + t, 0:2, 0:4, :] = coarsen_plane(residuals[2 * t] + residuals[2 * t + 1], 2)
    waiting = gather2(p2.at[1], s2[4:6, 0:2, 0:4, :])
    for t in range(3, 7):
        v1[2, t, own1, 0:8, :] = v1[1, t, own1, 0:8, :]
    halo1_in = swap1(v1.at[2], 3)
    arrived(waiting)
    for t in range(3):
        unpack2(p2[1, t], s2, 2 + 2 * t)

    for t in range(2, 8):
        u2[t] = DAMPING * s2[t] / (2.0 + m2[t])
    sweep_ring(u2, v2, s2, m2, 3, 7, 2)
    remainders = []
    for t in (4, 5):
        mid, total = image(v2, t, 2)
        remainders.append(s2[t] - ((2.0 + m2[t]) * mid - 0.25 * total))
    d3[5, 0] = pack3(coarsen_ring(*remainders))
    d3[5, 1] = pack3(mass3)
    waiting = [
        send(d3.at[5], d3.at[5 - a], (a, 0, 0)) for k in range(1, 6) for a in (k, -k)
    ]
    d2_own[0] = p2[1, 1]
    pairs = v2[4:6].reshape(2, 4, 2, 8, 128)
    d2_own[2] = pack4(pairs[0, :, 0], pairs[0, :, 1], pairs[1, :, 0], pairs[1, :, 1])
    halo2_in = [
        send(d2_own, d2_in.at[2 - a], (a, 0, 0)) for a in (1, -1, 2, -2)
    ]
    arrived(waiting)

    for t in range(11):
        unpack3(d3[t, 0], s3, t)
        unpack3(d3[t, 1], m3, t)
        v3[0, t] = DAMPING * s3[t] / (1.0 + m3[t])
    for step in range(3):
        sweep_ring(v3.at[step], v3.at[step + 1], s3, m3, 1 + step, 10 - step, 3)

    arrived(halo2_in)
    for k, at in ((0, 0), (1, 2), (3, 6), (4, 8)):
        if k in (0, 4):
            unpack2(d2_in[k, 0], s2, at)
            unpack2(d2_in[k, 1], m2, at)
        unpack2(d2_in[k, 2], v2, at)
    for t in range(10):
        e = v3[3, 3 + t // 2]
        e = jnp.broadcast_to(e[:, None], (4, 2, 8, 128)).reshape(8, 8, 128)
        v2[t] = v2[t] + e
    sweep_ring(v2, u2, s2, m2, 1, 9, 2)
    sweep_ring(u2, v2, s2, m2, 2, 8, 2)

    arrived(halo1_in)
    for copy in halo1_in:
        copy.wait_send()
    copies = [copy for copy in copies if not any(copy is old for old in halo1_in)]
    for tc in range(6):
        for z in range(6):
            e = v2[2 + tc, (z - 2) % 8]
            tmp[z, pl.ds(0, 8, stride=2), :] = e
            tmp[z, pl.ds(1, 8, stride=2), :] = e
        e = tmp[0:6, 0:16, :]
        e = jnp.broadcast_to(e[:, None], (6, 2, 16, 128)).reshape(12, 16, 128)[1:11]
        for k in range(2):
            t = 2 * (tc - 2) + k + 3
            if 0 <= t < 10:
                v1[2, t] = v1[2, t] + e
    sweep1(2, 3, 2)
    sweep1(3, 4, 1)

    for tc in range(6):
        e = v1[4, 2 + tc, pl.ds(2, 6)]
        tmp[0:6, pl.ds(OFF, 8, stride=2), :] = e[:, 0:8]
        tmp[0:6, pl.ds(OFF + 1, 8, stride=2), :] = e[:, 0:8]
        tmp[0:6, OFF - 1 : OFF, :] = e[:, 15:16]
        tmp[0:6, OFF + 16 : OFF + 17, :] = e[:, 8:9]
        e = tmp[...]
        e = jnp.broadcast_to(e[:, None], (6, 2, 32, 128)).reshape(12, 32, 128)[1:11]
        for k in range(2):
            t = 2 * (tc - 1) + k + 1
            if 0 <= t < 10:
                v0[2, t] = v0[1, t] + e
    sweep0(2, 3)
    arrived(swap0(3))
    sweep0(3, 4)
    arrived(swap0(4))

    def finish(t):
        res_ref[t] = residual0(4, t)
        sol_ref[t] = v0[4, t + 1, z_all, y_all, :]

    loop(0, 8, finish)
    for copy in copies:
        copy.wait_send()


def per_device(right_side, mass_field):
    f32 = jnp.float32
    block = jax.ShapeDtypeStruct(right_side.shape, f32)
    vmem = pl.BlockSpec(memory_space=pltpu.VMEM)
    shapes = [
        (5, 10, 10, 32, 128),
        (10, 10, 16, 128), (10, 10, 16, 128), (5, 10, 10, 16, 128),
        (2, 3, 4, 8, 128), (10, 8, 8, 128), (10, 8, 8, 128), (10, 8, 8, 128), (10, 8, 8, 128),
        (3, 4, 8, 128), (5, 3, 4, 8, 128),
        (11, 2, 8, 128), (11, 4, 8, 128), (11, 4, 8, 128), (4, 11, 4, 8, 128),
        (6, 32, 128),
    ]
    scratch = [pltpu.VMEM(shape, f32) for shape in shapes]
    scratch += [pltpu.SemaphoreType.DMA((COPIES,))] * 2
    return pl.pallas_call(
        kernel,
        out_shape=(block, block),
        in_specs=[vmem, vmem],
        out_specs=(vmem, vmem),
        scratch_shapes=scratch,
        compiler_params=pltpu.CompilerParams(
            collective_id=0, has_side_effects=True, vmem_limit_bytes=48 * 1024 * 1024
        ),
    )(right_side, mass_field)


def solution(mesh):
    placed = (P("ta", "gz", "gy", None), P("ta", "gz", "gy", None))
    return jax.shard_map(
        per_device, mesh=mesh, in_specs=placed, out_specs=placed, check_vma=False
    )
```

```python
import jax
import jax.numpy as jnp
from jax import lax
from jax.experimental import pallas as pl
from jax.experimental.pallas import tpu as pltpu
from jax.sharding import PartitionSpec as P

DAMPING = 0.7
OFF = 8
ROWS = 8192
MESH = pl.DeviceIdType.MESH


def lanes(like):
    return lax.broadcasted_iota(jnp.int32, like.shape, like.ndim - 1)


def rows(like):
    return lax.broadcasted_iota(jnp.int32, like.shape, like.ndim - 2)


def roll(x, shift, axis):
    return pltpu.roll(x, shift % x.shape[axis], axis)


def ring(x, shift, axis=0):
    shift %= x.shape[axis]
    cut = x.shape[axis] - shift
    return jnp.concatenate(
        [lax.slice_in_dim(x, cut, x.shape[axis], axis=axis), lax.slice_in_dim(x, 0, cut, axis=axis)], axis=axis
    )


def even(index, step):
    return jnp.bitwise_and(index, step) == 0


def partner(x, step, axis):
    index = lax.broadcasted_iota(jnp.int32, x.shape, axis)
    return jnp.where(even(index, step), roll(x, -step, axis), roll(x, step, axis))


def spread(x, step, axis):
    index = lax.broadcasted_iota(jnp.int32, x.shape, axis)
    low = even(index, step)
    return jnp.where(low, x, roll(x, step, axis)), jnp.where(low, roll(x, -step, axis), x)


def pack4(a, b, c, d):
    lane = lanes(a)
    return jnp.where(
        even(lane, 2), jnp.where(even(lane, 1), a, b), jnp.where(even(lane, 1), c, d)
    )


def unpack4(x):
    last = x.ndim - 1
    first, second = spread(x, 1, last)
    a, c = spread(first, 2, last)
    b, d = spread(second, 2, last)
    return a, b, c, d


def kernel(
    s_hbm, m_hbm, sol_ref, res_ref,
    s0, m0, w0, r0, v0, ht, hz, hy, s1, m1, w1, v1, p2, s2, m2, w2, u2, v2, d2_own, d2_in, d3, s3, w3, v3, tmp, bytes_ref,
    load_sem, send_sem, recv_sem,
):
    ta, gz, gy = lax.axis_index("ta"), lax.axis_index("gz"), lax.axis_index("gy")
    nta, ngz, ngy = lax.axis_size("ta"), lax.axis_size("gz"), lax.axis_size("gy")

    load_m = pltpu.make_async_copy(m_hbm, m0, load_sem.at[0])
    load_s = pltpu.make_async_copy(s_hbm, s0, load_sem.at[1])
    load_m.start()
    load_s.start()

    def device(a, b, c):
        return (
            lax.rem(ta + (a + nta), nta),
            lax.rem(gz + (b + ngz), ngz),
            lax.rem(gy + c, ngy),
        )

    barrier = pltpu.get_barrier_semaphore()
    near = [(a, b, c) for a in (0, 1, -1) for b in range(4) for c in range(2)][1:]
    far = [(a, 0, 0) for k in range(2, 6) for a in (k, -k)]
    for offset in near + far:
        pl.semaphore_signal(barrier, inc=1, device_id=device(*offset), device_id_type=MESH)

    groups = []
    sends = [0, 0]

    class Group:
        def __init__(self, sender=0):
            self.number, self.count, self.sender = len(groups), 0, sender
            groups.append(self)

        def send(self, src, dst, offset):
            size = 1
            for extent in dst.shape[:-1]:
                size *= extent
            self.count += size
            sends[self.sender] += size
            pltpu.make_async_remote_copy(
                src_ref=src,
                dst_ref=dst,
                send_sem=send_sem.at[self.sender],
                recv_sem=recv_sem.at[self.number],
                device_id=device(*offset),
                device_id_type=MESH,
            ).start()

        def arrived(self):
            whole = bytes_ref.at[pl.ds(0, self.count)]
            pltpu.make_async_copy(whole, whole, recv_sem.at[self.number]).wait()

    def all_sent(sender):
        whole = bytes_ref.at[pl.ds(0, sends[sender])]
        pltpu.make_async_copy(whole, whole, send_sem.at[sender]).wait()

    def loop(low, high, body):
        lax.fori_loop(low, high, lambda t, c: (body(t), c)[1], 0)

    t_all, y_all = pl.ds(1, 8), pl.ds(OFF, 16)
    z_all = t_all

    def swap0(slot, n):
        buf = v0.at[slot]
        group = Group()
        group.send(buf.at[t_all, 8, y_all], hz.at[n, 0], (0, 1, 0))
        group.send(buf.at[t_all, 1, y_all], hz.at[n, 1], (0, -1, 0))
        one = pl.ds(0, 1)
        whole = pl.ds(0, 8)
        group.send(buf.at[t_all, z_all, pl.ds(OFF + 15, 1)], hy.at[n, 0, whole, whole, one], (0, 0, 1))
        group.send(buf.at[t_all, z_all, pl.ds(OFF, 1)], hy.at[n, 1, whole, whole, pl.ds(7, 1)], (0, 0, 1))
        group.send(buf.at[8, z_all, y_all], ht.at[n, 0], (1, 0, 0))
        group.send(buf.at[1, z_all, y_all], ht.at[n, 1], (-1, 0, 0))
        return group

    def around0(slot, t):
        buf = v0.at[slot]
        mid = buf[t + 1, z_all, y_all, :]
        total = buf[t, z_all, y_all, :] + buf[t + 2, z_all, y_all, :]
        total += buf[t + 1, pl.ds(0, 8), y_all, :] + buf[t + 1, pl.ds(2, 8), y_all, :]
        total += buf[t + 1, z_all, pl.ds(OFF - 1, 16), :] + buf[t + 1, z_all, pl.ds(OFF + 1, 16), :]
        return mid, total + roll(mid, 1, 2) + roll(mid, -1, 2)

    def clear0(slot):
        zero = jnp.zeros((8, 16, 128), jnp.float32)
        v0[slot, 0, z_all, y_all, :] = zero
        v0[slot, 9, z_all, y_all, :] = zero
        rim = jnp.zeros((8, OFF, 128), jnp.float32)

        def body(t):
            v0[slot, t + 1, 0, y_all, :] = zero[0]
            v0[slot, t + 1, 9, y_all, :] = zero[0]
            v0[slot, t + 1, z_all, pl.ds(0, OFF), :] = rim
            v0[slot, t + 1, z_all, pl.ds(OFF + 16, OFF), :] = rim

        loop(0, 8, body)

    def sweep0(slot, out):
        def body(t):
            mid, total = around0(slot, t)
            v0[out, t + 1, z_all, y_all, :] = (1.0 - DAMPING) * mid + v0[0, t + 1, z_all, y_all, :] + w0[t] * total

        loop(0, 8, body)

    def residual0(slot, t):
        mid, total = around0(slot, t)
        return s0[t] - ((8.0 + m0[t]) * mid - total)

    def halo_y(n, t):
        low, high = hy[n, 0, t], hy[n, 1, t]
        low = jnp.where(rows(low) == 0, low, 0.0)
        high = jnp.where(rows(high) == 7, high, 0.0)
        return jnp.concatenate([low, high], axis=1)

    def fix0(out, n):
        def body(t):
            v0[out, t + 1, z_all, y_all, :] = v0[out, t + 1, z_all, y_all, :] + w0[t] * halo_y(n, t)
            for side, z in ((0, 0), (1, 7)):
                v0[out, t + 1, z + 1, y_all, :] = v0[out, t + 1, z + 1, y_all, :] + w0[t, z] * hz[n, side, t]

        loop(0, 8, body)
        for side, t in ((0, 0), (1, 7)):
            v0[out, t + 1, z_all, y_all, :] = v0[out, t + 1, z_all, y_all, :] + w0[t] * ht[n, side]

    def add_halos(ref, n):
        def body(t):
            ref[t] = ref[t] + halo_y(n, t)
            for side, z in ((0, 0), (1, 7)):
                ref[t, z] = ref[t, z] + hz[n, side, t]

        loop(0, 8, body)
        for side, t in ((0, 0), (1, 7)):
            ref[t] = ref[t] + ht[n, side]

    def coarsen_plane(a, step):
        nz, ny, _ = a.shape
        a = a.reshape(nz // 2, 2, ny, 128)
        tmp[0 : nz // 2, 0:ny, :] = a[:, 0] + a[:, 1]
        b = tmp[0 : nz // 2, pl.ds(0, ny // 2, stride=2), :]
        b += tmp[0 : nz // 2, pl.ds(1, ny // 2, stride=2), :]
        return (b + partner(b, step, 2)) * (1.0 / 16.0)

    def swap1(buf, radius, sender=0):
        def span(k, side):
            if side == 0:
                return pl.ds(3, 4), pl.ds(3, 4)
            if side == 1:
                return pl.ds(7 - k, k), pl.ds(3 - k, k)
            return pl.ds(3, k), pl.ds(7, k)

        group = Group(sender)
        offsets = [(a, b, c) for a in (0, 1, -1) for b in (0, 1, -1) for c in (0, 1, -1)][1:]
        for a, b, c in sorted(offsets, key=lambda o: -sum(map(abs, o))):
            k = radius + 1 - abs(a) - abs(b) - abs(c)
            if k < 1:
                continue
            (t_src, t_dst), (z_src, z_dst) = span(k, a), span(k, b)
            y = {0: pl.ds(0, 8), 1: pl.ds(8 - k, k), -1: pl.ds(0, k)}[c]
            y_dst = y if c == 0 else pl.ds(y.start + 8, y.size)
            group.send(buf.at[t_src, z_src, y], buf.at[t_dst, z_dst, y_dst], (a, b, abs(c)))
        return group

    def around1(slot, t, radius):
        nz = 4 + 2 * radius
        z = 3 - radius
        buf = v1.at[slot]
        mid = buf[t, pl.ds(z, nz)]
        total = buf[t - 1, pl.ds(z, nz)] + buf[t + 1, pl.ds(z, nz)]
        total += buf[t, pl.ds(z - 1, nz)] + buf[t, pl.ds(z + 1, nz)]
        total += roll(mid, 1, 1) + roll(mid, -1, 1)
        return mid, total + roll(mid, 2, 2) + roll(mid, -2, 2)

    def sweep1(slot, out, radius):
        z = pl.ds(3 - radius, 4 + 2 * radius)

        def body(t):
            mid, total = around1(slot, t, radius)
            v1[out, t, z] = (1.0 - DAMPING) * mid + v1[0, t, z] + w1[t, z] * total

        loop(3 - radius, 7 + radius, body)

    def gather2(buf, block):
        buf[1, 0, 0:4, :] = pack4(block[0, 0], block[0, 1], block[1, 0], block[1, 1])
        own = buf.at[1, 0, pl.ds(0, 4)]
        group = Group()
        for a, b, c in sorted(near, key=lambda o: -(abs(o[0]) + (0, 1, 2, 1)[o[1]] + 2 * o[2])):
            group.send(own, buf.at[1 - a, (4 - b) % 4, pl.ds(4 * c, 4)], (a, b, c))
        return group

    def unpack2(x, into, at):
        a, b, c, d = unpack4(x)
        into[at] = jnp.stack([a, b], axis=1).reshape(8, 8, 128)
        into[at + 1] = jnp.stack([c, d], axis=1).reshape(8, 8, 128)

    def image(buf, t, count, level):
        mid = buf[pl.ds(t, count)]
        total = buf[pl.ds(t - 1, count)] + buf[pl.ds(t + 1, count)] + ring(mid, 1, 1) + ring(mid, -1, 1)
        step = level - 1
        total += roll(mid, step, 2) + roll(mid, -step, 2)
        step = 1 << level
        return mid, total + roll(mid, step, 3) + roll(mid, -step, 3)

    def sweep_ring(buf, out, first, weight, low, high, level, count):
        def body(i):
            t = low + i * count
            mid, total = image(buf, t, count, level)
            span = pl.ds(t, count)
            out[span] = (1.0 - DAMPING) * mid + first[span] + weight[span] * total

        if high - low == count:
            body(0)
        else:
            loop(0, (high - low) // count, body)

    def coarsen_ring(first, second):
        a = (first + second).reshape(4, 2, 8, 128)
        a = a[:, 0] + a[:, 1]
        a += partner(a, 1, 1)
        return (a + partner(a, 4, 2)) * (1.0 / 16.0)

    def pack3(x):
        row, lane = rows(x[0]), lanes(x[0])
        return jnp.where(
            even(row, 1), jnp.where(even(lane, 1), x[0], x[2]), jnp.where(even(lane, 1), x[1], x[3])
        )

    def unpack3(x):
        first, second = spread(x, 1, 0)
        a, c = spread(first, 1, 1)
        b, d = spread(second, 1, 1)
        return jnp.stack([a, b, c, d])

    load_m.wait()
    load_s.wait()

    def first0(t):
        w = DAMPING / (8.0 + m0[t])
        w0[t] = w
        v0[0, t + 1, z_all, y_all, :] = w * s0[t]

    loop(0, 8, first0)
    pl.semaphore_wait(barrier, len(near) + len(far))
    halos = swap0(0, 0)

    def mass1(t):
        m1[t + 3, pl.ds(3, 4), 0:8, :] = coarsen_plane(m0[2 * t] + m0[2 * t + 1], 1)

    loop(0, 4, mass1)
    own1 = pl.ds(3, 4)
    for t in range(2):
        s2[4 + t, 0:2, 0:4, :] = coarsen_plane(
            m1[3 + 2 * t, own1, 0:8, :] + m1[4 + 2 * t, own1, 0:8, :], 2
        )
    mass2_in = gather2(p2.at[0], s2[4:6, 0:2, 0:4, :])
    mass1_in = swap1(m1, 2)
    for slot in (0, 1, 3, 4):
        clear0(slot)
    sweep0(0, 1)

    halos.arrived()
    fix0(1, 0)
    halos = swap0(1, 1)

    def rest0(t):
        r0[t] = residual0(1, t)

    loop(0, 8, rest0)
    halos.arrived()
    add_halos(r0, 1)

    def down0(t):
        s1[t + 3, own1, 0:8, :] = coarsen_plane(r0[2 * t] + r0[2 * t + 1], 1)

    loop(0, 4, down0)
    source1_in = swap1(s1, 2)
    mass1_in.arrived()
    mass2_in.arrived()
    z_two = pl.ds(1, 8)

    def weight1(t):
        w1[t, z_two] = 0.5 * DAMPING / (4.0 + m1[t, z_two])

    loop(1, 9, weight1)
    loop(0, 3, lambda t: unpack2(p2[0, t], m2, 2 + 2 * t))
    mass3 = coarsen_ring(m2[4], m2[5])
    d3[5, 1] = pack3(mass3)
    d2_own[1] = p2[0, 1]

    def weight2(t):
        w2[t] = 0.25 * DAMPING / (2.0 + m2[t])

    loop(2, 8, weight2)
    source1_in.arrived()

    def first1(t):
        v1[0, t, z_two] = 2.0 * w1[t, z_two] * s1[t, z_two]

    loop(1, 9, first1)
    sweep1(0, 1, 1)

    def down1(t):
        mid, total = around1(1, 3 + t, 0)
        mid, total = mid[:, 0:8], total[:, 0:8]
        d = 4.0 + m1[3 + t, own1, 0:8, :]
        r0[t, 0:4, 0:8, :] = s1[3 + t, own1, 0:8, :] - (d * mid - 0.5 * total)

    loop(0, 4, down1)
    for t in range(2):
        s2[4 + t, 0:2, 0:4, :] = coarsen_plane(r0[2 * t, 0:4, 0:8, :] + r0[2 * t + 1, 0:4, 0:8, :], 2)
    source2_in = gather2(p2.at[1], s2[4:6, 0:2, 0:4, :])
    for t in range(3, 7):
        v1[2, t, own1, 0:8, :] = v1[1, t, own1, 0:8, :]
    halo1_in = swap1(v1.at[2], 3, 1)
    source2_in.arrived()
    loop(0, 3, lambda t: unpack2(p2[1, t], s2, 2 + 2 * t))

    def first2(t):
        u2[t] = 4.0 * w2[t] * s2[t]

    loop(2, 8, first2)
    sweep_ring(u2, v2, u2, w2, 3, 7, 2, 4)
    mid, total = image(v2, 4, 2, 2)
    remainder = s2[4:6] - ((2.0 + m2[4:6]) * mid - 0.25 * total)
    d3[5, 0] = pack3(coarsen_ring(remainder[0], remainder[1]))
    planes_in = Group()
    for k in range(5, 0, -1):
        for a in (k, -k):
            planes_in.send(d3.at[5], d3.at[5 - a], (a, 0, 0))
    d2_own[0] = p2[1, 1]
    pairs = v2[4:6].reshape(2, 4, 2, 8, 128)
    d2_own[2] = pack4(pairs[0, :, 0], pairs[0, :, 1], pairs[1, :, 0], pairs[1, :, 1])
    halo2_in = Group()
    for a in (1, -1, 2, -2):
        halo2_in.send(d2_own, d2_in.at[2 - a], (a, 0, 0))
    planes_in.arrived()

    def first3(t):
        w = 0.125 * DAMPING / (1.0 + unpack3(d3[t, 1]))
        w3[t] = w
        v3[0, t] = 8.0 * w * unpack3(d3[t, 0])

    loop(0, 11, first3)
    for step in range(3):
        sweep_ring(v3.at[step], v3.at[step + 1], v3.at[0], w3, 1 + step, 10 - step, 3, 9 - 2 * step)

    halo2_in.arrived()
    for k, at in ((0, 0), (4, 8)):
        unpack2(d2_in[k, 0], s2, at)
        unpack2(d2_in[k, 1], m2, at)
    for k, at in ((0, 0), (1, 2), (3, 6), (4, 8)):
        unpack2(d2_in[k, 2], v2, at)
    for at in (0, 8):
        w = 0.25 * DAMPING / (2.0 + m2[at : at + 2])
        w2[at : at + 2] = w
        u2[at : at + 2] = 4.0 * w * s2[at : at + 2]

    def correct2(t):
        e = v3[3, 3 + t]
        e = jnp.broadcast_to(e[:, None], (4, 2, 8, 128)).reshape(8, 8, 128)
        for k in range(2):
            v2[2 * t + k] = v2[2 * t + k] + e

    loop(0, 5, correct2)
    sweep_ring(v2, s2, u2, w2, 1, 9, 2, 2)
    sweep_ring(s2, v2, u2, w2, 2, 8, 2, 2)

    halo1_in.arrived()
    all_sent(1)

    def expand1(tc):
        for z in range(6):
            e = v2[2 + tc, (z - 2) % 8]
            tmp[z, pl.ds(0, 8, stride=2), :] = e
            tmp[z, pl.ds(1, 8, stride=2), :] = e
        e = tmp[0:6, 0:16, :]
        return jnp.broadcast_to(e[:, None], (6, 2, 16, 128)).reshape(12, 16, 128)[1:11]

    e = expand1(0)
    v1[2, 0] = v1[2, 0] + e

    def correct1(tc):
        e = expand1(tc)
        for k in range(2):
            v1[2, 2 * tc + k - 1] = v1[2, 2 * tc + k - 1] + e

    loop(1, 5, correct1)
    e = expand1(5)
    v1[2, 9] = v1[2, 9] + e
    sweep1(2, 3, 2)
    sweep1(3, 4, 1)

    def expand0(tc):
        e = v1[4, 2 + tc, pl.ds(2, 6)]
        tmp[0:6, pl.ds(OFF, 8, stride=2), :] = e[:, 0:8]
        tmp[0:6, pl.ds(OFF + 1, 8, stride=2), :] = e[:, 0:8]
        tmp[0:6, OFF - 1 : OFF, :] = e[:, 15:16]
        tmp[0:6, OFF + 16 : OFF + 17, :] = e[:, 8:9]
        e = tmp[...]
        return jnp.broadcast_to(e[:, None], (6, 2, 32, 128)).reshape(12, 32, 128)[1:11]

    v0[2, 0] = expand0(0)

    def correct0(tc):
        e = expand0(tc)
        for k in range(2):
            v0[2, 2 * tc + k - 1] = v0[1, 2 * tc + k - 1] + e

    loop(1, 5, correct0)
    v0[2, 9] = expand0(5)
    sweep0(2, 3)
    fix0(3, 1)
    halos = swap0(3, 2)
    sweep0(3, 4)
    halos.arrived()
    fix0(4, 2)
    halos = swap0(4, 3)

    def finish(t):
        res_ref[t] = residual0(4, t)
        sol_ref[t] = v0[4, t + 1, z_all, y_all, :]

    loop(0, 8, finish)
    halos.arrived()
    add_halos(res_ref, 3)
    all_sent(0)


def per_device(right_side, mass_field):
    f32 = jnp.float32
    block = jax.ShapeDtypeStruct(right_side.shape, f32)
    vmem = pl.BlockSpec(memory_space=pltpu.VMEM)
    hbm = pl.BlockSpec(memory_space=pltpu.HBM)
    own, ring2, ring3 = (8, 8, 16, 128), (10, 8, 8, 128), (11, 4, 8, 128)
    shapes = [
        own, own, own, own, (5, 10, 10, 32, 128),
        (4, 2, 8, 16, 128), (4, 2, 8, 16, 128), (4, 2, 8, 8, 8, 128),
        (10, 10, 16, 128), (10, 10, 16, 128), (10, 10, 16, 128), (5, 10, 10, 16, 128),
        (2, 3, 4, 8, 128), ring2, ring2, ring2, ring2, ring2, (3, 4, 8, 128), (5, 3, 4, 8, 128),
        (11, 2, 8, 128), ring3, ring3, (4,) + ring3,
        (6, 32, 128), (ROWS, 128),
    ]
    scratch = [pltpu.VMEM(shape, f32) for shape in shapes]
    scratch += [pltpu.SemaphoreType.DMA((count,)) for count in (2, 2, 11)]
    return pl.pallas_call(
        kernel,
        out_shape=(block, block),
        in_specs=[hbm, hbm],
        out_specs=(vmem, vmem),
        scratch_shapes=scratch,
        compiler_params=pltpu.CompilerParams(
            collective_id=0, has_side_effects=True, vmem_limit_bytes=56 * 1024 * 1024
        ),
    )(right_side, mass_field)


def solution(mesh):
    placed = (P("ta", "gz", "gy", None), P("ta", "gz", "gy", None))
    return jax.shard_map(
        per_device, mesh=mesh, in_specs=placed, out_specs=placed, check_vma=False
    )
```

```python
import jax
import jax.numpy as jnp
from jax import lax
from jax.experimental import pallas as pl
from jax.experimental.pallas import tpu as pltpu
from jax.sharding import PartitionSpec as P

DAMPING = 0.7
OFF = 8
ROWS = 8192
MESH = pl.DeviceIdType.MESH


def lanes(like):
    return lax.broadcasted_iota(jnp.int32, like.shape, like.ndim - 1)


def rows(like):
    return lax.broadcasted_iota(jnp.int32, like.shape, like.ndim - 2)


def roll(x, shift, axis):
    return pltpu.roll(x, shift % x.shape[axis], axis)


def ring(x, shift, axis=0):
    shift %= x.shape[axis]
    cut = x.shape[axis] - shift
    return jnp.concatenate(
        [lax.slice_in_dim(x, cut, x.shape[axis], axis=axis), lax.slice_in_dim(x, 0, cut, axis=axis)], axis=axis
    )


def even(index, step):
    return jnp.bitwise_and(index, step) == 0


def partner(x, step, axis):
    index = lax.broadcasted_iota(jnp.int32, x.shape, axis)
    return jnp.where(even(index, step), roll(x, -step, axis), roll(x, step, axis))


def spread(x, step, axis):
    index = lax.broadcasted_iota(jnp.int32, x.shape, axis)
    low = even(index, step)
    return jnp.where(low, x, roll(x, step, axis)), jnp.where(low, roll(x, -step, axis), x)


def pack4(a, b, c, d):
    lane = lanes(a)
    return jnp.where(
        even(lane, 2), jnp.where(even(lane, 1), a, b), jnp.where(even(lane, 1), c, d)
    )


def unpack4(x):
    last = x.ndim - 1
    first, second = spread(x, 1, last)
    a, c = spread(first, 2, last)
    b, d = spread(second, 2, last)
    return a, b, c, d


def kernel(
    s_hbm, m_hbm, sol_ref, res_ref,
    s0, m0, w0, r0, v0, ht, hz, hy, s1, m1, w1, v1, p2, s2, m2, w2, u2, v2, d2_own, d2_in, d3, s3, w3, v3, tmp, bytes_ref,
    load_sem, send_sem, recv_sem,
):
    ta, gz, gy = lax.axis_index("ta"), lax.axis_index("gz"), lax.axis_index("gy")
    nta, ngz, ngy = lax.axis_size("ta"), lax.axis_size("gz"), lax.axis_size("gy")

    load_m = pltpu.make_async_copy(m_hbm, m0, load_sem.at[0])
    load_s = pltpu.make_async_copy(s_hbm, s0, load_sem.at[1])
    load_m.start()
    load_s.start()

    def device(a, b, c):
        return (
            lax.rem(ta + (a + nta), nta),
            lax.rem(gz + (b + ngz), ngz),
            lax.rem(gy + c, ngy),
        )

    barrier = pltpu.get_barrier_semaphore()
    near = [(a, b, c) for a in (0, 1, -1) for b in range(4) for c in range(2)][1:]
    faces = [(1, 0, 0), (-1, 0, 0), (0, 1, 0), (0, -1, 0), (0, 0, 1)]
    for offset in faces:
        pl.semaphore_signal(barrier, inc=1, device_id=device(*offset), device_id_type=MESH)

    groups = []
    sends = [0, 0]

    class Group:
        def __init__(self, sender=0):
            self.number, self.count, self.sender = len(groups), 0, sender
            groups.append(self)

        def send(self, src, dst, offset):
            size = 1
            for extent in dst.shape[:-1]:
                size *= extent
            self.count += size
            sends[self.sender] += size
            pltpu.make_async_remote_copy(
                src_ref=src,
                dst_ref=dst,
                send_sem=send_sem.at[self.sender],
                recv_sem=recv_sem.at[self.number],
                device_id=device(*offset),
                device_id_type=MESH,
            ).start()

        def arrived(self):
            whole = bytes_ref.at[pl.ds(0, self.count)]
            pltpu.make_async_copy(whole, whole, recv_sem.at[self.number]).wait()

    def all_sent(sender):
        whole = bytes_ref.at[pl.ds(0, sends[sender])]
        pltpu.make_async_copy(whole, whole, send_sem.at[sender]).wait()

    def loop(low, high, body):
        lax.fori_loop(low, high, lambda t, c: (body(t), c)[1], 0)

    t_all, y_all = pl.ds(1, 8), pl.ds(OFF, 16)
    z_all = t_all

    def swap0(slot, n):
        buf = v0.at[slot]
        group = Group()
        group.send(buf.at[t_all, 8, y_all], hz.at[n, 0], (0, 1, 0))
        group.send(buf.at[t_all, 1, y_all], hz.at[n, 1], (0, -1, 0))
        one = pl.ds(0, 1)
        whole = pl.ds(0, 8)
        group.send(buf.at[t_all, z_all, pl.ds(OFF + 15, 1)], hy.at[n, 0, whole, whole, one], (0, 0, 1))
        group.send(buf.at[t_all, z_all, pl.ds(OFF, 1)], hy.at[n, 1, whole, whole, pl.ds(7, 1)], (0, 0, 1))
        group.send(buf.at[8, z_all, y_all], ht.at[n, 0], (1, 0, 0))
        group.send(buf.at[1, z_all, y_all], ht.at[n, 1], (-1, 0, 0))
        return group

    def around0(slot, t):
        buf = v0.at[slot]
        mid = buf[t + 1, z_all, y_all, :]
        total = buf[t, z_all, y_all, :] + buf[t + 2, z_all, y_all, :]
        total += buf[t + 1, pl.ds(0, 8), y_all, :] + buf[t + 1, pl.ds(2, 8), y_all, :]
        total += buf[t + 1, z_all, pl.ds(OFF - 1, 16), :] + buf[t + 1, z_all, pl.ds(OFF + 1, 16), :]
        return mid, total + roll(mid, 1, 2) + roll(mid, -1, 2)

    def clear0(slot):
        zero = jnp.zeros((8, 16, 128), jnp.float32)
        v0[slot, 0, z_all, y_all, :] = zero
        v0[slot, 9, z_all, y_all, :] = zero
        rim = jnp.zeros((8, OFF, 128), jnp.float32)

        def body(t):
            v0[slot, t + 1, 0, y_all, :] = zero[0]
            v0[slot, t + 1, 9, y_all, :] = zero[0]
            v0[slot, t + 1, z_all, pl.ds(0, OFF), :] = rim
            v0[slot, t + 1, z_all, pl.ds(OFF + 16, OFF), :] = rim

        loop(0, 8, body)

    def sweep0(slot, out):
        def body(t):
            mid, total = around0(slot, t)
            v0[out, t + 1, z_all, y_all, :] = (1.0 - DAMPING) * mid + v0[0, t + 1, z_all, y_all, :] + w0[t] * total

        loop(0, 8, body)

    def residual0(slot, t):
        mid, total = around0(slot, t)
        return s0[t] - ((8.0 + m0[t]) * mid - total)

    def halo_y(n, t):
        low, high = hy[n, 0, t], hy[n, 1, t]
        low = jnp.where(rows(low) == 0, low, 0.0)
        high = jnp.where(rows(high) == 7, high, 0.0)
        return jnp.concatenate([low, high], axis=1)

    def fix0(out, n):
        def body(t):
            v0[out, t + 1, z_all, y_all, :] = v0[out, t + 1, z_all, y_all, :] + w0[t] * halo_y(n, t)
            for side, z in ((0, 0), (1, 7)):
                v0[out, t + 1, z + 1, y_all, :] = v0[out, t + 1, z + 1, y_all, :] + w0[t, z] * hz[n, side, t]

        loop(0, 8, body)
        for side, t in ((0, 0), (1, 7)):
            v0[out, t + 1, z_all, y_all, :] = v0[out, t + 1, z_all, y_all, :] + w0[t] * ht[n, side]

    def add_halos(ref, n):
        def body(t):
            ref[t] = ref[t] + halo_y(n, t)
            for side, z in ((0, 0), (1, 7)):
                ref[t, z] = ref[t, z] + hz[n, side, t]

        loop(0, 8, body)
        for side, t in ((0, 0), (1, 7)):
            ref[t] = ref[t] + ht[n, side]

    def coarsen_plane(a, step):
        nz, ny, _ = a.shape
        a = a.reshape(nz // 2, 2, ny, 128)
        tmp[0 : nz // 2, 0:ny, :] = a[:, 0] + a[:, 1]
        b = tmp[0 : nz // 2, pl.ds(0, ny // 2, stride=2), :]
        b += tmp[0 : nz // 2, pl.ds(1, ny // 2, stride=2), :]
        return (b + partner(b, step, 2)) * (1.0 / 16.0)

    def swap1(buf, radius, sender=0):
        def span(k, side):
            if side == 0:
                return pl.ds(3, 4), pl.ds(3, 4)
            if side == 1:
                return pl.ds(7 - k, k), pl.ds(3 - k, k)
            return pl.ds(3, k), pl.ds(7, k)

        group = Group(sender)
        offsets = [(a, b, c) for a in (0, 1, -1) for b in (0, 1, -1) for c in (0, 1, -1)][1:]
        for a, b, c in sorted(offsets, key=lambda o: -sum(map(abs, o))):
            k = radius + 1 - abs(a) - abs(b) - abs(c)
            if k < 1:
                continue
            (t_src, t_dst), (z_src, z_dst) = span(k, a), span(k, b)
            y = {0: pl.ds(0, 8), 1: pl.ds(8 - k, k), -1: pl.ds(0, k)}[c]
            y_dst = y if c == 0 else pl.ds(y.start + 8, y.size)
            group.send(buf.at[t_src, z_src, y], buf.at[t_dst, z_dst, y_dst], (a, b, abs(c)))
        return group

    def around1(slot, t, radius):
        nz = 4 + 2 * radius
        z = 3 - radius
        buf = v1.at[slot]
        mid = buf[t, pl.ds(z, nz)]
        total = buf[t - 1, pl.ds(z, nz)] + buf[t + 1, pl.ds(z, nz)]
        total += buf[t, pl.ds(z - 1, nz)] + buf[t, pl.ds(z + 1, nz)]
        total += roll(mid, 1, 1) + roll(mid, -1, 1)
        return mid, total + roll(mid, 2, 2) + roll(mid, -2, 2)

    def sweep1(slot, out, radius):
        z = pl.ds(3 - radius, 4 + 2 * radius)

        def body(t):
            mid, total = around1(slot, t, radius)
            v1[out, t, z] = (1.0 - DAMPING) * mid + v1[0, t, z] + w1[t, z] * total

        loop(3 - radius, 7 + radius, body)

    def pack2(kind, block):
        p2[1, 0, kind, 0:4, :] = pack4(block[0, 0], block[0, 1], block[1, 0], block[1, 1])

    def gather2():
        whole = pl.ds(0, 2)
        own = p2.at[1, 0, whole, pl.ds(0, 4)]
        group = Group()
        for a, b, c in sorted(near, key=lambda o: -(abs(o[0]) + (0, 1, 2, 1)[o[1]] + 2 * o[2])):
            group.send(own, p2.at[1 - a, (4 - b) % 4, whole, pl.ds(4 * c, 4)], (a, b, c))
        return group

    def unpack2(x, into, at):
        a, b, c, d = unpack4(x)
        into[at] = jnp.stack([a, b], axis=1).reshape(8, 8, 128)
        into[at + 1] = jnp.stack([c, d], axis=1).reshape(8, 8, 128)

    def image(buf, t, count, level):
        mid = buf[pl.ds(t, count)]
        total = buf[pl.ds(t - 1, count)] + buf[pl.ds(t + 1, count)] + ring(mid, 1, 1) + ring(mid, -1, 1)
        step = level - 1
        total += roll(mid, step, 2) + roll(mid, -step, 2)
        step = 1 << level
        return mid, total + roll(mid, step, 3) + roll(mid, -step, 3)

    def sweep_ring(buf, out, first, weight, low, high, level, count):
        def body(i):
            t = low + i * count
            mid, total = image(buf, t, count, level)
            span = pl.ds(t, count)
            out[span] = (1.0 - DAMPING) * mid + first[span] + weight[span] * total

        if high - low == count:
            body(0)
        else:
            loop(0, (high - low) // count, body)

    def coarsen_ring(first, second):
        a = (first + second).reshape(4, 2, 8, 128)
        a = a[:, 0] + a[:, 1]
        a += partner(a, 1, 1)
        return (a + partner(a, 4, 2)) * (1.0 / 16.0)

    def pack3(x):
        row, lane = rows(x[0]), lanes(x[0])
        return jnp.where(
            even(row, 1), jnp.where(even(lane, 1), x[0], x[2]), jnp.where(even(lane, 1), x[1], x[3])
        )

    def unpack3(x):
        first, second = spread(x, 1, 0)
        a, c = spread(first, 1, 1)
        b, d = spread(second, 1, 1)
        return jnp.stack([a, b, c, d])

    load_m.wait()
    load_s.wait()

    def first0(t):
        w = DAMPING / (8.0 + m0[t])
        w0[t] = w
        v0[0, t + 1, z_all, y_all, :] = w * s0[t]

    loop(0, 8, first0)
    pl.semaphore_wait(barrier, len(faces))
    halos = swap0(0, 0)

    def mass1(t):
        m1[t + 3, pl.ds(3, 4), 0:8, :] = coarsen_plane(m0[2 * t] + m0[2 * t + 1], 1)

    loop(0, 4, mass1)
    own1 = pl.ds(3, 4)
    for t in range(2):
        s2[4 + t, 0:2, 0:4, :] = coarsen_plane(
            m1[3 + 2 * t, own1, 0:8, :] + m1[4 + 2 * t, own1, 0:8, :], 2
        )
    pack2(1, s2[4:6, 0:2, 0:4, :])
    for slot in (0, 1, 3, 4):
        clear0(slot)
    sweep0(0, 1)

    halos.arrived()
    fix0(1, 0)
    halos = swap0(1, 1)
    mass1_in = swap1(m1, 2)

    def rest0(t):
        r0[t] = residual0(1, t)

    loop(0, 8, rest0)
    halos.arrived()
    add_halos(r0, 1)

    def down0(t):
        s1[t + 3, own1, 0:8, :] = coarsen_plane(r0[2 * t] + r0[2 * t + 1], 1)

    loop(0, 4, down0)
    source1_in = swap1(s1, 2)
    mass1_in.arrived()
    z_two = pl.ds(1, 8)

    def weight1(t):
        w1[t, z_two] = 0.5 * DAMPING / (4.0 + m1[t, z_two])

    loop(1, 9, weight1)
    source1_in.arrived()

    def first1(t):
        v1[0, t, z_two] = 2.0 * w1[t, z_two] * s1[t, z_two]

    loop(1, 9, first1)
    sweep1(0, 1, 1)

    def down1(t):
        mid, total = around1(1, 3 + t, 0)
        mid, total = mid[:, 0:8], total[:, 0:8]
        d = 4.0 + m1[3 + t, own1, 0:8, :]
        r0[t, 0:4, 0:8, :] = s1[3 + t, own1, 0:8, :] - (d * mid - 0.5 * total)

    loop(0, 4, down1)
    for t in range(2):
        s2[4 + t, 0:2, 0:4, :] = coarsen_plane(r0[2 * t, 0:4, 0:8, :] + r0[2 * t + 1, 0:4, 0:8, :], 2)
    pack2(0, s2[4:6, 0:2, 0:4, :])
    source2_in = gather2()
    for t in range(3, 7):
        v1[2, t, own1, 0:8, :] = v1[1, t, own1, 0:8, :]
    halo1_in = swap1(v1.at[2], 3, 1)
    source2_in.arrived()

    def first2(t):
        unpack2(p2[t, :, 0], s2, 2 + 2 * t)
        unpack2(p2[t, :, 1], m2, 2 + 2 * t)
        span = pl.ds(2 + 2 * t, 2)
        w = 0.25 * DAMPING / (2.0 + m2[span])
        w2[span] = w
        u2[span] = 4.0 * w * s2[span]

    loop(0, 3, first2)
    sweep_ring(u2, v2, u2, w2, 3, 7, 2, 4)
    mid, total = image(v2, 4, 2, 2)
    remainder = s2[4:6] - ((2.0 + m2[4:6]) * mid - 0.25 * total)
    d3[5, 0] = pack3(coarsen_ring(remainder[0], remainder[1]))
    d3[5, 1] = pack3(coarsen_ring(m2[4], m2[5]))
    planes_in = Group()
    for k in range(5, 0, -1):
        for a in (k, -k):
            planes_in.send(d3.at[5], d3.at[5 - a], (a, 0, 0))
    d2_own[0] = p2[1, :, 0]
    d2_own[1] = p2[1, :, 1]
    pairs = v2[4:6].reshape(2, 4, 2, 8, 128)
    d2_own[2] = pack4(pairs[0, :, 0], pairs[0, :, 1], pairs[1, :, 0], pairs[1, :, 1])
    halo2_in = Group()
    for a in (1, -1, 2, -2):
        halo2_in.send(d2_own, d2_in.at[2 - a], (a, 0, 0))
    planes_in.arrived()

    def first3(t):
        w = 0.125 * DAMPING / (1.0 + unpack3(d3[t, 1]))
        w3[t] = w
        v3[0, t] = 8.0 * w * unpack3(d3[t, 0])

    loop(0, 11, first3)
    for step in range(3):
        sweep_ring(v3.at[step], v3.at[step + 1], v3.at[0], w3, 1 + step, 10 - step, 3, 9 - 2 * step)

    halo2_in.arrived()
    for k, at in ((0, 0), (4, 8)):
        unpack2(d2_in[k, 0], s2, at)
        unpack2(d2_in[k, 1], m2, at)
    for k, at in ((0, 0), (1, 2), (3, 6), (4, 8)):
        unpack2(d2_in[k, 2], v2, at)
    for at in (0, 8):
        w = 0.25 * DAMPING / (2.0 + m2[at : at + 2])
        w2[at : at + 2] = w
        u2[at : at + 2] = 4.0 * w * s2[at : at + 2]

    def correct2(t):
        e = v3[3, 3 + t]
        e = jnp.broadcast_to(e[:, None], (4, 2, 8, 128)).reshape(8, 8, 128)
        for k in range(2):
            v2[2 * t + k] = v2[2 * t + k] + e

    loop(0, 5, correct2)
    sweep_ring(v2, s2, u2, w2, 1, 9, 2, 2)
    sweep_ring(s2, v2, u2, w2, 2, 8, 2, 2)

    halo1_in.arrived()
    all_sent(1)

    def expand1(tc):
        for z in range(6):
            e = v2[2 + tc, (z - 2) % 8]
            tmp[z, pl.ds(0, 8, stride=2), :] = e
            tmp[z, pl.ds(1, 8, stride=2), :] = e
        e = tmp[0:6, 0:16, :]
        return jnp.broadcast_to(e[:, None], (6, 2, 16, 128)).reshape(12, 16, 128)[1:11]

    e = expand1(0)
    v1[2, 0] = v1[2, 0] + e

    def correct1(tc):
        e = expand1(tc)
        for k in range(2):
            v1[2, 2 * tc + k - 1] = v1[2, 2 * tc + k - 1] + e

    loop(1, 5, correct1)
    e = expand1(5)
    v1[2, 9] = v1[2, 9] + e
    sweep1(2, 3, 2)
    sweep1(3, 4, 1)

    def expand0(tc):
        e = v1[4, 2 + tc, pl.ds(2, 6)]
        tmp[0:6, pl.ds(OFF, 8, stride=2), :] = e[:, 0:8]
        tmp[0:6, pl.ds(OFF + 1, 8, stride=2), :] = e[:, 0:8]
        tmp[0:6, OFF - 1 : OFF, :] = e[:, 15:16]
        tmp[0:6, OFF + 16 : OFF + 17, :] = e[:, 8:9]
        e = tmp[...]
        return jnp.broadcast_to(e[:, None], (6, 2, 32, 128)).reshape(12, 32, 128)[1:11]

    v0[2, 0] = expand0(0)

    def correct0(tc):
        e = expand0(tc)
        for k in range(2):
            v0[2, 2 * tc + k - 1] = v0[1, 2 * tc + k - 1] + e

    loop(1, 5, correct0)
    v0[2, 9] = expand0(5)
    sweep0(2, 3)
    fix0(3, 1)
    halos = swap0(3, 2)
    sweep0(3, 4)
    halos.arrived()
    fix0(4, 2)
    halos = swap0(4, 3)

    def finish(t):
        res_ref[t] = residual0(4, t)
        sol_ref[t] = v0[4, t + 1, z_all, y_all, :]

    loop(0, 8, finish)
    halos.arrived()
    add_halos(res_ref, 3)
    all_sent(0)


def per_device(right_side, mass_field):
    f32 = jnp.float32
    block = jax.ShapeDtypeStruct(right_side.shape, f32)
    vmem = pl.BlockSpec(memory_space=pltpu.VMEM)
    hbm = pl.BlockSpec(memory_space=pltpu.HBM)
    own, ring2, ring3 = (8, 8, 16, 128), (10, 8, 8, 128), (11, 4, 8, 128)
    shapes = [
        own, own, own, own, (5, 10, 10, 32, 128),
        (4, 2, 8, 16, 128), (4, 2, 8, 16, 128), (4, 2, 8, 8, 8, 128),
        (10, 10, 16, 128), (10, 10, 16, 128), (10, 10, 16, 128), (5, 10, 10, 16, 128),
        (3, 4, 2, 8, 128), ring2, ring2, ring2, ring2, ring2, (3, 4, 8, 128), (5, 3, 4, 8, 128),
        (11, 2, 8, 128), ring3, ring3, (4,) + ring3,
        (6, 32, 128), (ROWS, 128),
    ]
    scratch = [pltpu.VMEM(shape, f32) for shape in shapes]
    scratch += [pltpu.SemaphoreType.DMA((count,)) for count in (2, 2, 10)]
    return pl.pallas_call(
        kernel,
        out_shape=(block, block),
        in_specs=[hbm, hbm],
        out_specs=(vmem, vmem),
        scratch_shapes=scratch,
        compiler_params=pltpu.CompilerParams(
            collective_id=0, has_side_effects=True, vmem_limit_bytes=56 * 1024 * 1024
        ),
    )(right_side, mass_field)


def solution(mesh):
    placed = (P("ta", "gz", "gy", None), P("ta", "gz", "gy", None))
    return jax.shard_map(
        per_device, mesh=mesh, in_specs=placed, out_specs=placed, check_vma=False
    )
```

```python
import jax
import jax.numpy as jnp
from jax import lax
from jax.experimental import pallas as pl
from jax.experimental.pallas import tpu as pltpu
from jax.sharding import PartitionSpec as P

DAMPING = 0.7
OFF = 8
GROUP = 2
GROUP1 = 2
ROWS = 8192
MESH = pl.DeviceIdType.MESH


def lanes(like):
    return lax.broadcasted_iota(jnp.int32, like.shape, like.ndim - 1)


def rows(like):
    return lax.broadcasted_iota(jnp.int32, like.shape, like.ndim - 2)


def roll(x, shift, axis):
    return pltpu.roll(x, shift % x.shape[axis], axis)


def ring(x, shift, axis=0):
    shift %= x.shape[axis]
    cut = x.shape[axis] - shift
    return jnp.concatenate(
        [lax.slice_in_dim(x, cut, x.shape[axis], axis=axis), lax.slice_in_dim(x, 0, cut, axis=axis)], axis=axis
    )


def even(index, step):
    return jnp.bitwise_and(index, step) == 0


def partner(x, step, axis):
    index = lax.broadcasted_iota(jnp.int32, x.shape, axis)
    return jnp.where(even(index, step), roll(x, -step, axis), roll(x, step, axis))


def spread(x, step, axis):
    index = lax.broadcasted_iota(jnp.int32, x.shape, axis)
    low = even(index, step)
    return jnp.where(low, x, roll(x, step, axis)), jnp.where(low, roll(x, -step, axis), x)


def pack4(a, b, c, d):
    lane = lanes(a)
    return jnp.where(
        even(lane, 2), jnp.where(even(lane, 1), a, b), jnp.where(even(lane, 1), c, d)
    )


def unpack4(x):
    last = x.ndim - 1
    first, second = spread(x, 1, last)
    a, c = spread(first, 2, last)
    b, d = spread(second, 2, last)
    return a, b, c, d


def kernel(
    s_hbm, m_hbm, sol_ref, res_ref,
    s0, m0, w0, r0, v0_0, v0_1, v0_2, v0_3, v0_4, ht, hz, hy,
    s1, m1, w1, v1_0, v1_1, v1_2, v1_3, v1_4, p2, s2, m2, w2, u2, v2, d2_own, d2_in, d3, w3, v3_0, v3_1, v3_2, v3_3, tmp, bytes_ref,
    load_sem, send_sem, recv_sem,
):
    ta, gz, gy = lax.axis_index("ta"), lax.axis_index("gz"), lax.axis_index("gy")
    nta, ngz, ngy = lax.axis_size("ta"), lax.axis_size("gz"), lax.axis_size("gy")

    v0, v1 = (v0_0, v0_1, v0_2, v0_3, v0_4), (v1_0, v1_1, v1_2, v1_3, v1_4)
    v3 = (v3_0, v3_1, v3_2, v3_3)
    load_m = pltpu.make_async_copy(m_hbm, m0, load_sem.at[0])
    load_s = pltpu.make_async_copy(s_hbm, s0, load_sem.at[1])
    load_m.start()
    load_s.start()

    def device(a, b, c):
        return (
            lax.rem(ta + (a + nta), nta),
            lax.rem(gz + (b + ngz), ngz),
            lax.rem(gy + c, ngy),
        )

    barrier = pltpu.get_barrier_semaphore()
    near = [(a, b, c) for a in (0, 1, -1) for b in range(4) for c in range(2)][1:]
    faces = [(1, 0, 0), (-1, 0, 0), (0, 1, 0), (0, -1, 0), (0, 0, 1)]
    for offset in faces:
        pl.semaphore_signal(barrier, inc=1, device_id=device(*offset), device_id_type=MESH)

    groups = []
    sends = [0, 0]

    class Group:
        def __init__(self, sender=0):
            self.number, self.count, self.sender = len(groups), 0, sender
            groups.append(self)

        def send(self, src, dst, offset):
            size = 1
            for extent in dst.shape[:-1]:
                size *= extent
            self.count += size
            sends[self.sender] += size
            pltpu.make_async_remote_copy(
                src_ref=src,
                dst_ref=dst,
                send_sem=send_sem.at[self.sender],
                recv_sem=recv_sem.at[self.number],
                device_id=device(*offset),
                device_id_type=MESH,
            ).start()

        def arrived(self):
            whole = bytes_ref.at[pl.ds(0, self.count)]
            pltpu.make_async_copy(whole, whole, recv_sem.at[self.number]).wait()

    def all_sent(sender):
        whole = bytes_ref.at[pl.ds(0, sends[sender])]
        pltpu.make_async_copy(whole, whole, send_sem.at[sender]).wait()

    def loop(low, high, body):
        lax.fori_loop(low, high, lambda t, c: (body(t), c)[1], 0)

    t_all, y_all = pl.ds(1, 8), pl.ds(OFF, 16)
    z_all = t_all

    def swap0(slot, n):
        buf = v0[slot]
        group = Group()
        group.send(buf.at[t_all, 8, y_all], hz.at[n, 0], (0, 1, 0))
        group.send(buf.at[t_all, 1, y_all], hz.at[n, 1], (0, -1, 0))
        one = pl.ds(0, 1)
        whole = pl.ds(0, 8)
        group.send(buf.at[t_all, z_all, pl.ds(OFF + 15, 1)], hy.at[n, 0, whole, whole, one], (0, 0, 1))
        group.send(buf.at[t_all, z_all, pl.ds(OFF, 1)], hy.at[n, 1, whole, whole, pl.ds(7, 1)], (0, 0, 1))
        group.send(buf.at[8, z_all, y_all], ht.at[n, 0], (1, 0, 0))
        group.send(buf.at[1, z_all, y_all], ht.at[n, 1], (-1, 0, 0))
        return group

    def around0(slot, t):
        buf = v0[slot]
        here = pl.ds(t + 1, GROUP)
        mid = buf[here, z_all, y_all, :]
        total = roll(mid, 1, 3) + roll(mid, -1, 3)
        total += buf[pl.ds(t, GROUP), z_all, y_all, :] + buf[pl.ds(t + 2, GROUP), z_all, y_all, :]
        total += buf[here, pl.ds(0, 8), y_all, :] + buf[here, pl.ds(2, 8), y_all, :]
        return mid, total + buf[here, z_all, pl.ds(OFF - 1, 16), :] + buf[here, z_all, pl.ds(OFF + 1, 16), :]

    def clear0(slot):
        zero = jnp.zeros((8, 16, 128), jnp.float32)
        v0[slot][0, z_all, y_all, :] = zero
        v0[slot][9, z_all, y_all, :] = zero
        rim = jnp.zeros((8, OFF, 128), jnp.float32)

        def body(t):
            v0[slot][t + 1, 0, y_all, :] = zero[0]
            v0[slot][t + 1, 9, y_all, :] = zero[0]
            v0[slot][t + 1, z_all, pl.ds(0, OFF), :] = rim
            v0[slot][t + 1, z_all, pl.ds(OFF + 16, OFF), :] = rim

        loop(0, 8, body)

    def sweep0(slot, out):
        def body(i):
            t = i * GROUP
            mid, total = around0(slot, t)
            here = pl.ds(t + 1, GROUP)
            old = (1.0 - DAMPING) * mid + v0[0][here, z_all, y_all, :]
            v0[out][here, z_all, y_all, :] = old + w0[pl.ds(t, GROUP)] * total

        loop(0, 8 // GROUP, body)

    def residual0(slot, t):
        mid, total = around0(slot, t)
        return s0[pl.ds(t, GROUP)] - ((8.0 + m0[pl.ds(t, GROUP)]) * mid - total)

    def halo_y(n, t):
        low, high = hy[n, 0, t], hy[n, 1, t]
        low = jnp.where(rows(low) == 0, low, 0.0)
        high = jnp.where(rows(high) == 7, high, 0.0)
        return jnp.concatenate([low, high], axis=1)

    def fix0(out, n):
        def body(t):
            v0[out][t + 1, z_all, y_all, :] = v0[out][t + 1, z_all, y_all, :] + w0[t] * halo_y(n, t)
            for side, z in ((0, 0), (1, 7)):
                v0[out][t + 1, z + 1, y_all, :] = v0[out][t + 1, z + 1, y_all, :] + w0[t, z] * hz[n, side, t]

        loop(0, 8, body)
        for side, t in ((0, 0), (1, 7)):
            v0[out][t + 1, z_all, y_all, :] = v0[out][t + 1, z_all, y_all, :] + w0[t] * ht[n, side]

    def add_halos(ref, n):
        def body(t):
            ref[t] = ref[t] + halo_y(n, t)
            for side, z in ((0, 0), (1, 7)):
                ref[t, z] = ref[t, z] + hz[n, side, t]

        loop(0, 8, body)
        for side, t in ((0, 0), (1, 7)):
            ref[t] = ref[t] + ht[n, side]

    def coarsen_plane(a, step):
        nz, ny, _ = a.shape
        a = a.reshape(nz // 2, 2, ny, 128)
        tmp[0 : nz // 2, 0:ny, :] = a[:, 0] + a[:, 1]
        b = tmp[0 : nz // 2, pl.ds(0, ny // 2, stride=2), :]
        b += tmp[0 : nz // 2, pl.ds(1, ny // 2, stride=2), :]
        return (b + partner(b, step, 2)) * (1.0 / 16.0)

    def swap1(buf, radius, sender=0):
        def span(k, side):
            if side == 0:
                return pl.ds(3, 4), pl.ds(3, 4)
            if side == 1:
                return pl.ds(7 - k, k), pl.ds(3 - k, k)
            return pl.ds(3, k), pl.ds(7, k)

        group = Group(sender)
        offsets = [(a, b, c) for a in (0, 1, -1) for b in (0, 1, -1) for c in (0, 1, -1)][1:]
        for a, b, c in sorted(offsets, key=lambda o: -sum(map(abs, o))):
            k = radius + 1 - abs(a) - abs(b) - abs(c)
            if k < 1:
                continue
            (t_src, t_dst), (z_src, z_dst) = span(k, a), span(k, b)
            y = {0: pl.ds(0, 8), 1: pl.ds(8 - k, k), -1: pl.ds(0, k)}[c]
            y_dst = y if c == 0 else pl.ds(y.start + 8, y.size)
            group.send(buf.at[t_src, z_src, y], buf.at[t_dst, z_dst, y_dst], (a, b, abs(c)))
        return group

    def around1(slot, t, count, radius):
        nz = 4 + 2 * radius
        z = 3 - radius
        buf = v1[slot]
        here = pl.ds(t, count)
        mid = buf[here, pl.ds(z, nz)]
        total = roll(mid, 2, 3) + roll(mid, -2, 3)
        total += buf[pl.ds(t - 1, count), pl.ds(z, nz)] + buf[pl.ds(t + 1, count), pl.ds(z, nz)]
        total += buf[here, pl.ds(z - 1, nz)] + buf[here, pl.ds(z + 1, nz)]
        return mid, total + roll(mid, 1, 2) + roll(mid, -1, 2)

    def sweep1(slot, out, radius):
        z = pl.ds(3 - radius, 4 + 2 * radius)

        def body(i):
            t = 3 - radius + i * GROUP1
            mid, total = around1(slot, t, GROUP1, radius)
            here = pl.ds(t, GROUP1)
            v1[out][here, z] = (1.0 - DAMPING) * mid + v1[0][here, z] + w1[here, z] * total

        loop(0, (4 + 2 * radius) // GROUP1, body)

    def pack2(kind, block):
        p2[1, 0, kind, 0:4, :] = pack4(block[0, 0], block[0, 1], block[1, 0], block[1, 1])

    def gather2():
        whole = pl.ds(0, 2)
        own = p2.at[1, 0, whole, pl.ds(0, 4)]
        group = Group()
        for a, b, c in sorted(near, key=lambda o: -(abs(o[0]) + (0, 1, 2, 1)[o[1]] + 2 * o[2])):
            group.send(own, p2.at[1 - a, (4 - b) % 4, whole, pl.ds(4 * c, 4)], (a, b, c))
        return group

    def unpack2(x, into, at):
        a, b, c, d = unpack4(x)
        into[at] = jnp.stack([a, b], axis=1).reshape(8, 8, 128)
        into[at + 1] = jnp.stack([c, d], axis=1).reshape(8, 8, 128)

    def image(buf, t, count, level):
        mid = buf[pl.ds(t, count)]
        step = 1 << level
        total = roll(mid, step, 3) + roll(mid, -step, 3)
        total += buf[pl.ds(t - 1, count)] + buf[pl.ds(t + 1, count)] + ring(mid, 1, 1) + ring(mid, -1, 1)
        step = level - 1
        return mid, total + roll(mid, step, 2) + roll(mid, -step, 2)

    def sweep_ring(buf, out, first, weight, low, high, level, count):
        def body(i):
            t = low + i * count
            mid, total = image(buf, t, count, level)
            span = pl.ds(t, count)
            out[span] = (1.0 - DAMPING) * mid + first[span] + weight[span] * total

        if high - low == count:
            body(0)
        else:
            loop(0, (high - low) // count, body)

    def coarsen_ring(first, second):
        a = (first + second).reshape(4, 2, 8, 128)
        a = a[:, 0] + a[:, 1]
        a += partner(a, 1, 1)
        return (a + partner(a, 4, 2)) * (1.0 / 16.0)

    def pack3(x):
        row, lane = rows(x[0]), lanes(x[0])
        return jnp.where(
            even(row, 1), jnp.where(even(lane, 1), x[0], x[2]), jnp.where(even(lane, 1), x[1], x[3])
        )

    def unpack3(x):
        first, second = spread(x, 1, 0)
        a, c = spread(first, 1, 1)
        b, d = spread(second, 1, 1)
        return jnp.stack([a, b, c, d])

    load_m.wait()
    load_s.wait()

    def first0(t):
        w = DAMPING / (8.0 + m0[t])
        w0[t] = w
        v0[0][t + 1, z_all, y_all, :] = w * s0[t]

    loop(0, 8, first0)
    pl.semaphore_wait(barrier, len(faces))
    halos = swap0(0, 0)

    def mass1(t):
        m1[t + 3, pl.ds(3, 4), 0:8, :] = coarsen_plane(m0[2 * t] + m0[2 * t + 1], 1)

    loop(0, 4, mass1)
    own1 = pl.ds(3, 4)
    for t in range(2):
        s2[4 + t, 0:2, 0:4, :] = coarsen_plane(
            m1[3 + 2 * t, own1, 0:8, :] + m1[4 + 2 * t, own1, 0:8, :], 2
        )
    pack2(1, s2[4:6, 0:2, 0:4, :])
    for slot in (0, 1, 3, 4):
        clear0(slot)
    sweep0(0, 1)

    halos.arrived()
    fix0(1, 0)
    halos = swap0(1, 1)
    mass1_in = swap1(m1, 2)

    def rest0(i):
        r0[pl.ds(i * GROUP, GROUP)] = residual0(1, i * GROUP)

    loop(0, 8 // GROUP, rest0)
    halos.arrived()
    add_halos(r0, 1)

    def down0(t):
        s1[t + 3, own1, 0:8, :] = coarsen_plane(r0[2 * t] + r0[2 * t + 1], 1)

    loop(0, 4, down0)
    source1_in = swap1(s1, 2)
    mass1_in.arrived()
    z_two = pl.ds(1, 8)

    def weight1(t):
        w1[t, z_two] = 0.5 * DAMPING / (4.0 + m1[t, z_two])

    loop(1, 9, weight1)
    source1_in.arrived()

    def first1(t):
        v1[0][t, z_two] = 2.0 * w1[t, z_two] * s1[t, z_two]

    loop(1, 9, first1)
    sweep1(0, 1, 1)

    mid, total = around1(1, 3, 4, 0)
    mid, total = mid[:, :, 0:8], total[:, :, 0:8]
    d = 4.0 + m1[own1, own1, 0:8, :]
    r0[0:4, 0:4, 0:8, :] = s1[own1, own1, 0:8, :] - (d * mid - 0.5 * total)
    for t in range(2):
        s2[4 + t, 0:2, 0:4, :] = coarsen_plane(r0[2 * t, 0:4, 0:8, :] + r0[2 * t + 1, 0:4, 0:8, :], 2)
    pack2(0, s2[4:6, 0:2, 0:4, :])
    source2_in = gather2()
    for t in range(3, 7):
        v1[2][t, own1, 0:8, :] = v1[1][t, own1, 0:8, :]
    halo1_in = swap1(v1[2], 3, 1)
    source2_in.arrived()

    def first2(t):
        unpack2(p2[t, :, 0], s2, 2 + 2 * t)
        unpack2(p2[t, :, 1], m2, 2 + 2 * t)
        span = pl.ds(2 + 2 * t, 2)
        w = 0.25 * DAMPING / (2.0 + m2[span])
        w2[span] = w
        u2[span] = 4.0 * w * s2[span]

    loop(0, 3, first2)
    sweep_ring(u2, v2, u2, w2, 3, 7, 2, 4)
    mid, total = image(v2, 4, 2, 2)
    remainder = s2[4:6] - ((2.0 + m2[4:6]) * mid - 0.25 * total)
    d3[5, 0] = pack3(coarsen_ring(remainder[0], remainder[1]))
    d3[5, 1] = pack3(coarsen_ring(m2[4], m2[5]))
    planes_in = Group()
    for k in range(5, 0, -1):
        for a in (k, -k):
            planes_in.send(d3.at[5], d3.at[5 - a], (a, 0, 0))
    d2_own[0] = p2[1, :, 0]
    d2_own[1] = p2[1, :, 1]
    pairs = v2[4:6].reshape(2, 4, 2, 8, 128)
    d2_own[2] = pack4(pairs[0, :, 0], pairs[0, :, 1], pairs[1, :, 0], pairs[1, :, 1])
    halo2_in = Group()
    for a in (1, -1, 2, -2):
        halo2_in.send(d2_own, d2_in.at[2 - a], (a, 0, 0))
    planes_in.arrived()

    def first3(t):
        w = 0.125 * DAMPING / (1.0 + unpack3(d3[t, 1]))
        w3[t] = w
        v3[0][t] = 8.0 * w * unpack3(d3[t, 0])

    loop(0, 11, first3)
    for step in range(3):
        sweep_ring(v3[step], v3[step + 1], v3[0], w3, 1 + step, 10 - step, 3, 9 - 2 * step)

    halo2_in.arrived()
    for k, at in ((0, 0), (4, 8)):
        unpack2(d2_in[k, 0], s2, at)
        unpack2(d2_in[k, 1], m2, at)
    for k, at in ((0, 0), (1, 2), (3, 6), (4, 8)):
        unpack2(d2_in[k, 2], v2, at)
    for at in (0, 8):
        w = 0.25 * DAMPING / (2.0 + m2[at : at + 2])
        w2[at : at + 2] = w
        u2[at : at + 2] = 4.0 * w * s2[at : at + 2]

    def correct2(t):
        e = v3[3][3 + t]
        e = jnp.broadcast_to(e[:, None], (4, 2, 8, 128)).reshape(8, 8, 128)
        for k in range(2):
            v2[2 * t + k] = v2[2 * t + k] + e

    loop(0, 5, correct2)
    sweep_ring(v2, s2, u2, w2, 1, 9, 2, 4)
    sweep_ring(s2, v2, u2, w2, 2, 8, 2, 3)

    halo1_in.arrived()
    all_sent(1)

    def expand1(tc):
        for z in range(6):
            e = v2[2 + tc, (z - 2) % 8]
            tmp[z, pl.ds(0, 8, stride=2), :] = e
            tmp[z, pl.ds(1, 8, stride=2), :] = e
        e = tmp[0:6, 0:16, :]
        return jnp.broadcast_to(e[:, None], (6, 2, 16, 128)).reshape(12, 16, 128)[1:11]

    e = expand1(0)
    v1[2][0] = v1[2][0] + e

    def correct1(tc):
        e = expand1(tc)
        for k in range(2):
            v1[2][2 * tc + k - 1] = v1[2][2 * tc + k - 1] + e

    loop(1, 5, correct1)
    e = expand1(5)
    v1[2][9] = v1[2][9] + e
    sweep1(2, 3, 2)
    sweep1(3, 4, 1)

    def expand0(tc):
        e = v1[4][2 + tc, pl.ds(2, 6)]
        tmp[0:6, pl.ds(OFF, 8, stride=2), :] = e[:, 0:8]
        tmp[0:6, pl.ds(OFF + 1, 8, stride=2), :] = e[:, 0:8]
        tmp[0:6, OFF - 1 : OFF, :] = e[:, 15:16]
        tmp[0:6, OFF + 16 : OFF + 17, :] = e[:, 8:9]
        e = tmp[...]
        return jnp.broadcast_to(e[:, None], (6, 2, 32, 128)).reshape(12, 32, 128)[1:11]

    v0[2][0] = expand0(0)

    def correct0(tc):
        e = expand0(tc)
        for k in range(2):
            v0[2][2 * tc + k - 1] = v0[1][2 * tc + k - 1] + e

    loop(1, 5, correct0)
    v0[2][9] = expand0(5)
    sweep0(2, 3)
    fix0(3, 1)
    halos = swap0(3, 2)
    sweep0(3, 4)
    halos.arrived()
    fix0(4, 2)
    halos = swap0(4, 3)

    def finish(i):
        here = pl.ds(i * GROUP, GROUP)
        res_ref[here] = residual0(4, i * GROUP)
        sol_ref[here] = v0[4][pl.ds(i * GROUP + 1, GROUP), z_all, y_all, :]

    loop(0, 8 // GROUP, finish)
    halos.arrived()
    add_halos(res_ref, 3)
    all_sent(0)


def per_device(right_side, mass_field):
    f32 = jnp.float32
    block = jax.ShapeDtypeStruct(right_side.shape, f32)
    vmem = pl.BlockSpec(memory_space=pltpu.VMEM)
    hbm = pl.BlockSpec(memory_space=pltpu.HBM)
    own, ring2, ring3 = (8, 8, 16, 128), (10, 8, 8, 128), (11, 4, 8, 128)
    shapes = [
        own, own, own, own, *[(10, 10, 32, 128)] * 5,
        (4, 2, 8, 16, 128), (4, 2, 8, 16, 128), (4, 2, 8, 8, 8, 128),
        *[(10, 10, 16, 128)] * 8,
        (3, 4, 2, 8, 128), ring2, ring2, ring2, ring2, ring2, (3, 4, 8, 128), (5, 3, 4, 8, 128),
        (11, 2, 8, 128), *[ring3] * 5,
        (6, 32, 128), (ROWS, 128),
    ]
    scratch = [pltpu.VMEM(shape, f32) for shape in shapes]
    scratch += [pltpu.SemaphoreType.DMA((count,)) for count in (2, 2, 10)]
    return pl.pallas_call(
        kernel,
        out_shape=(block, block),
        in_specs=[hbm, hbm],
        out_specs=(vmem, vmem),
        scratch_shapes=scratch,
        compiler_params=pltpu.CompilerParams(
            collective_id=0, has_side_effects=True, vmem_limit_bytes=56 * 1024 * 1024
        ),
    )(right_side, mass_field)


def solution(mesh):
    placed = (P("ta", "gz", "gy", None), P("ta", "gz", "gy", None))
    return jax.shard_map(
        per_device, mesh=mesh, in_specs=placed, out_specs=placed, check_vma=False
    )
```

```python
import jax
import jax.numpy as jnp
from jax import lax
from jax.experimental import pallas as pl
from jax.experimental.pallas import tpu as pltpu
from jax.sharding import PartitionSpec as P

DAMPING = 0.7
OFF = 8
GROUP = 2
GROUP1 = 2
ROWS = 8192
MESH = pl.DeviceIdType.MESH


def lanes(like):
    return lax.broadcasted_iota(jnp.int32, like.shape, like.ndim - 1)


def rows(like):
    return lax.broadcasted_iota(jnp.int32, like.shape, like.ndim - 2)


def roll(x, shift, axis):
    return pltpu.roll(x, shift % x.shape[axis], axis)


def ring(x, shift, axis=0):
    shift %= x.shape[axis]
    cut = x.shape[axis] - shift
    return jnp.concatenate(
        [lax.slice_in_dim(x, cut, x.shape[axis], axis=axis), lax.slice_in_dim(x, 0, cut, axis=axis)], axis=axis
    )


def even(index, step):
    return jnp.bitwise_and(index, step) == 0


def partner(x, step, axis):
    index = lax.broadcasted_iota(jnp.int32, x.shape, axis)
    return jnp.where(even(index, step), roll(x, -step, axis), roll(x, step, axis))


def spread(x, step, axis):
    index = lax.broadcasted_iota(jnp.int32, x.shape, axis)
    low = even(index, step)
    return jnp.where(low, x, roll(x, step, axis)), jnp.where(low, roll(x, -step, axis), x)


def pack4(a, b, c, d):
    lane = lanes(a)
    return jnp.where(
        even(lane, 2), jnp.where(even(lane, 1), a, b), jnp.where(even(lane, 1), c, d)
    )


def unpack4(x):
    last = x.ndim - 1
    first, second = spread(x, 1, last)
    a, c = spread(first, 2, last)
    b, d = spread(second, 2, last)
    return a, b, c, d


def kernel(
    s_hbm, m_hbm, sol_ref, res_ref,
    s0, m0, w0, r0, v0_0, v0_1, v0_2, v0_3, v0_4, ht, hz, hy,
    s1, m1, w1, m2_own, v1_0, v1_1, v1_2, v1_3, v1_4, p2, s2, m2, w2, u2, v2, d2_own, d2_in, d3, w3, v3_0, v3_1, v3_2, v3_3, tmp, pairs, bytes_ref,
    load_sem, send_sem, recv_sem,
):
    ta, gz, gy = lax.axis_index("ta"), lax.axis_index("gz"), lax.axis_index("gy")
    nta, ngz, ngy = lax.axis_size("ta"), lax.axis_size("gz"), lax.axis_size("gy")

    v0, v1 = (v0_0, v0_1, v0_2, v0_3, v0_4), (v1_0, v1_1, v1_2, v1_3, v1_4)
    v3 = (v3_0, v3_1, v3_2, v3_3)
    load_m = pltpu.make_async_copy(m_hbm, m0, load_sem.at[0])
    load_s = pltpu.make_async_copy(s_hbm, s0, load_sem.at[1])
    load_m.start()
    load_s.start()

    def device(a, b, c):
        return (
            lax.rem(ta + (a + nta), nta),
            lax.rem(gz + (b + ngz), ngz),
            lax.rem(gy + c, ngy),
        )

    barrier = pltpu.get_barrier_semaphore()
    near = [(a, b, c) for a in (0, 1, -1) for b in range(4) for c in range(2)][1:]
    faces = [(1, 0, 0), (-1, 0, 0), (0, 1, 0), (0, -1, 0), (0, 0, 1)]
    for offset in faces:
        pl.semaphore_signal(barrier, inc=1, device_id=device(*offset), device_id_type=MESH)

    groups = []
    sends = [0, 0]

    class Group:
        def __init__(self, sender=0):
            self.number, self.count, self.sender = len(groups), 0, sender
            groups.append(self)

        def send(self, src, dst, offset):
            size = 1
            for extent in dst.shape[:-1]:
                size *= extent
            self.count += size
            sends[self.sender] += size
            pltpu.make_async_remote_copy(
                src_ref=src,
                dst_ref=dst,
                send_sem=send_sem.at[self.sender],
                recv_sem=recv_sem.at[self.number],
                device_id=device(*offset),
                device_id_type=MESH,
            ).start()

        def arrived(self):
            whole = bytes_ref.at[pl.ds(0, self.count)]
            pltpu.make_async_copy(whole, whole, recv_sem.at[self.number]).wait()

    def all_sent(sender):
        whole = bytes_ref.at[pl.ds(0, sends[sender])]
        pltpu.make_async_copy(whole, whole, send_sem.at[sender]).wait()

    def loop(low, high, body):
        lax.fori_loop(low, high, lambda t, c: (body(t), c)[1], 0)

    t_all, y_all = pl.ds(1, 8), pl.ds(OFF, 16)
    z_all = t_all

    def swap0(slot, n):
        buf = v0[slot]
        group = Group()
        group.send(buf.at[t_all, 8, y_all], hz.at[n, 0], (0, 1, 0))
        group.send(buf.at[t_all, 1, y_all], hz.at[n, 1], (0, -1, 0))
        one = pl.ds(0, 1)
        whole = pl.ds(0, 8)
        group.send(buf.at[t_all, z_all, pl.ds(OFF + 15, 1)], hy.at[n, 0, whole, whole, one], (0, 0, 1))
        group.send(buf.at[t_all, z_all, pl.ds(OFF, 1)], hy.at[n, 1, whole, whole, pl.ds(7, 1)], (0, 0, 1))
        group.send(buf.at[8, z_all, y_all], ht.at[n, 0], (1, 0, 0))
        group.send(buf.at[1, z_all, y_all], ht.at[n, 1], (-1, 0, 0))
        return group

    def around0(slot, t):
        buf = v0[slot]
        here = pl.ds(t + 1, GROUP)
        mid = buf[here, z_all, y_all, :]
        total = roll(mid, 1, 3) + roll(mid, -1, 3)
        total += buf[pl.ds(t, GROUP), z_all, y_all, :] + buf[pl.ds(t + 2, GROUP), z_all, y_all, :]
        total += buf[here, pl.ds(0, 8), y_all, :] + buf[here, pl.ds(2, 8), y_all, :]
        return mid, total + buf[here, z_all, pl.ds(OFF - 1, 16), :] + buf[here, z_all, pl.ds(OFF + 1, 16), :]

    def clear0(slot):
        zero = jnp.zeros((8, 16, 128), jnp.float32)
        v0[slot][0, z_all, y_all, :] = zero
        v0[slot][9, z_all, y_all, :] = zero
        rim = jnp.zeros((8, OFF, 128), jnp.float32)

        def body(t):
            v0[slot][t + 1, 0, y_all, :] = zero[0]
            v0[slot][t + 1, 9, y_all, :] = zero[0]
            v0[slot][t + 1, z_all, pl.ds(0, OFF), :] = rim
            v0[slot][t + 1, z_all, pl.ds(OFF + 16, OFF), :] = rim

        loop(0, 8, body)

    def sweep0(slot, out):
        def body(i):
            t = i * GROUP
            mid, total = around0(slot, t)
            here = pl.ds(t + 1, GROUP)
            old = (1.0 - DAMPING) * mid + v0[0][here, z_all, y_all, :]
            v0[out][here, z_all, y_all, :] = old + w0[pl.ds(t, GROUP)] * total

        loop(0, 8 // GROUP, body)

    def residual0(slot, t):
        mid, total = around0(slot, t)
        return s0[pl.ds(t, GROUP)] - ((8.0 + m0[pl.ds(t, GROUP)]) * mid - total)

    def halo_y(n, t):
        low, high = hy[n, 0, t], hy[n, 1, t]
        low = jnp.where(rows(low) == 0, low, 0.0)
        high = jnp.where(rows(high) == 7, high, 0.0)
        return jnp.concatenate([low, high], axis=1)

    def fix0(out, n):
        def body(t):
            v0[out][t + 1, z_all, y_all, :] = v0[out][t + 1, z_all, y_all, :] + w0[t] * halo_y(n, t)
            for side, z in ((0, 0), (1, 7)):
                v0[out][t + 1, z + 1, y_all, :] = v0[out][t + 1, z + 1, y_all, :] + w0[t, z] * hz[n, side, t]

        loop(0, 8, body)
        for side, t in ((0, 0), (1, 7)):
            v0[out][t + 1, z_all, y_all, :] = v0[out][t + 1, z_all, y_all, :] + w0[t] * ht[n, side]

    def add_halos(ref, n):
        def body(t):
            ref[t] = ref[t] + halo_y(n, t)
            for side, z in ((0, 0), (1, 7)):
                ref[t, z] = ref[t, z] + hz[n, side, t]

        loop(0, 8, body)
        for side, t in ((0, 0), (1, 7)):
            ref[t] = ref[t] + ht[n, side]

    def coarsen(a, step):
        nt, nz, ny, _ = a.shape
        a = a.reshape(nt // 2, 2, nz // 2, 2, ny, 128)
        a = a[:, 0] + a[:, 1]
        t, z = slice(0, nt // 2), slice(0, nz // 2)
        pairs[t, z, 0:ny, :] = a[:, :, 0] + a[:, :, 1]
        b = pairs[t, z, pl.ds(0, ny // 2, stride=2), :]
        b += pairs[t, z, pl.ds(1, ny // 2, stride=2), :]
        return (b + partner(b, step, 3)) * (1.0 / 16.0)

    def swap1(buf, radius, sender=0):
        def span(k, side):
            if side == 0:
                return pl.ds(3, 4), pl.ds(3, 4)
            if side == 1:
                return pl.ds(7 - k, k), pl.ds(3 - k, k)
            return pl.ds(3, k), pl.ds(7, k)

        group = Group(sender)
        offsets = [(a, b, c) for a in (0, 1, -1) for b in (0, 1, -1) for c in (0, 1, -1)][1:]
        for a, b, c in sorted(offsets, key=lambda o: -sum(map(abs, o))):
            k = radius + 1 - abs(a) - abs(b) - abs(c)
            if k < 1:
                continue
            (t_src, t_dst), (z_src, z_dst) = span(k, a), span(k, b)
            y = {0: pl.ds(0, 8), 1: pl.ds(8 - k, k), -1: pl.ds(0, k)}[c]
            y_dst = y if c == 0 else pl.ds(y.start + 8, y.size)
            group.send(buf.at[t_src, z_src, y], buf.at[t_dst, z_dst, y_dst], (a, b, abs(c)))
        return group

    def around1(slot, t, count, radius):
        nz = 4 + 2 * radius
        z = 3 - radius
        buf = v1[slot]
        here = pl.ds(t, count)
        mid = buf[here, pl.ds(z, nz)]
        total = roll(mid, 2, 3) + roll(mid, -2, 3)
        total += buf[pl.ds(t - 1, count), pl.ds(z, nz)] + buf[pl.ds(t + 1, count), pl.ds(z, nz)]
        total += buf[here, pl.ds(z - 1, nz)] + buf[here, pl.ds(z + 1, nz)]
        return mid, total + roll(mid, 1, 2) + roll(mid, -1, 2)

    def sweep1(slot, out, radius):
        z = pl.ds(3 - radius, 4 + 2 * radius)

        def body(i):
            t = 3 - radius + i * GROUP1
            mid, total = around1(slot, t, GROUP1, radius)
            here = pl.ds(t, GROUP1)
            v1[out][here, z] = (1.0 - DAMPING) * mid + v1[0][here, z] + w1[here, z] * total

        loop(0, (4 + 2 * radius) // GROUP1, body)

    def pack2(kind, block):
        p2[1, 0, kind, 0:4, :] = pack4(block[0, 0], block[0, 1], block[1, 0], block[1, 1])

    def gather2():
        whole = pl.ds(0, 2)
        own = p2.at[1, 0, whole, pl.ds(0, 4)]
        group = Group()
        for a, b, c in sorted(near, key=lambda o: -(abs(o[0]) + (0, 1, 2, 1)[o[1]] + 2 * o[2])):
            group.send(own, p2.at[1 - a, (4 - b) % 4, whole, pl.ds(4 * c, 4)], (a, b, c))
        return group

    def unpack2(x, into, at):
        a, b, c, d = unpack4(x)
        into[at] = jnp.stack([a, b], axis=1).reshape(8, 8, 128)
        into[at + 1] = jnp.stack([c, d], axis=1).reshape(8, 8, 128)

    def image(buf, t, count, level):
        mid = buf[pl.ds(t, count)]
        step = 1 << level
        total = roll(mid, step, 3) + roll(mid, -step, 3)
        total += buf[pl.ds(t - 1, count)] + buf[pl.ds(t + 1, count)] + ring(mid, 1, 1) + ring(mid, -1, 1)
        step = level - 1
        return mid, total + roll(mid, step, 2) + roll(mid, -step, 2)

    def sweep_ring(buf, out, first, weight, low, high, level, count):
        def body(i):
            t = low + i * count
            mid, total = image(buf, t, count, level)
            span = pl.ds(t, count)
            out[span] = (1.0 - DAMPING) * mid + first[span] + weight[span] * total

        if high - low == count:
            body(0)
        else:
            loop(0, (high - low) // count, body)

    def coarsen_ring(first, second):
        a = (first + second).reshape(4, 2, 8, 128)
        a = a[:, 0] + a[:, 1]
        a += partner(a, 1, 1)
        return (a + partner(a, 4, 2)) * (1.0 / 16.0)

    def pack3(x):
        row, lane = rows(x[0]), lanes(x[0])
        return jnp.where(
            even(row, 1), jnp.where(even(lane, 1), x[0], x[2]), jnp.where(even(lane, 1), x[1], x[3])
        )

    def unpack3(x):
        first, second = spread(x, 1, 0)
        a, c = spread(first, 1, 1)
        b, d = spread(second, 1, 1)
        return jnp.stack([a, b, c, d])

    load_m.wait()
    load_s.wait()

    def first0(t):
        w = DAMPING / (8.0 + m0[t])
        w0[t] = w
        v0[0][t + 1, z_all, y_all, :] = w * s0[t]

    loop(0, 8, first0)
    pl.semaphore_wait(barrier, len(faces))
    halos = swap0(0, 0)

    own1 = pl.ds(3, 4)
    m1[own1, own1, 0:8, :] = coarsen(m0[...], 1)
    m2_own[...] = coarsen(m1[own1, own1, 0:8, :], 2)
    pack2(1, m2_own[...])
    for slot in (0, 1, 3, 4):
        clear0(slot)
    sweep0(0, 1)

    halos.arrived()
    fix0(1, 0)
    halos = swap0(1, 1)
    mass1_in = swap1(m1, 2)

    def rest0(i):
        r0[pl.ds(i * GROUP, GROUP)] = residual0(1, i * GROUP)

    loop(0, 8 // GROUP, rest0)
    halos.arrived()
    add_halos(r0, 1)

    s1[...] = coarsen(r0[...], 1)
    d1 = 4.0 + m1[own1, own1, 0:8, :]
    v1[0][own1, own1, 0:8, :] = DAMPING * s1[...] / d1
    first1_in = swap1(v1[0], 2)
    mass1_in.arrived()
    z_two = pl.ds(1, 8)

    def weight1(t):
        w1[t, z_two] = 0.5 * DAMPING / (4.0 + m1[t, z_two])

    loop(1, 9, weight1)
    first1_in.arrived()
    sweep1(0, 1, 1)

    mid, total = around1(1, 3, 4, 0)
    mid, total = mid[:, :, 0:8], total[:, :, 0:8]
    d = 4.0 + m1[own1, own1, 0:8, :]
    source2 = coarsen(s1[...] - (d * mid - 0.5 * total), 2)
    pack2(0, DAMPING * source2 / (2.0 + m2_own[...]))
    source2_in = gather2()
    for t in range(3, 7):
        v1[2][t, own1, 0:8, :] = v1[1][t, own1, 0:8, :]
    halo1_in = swap1(v1[2], 3, 1)
    source2_in.arrived()

    def first2(t):
        unpack2(p2[t, :, 0], u2, 2 + 2 * t)
        unpack2(p2[t, :, 1], m2, 2 + 2 * t)
        span = pl.ds(2 + 2 * t, 2)
        w2[span] = 0.25 * DAMPING / (2.0 + m2[span])

    for t in range(3):
        first2(t)
    sweep_ring(u2, v2, u2, w2, 3, 7, 2, 4)
    mid, total = image(v2, 4, 2, 2)
    remainder = (2.0 + m2[4:6]) * (u2[4:6] * (1.0 / DAMPING) - mid) + 0.25 * total
    weight3 = DAMPING / (1.0 + coarsen_ring(m2[4], m2[5]))
    d3[5, 0] = pack3(weight3 * coarsen_ring(remainder[0], remainder[1]))
    d3[5, 1] = pack3(0.125 * weight3)
    planes_in = Group()
    for k in range(5, 0, -1):
        for a in (k, -k):
            planes_in.send(d3.at[5], d3.at[5 - a], (a, 0, 0))
    d2_own[0] = p2[1, :, 0]
    for k, field in ((1, w2), (2, v2)):
        halves = field[4:6].reshape(2, 4, 2, 8, 128)
        d2_own[k] = pack4(halves[0, :, 0], halves[0, :, 1], halves[1, :, 0], halves[1, :, 1])
    halo2_in = Group()
    for a in (1, -1, 2, -2):
        halo2_in.send(d2_own, d2_in.at[2 - a], (a, 0, 0))
    halo2_in.arrived()
    for k, at in ((0, 0), (4, 8)):
        unpack2(d2_in[k, 0], u2, at)
        unpack2(d2_in[k, 1], w2, at)
    for k, at in ((0, 0), (1, 2), (3, 6), (4, 8)):
        unpack2(d2_in[k, 2], v2, at)

    planes_in.arrived()

    for t in range(11):
        v3[0][t] = unpack3(d3[t, 0])
        w3[t] = unpack3(d3[t, 1])
    for step in range(3):
        sweep_ring(v3[step], v3[step + 1], v3[0], w3, 1 + step, 10 - step, 3, 9 - 2 * step)

    def correct2(t):
        e = v3[3][3 + t]
        e = jnp.broadcast_to(e[:, None], (4, 2, 8, 128)).reshape(8, 8, 128)
        for k in range(2):
            v2[2 * t + k] = v2[2 * t + k] + e

    loop(0, 5, correct2)
    sweep_ring(v2, s2, u2, w2, 1, 9, 2, 4)
    sweep_ring(s2, v2, u2, w2, 2, 8, 2, 3)

    halo1_in.arrived()
    all_sent(1)

    def expand1(tc):
        for z in range(6):
            e = v2[2 + tc, (z - 2) % 8]
            tmp[z, pl.ds(0, 8, stride=2), :] = e
            tmp[z, pl.ds(1, 8, stride=2), :] = e
        e = tmp[0:6, 0:16, :]
        return jnp.broadcast_to(e[:, None], (6, 2, 16, 128)).reshape(12, 16, 128)[1:11]

    e = expand1(0)
    v1[2][0] = v1[2][0] + e

    def correct1(tc):
        e = expand1(tc)
        for k in range(2):
            v1[2][2 * tc + k - 1] = v1[2][2 * tc + k - 1] + e

    loop(1, 5, correct1)
    e = expand1(5)
    v1[2][9] = v1[2][9] + e
    sweep1(2, 3, 2)
    sweep1(3, 4, 1)

    def expand0(tc):
        e = v1[4][2 + tc, pl.ds(2, 6)]
        tmp[0:6, pl.ds(OFF, 8, stride=2), :] = e[:, 0:8]
        tmp[0:6, pl.ds(OFF + 1, 8, stride=2), :] = e[:, 0:8]
        tmp[0:6, OFF - 1 : OFF, :] = e[:, 15:16]
        tmp[0:6, OFF + 16 : OFF + 17, :] = e[:, 8:9]
        e = tmp[...]
        return jnp.broadcast_to(e[:, None], (6, 2, 32, 128)).reshape(12, 32, 128)[1:11]

    v0[2][0] = expand0(0)

    def correct0(tc):
        e = expand0(tc)
        for k in range(2):
            v0[2][2 * tc + k - 1] = v0[1][2 * tc + k - 1] + e

    loop(1, 5, correct0)
    v0[2][9] = expand0(5)
    sweep0(2, 3)
    fix0(3, 1)
    halos = swap0(3, 2)
    sweep0(3, 4)
    halos.arrived()
    fix0(4, 2)
    halos = swap0(4, 3)

    def finish(i):
        here = pl.ds(i * GROUP, GROUP)
        res_ref[here] = residual0(4, i * GROUP)
        sol_ref[here] = v0[4][pl.ds(i * GROUP + 1, GROUP), z_all, y_all, :]

    loop(0, 8 // GROUP, finish)
    halos.arrived()
    add_halos(res_ref, 3)
    all_sent(0)


def per_device(right_side, mass_field):
    f32 = jnp.float32
    block = jax.ShapeDtypeStruct(right_side.shape, f32)
    vmem = pl.BlockSpec(memory_space=pltpu.VMEM)
    hbm = pl.BlockSpec(memory_space=pltpu.HBM)
    own, ring2, ring3 = (8, 8, 16, 128), (10, 8, 8, 128), (11, 4, 8, 128)
    shapes = [
        own, own, own, own, *[(10, 10, 32, 128)] * 5,
        (4, 2, 8, 16, 128), (4, 2, 8, 16, 128), (4, 2, 8, 8, 8, 128),
        (4, 4, 8, 128), *[(10, 10, 16, 128)] * 2, (2, 2, 4, 128), *[(10, 10, 16, 128)] * 5,
        (3, 4, 2, 8, 128), ring2, ring2, ring2, ring2, ring2, (3, 4, 8, 128), (5, 3, 4, 8, 128),
        (11, 2, 8, 128), *[ring3] * 5,
        (6, 32, 128), (4, 4, 16, 128), (ROWS, 128),
    ]
    scratch = [pltpu.VMEM(shape, f32) for shape in shapes]
    scratch += [pltpu.SemaphoreType.DMA((count,)) for count in (2, 2, 10)]
    return pl.pallas_call(
        kernel,
        out_shape=(block, block),
        in_specs=[hbm, hbm],
        out_specs=(vmem, vmem),
        scratch_shapes=scratch,
        compiler_params=pltpu.CompilerParams(
            collective_id=0, has_side_effects=True, vmem_limit_bytes=56 * 1024 * 1024
        ),
    )(right_side, mass_field)


def solution(mesh):
    placed = (P("ta", "gz", "gy", None), P("ta", "gz", "gy", None))
    return jax.shard_map(
        per_device, mesh=mesh, in_specs=placed, out_specs=placed, check_vma=False
    )
```

```python
import jax
import jax.numpy as jnp
from jax import lax
from jax.experimental import pallas as pl
from jax.experimental.pallas import tpu as pltpu
from jax.sharding import PartitionSpec as P

DAMPING = 0.7
OFF = 8
GROUP = 2
GROUP1 = 2
ROWS = 8192
MESH = pl.DeviceIdType.MESH


def lanes(like):
    return lax.broadcasted_iota(jnp.int32, like.shape, like.ndim - 1)


def rows(like):
    return lax.broadcasted_iota(jnp.int32, like.shape, like.ndim - 2)


def roll(x, shift, axis):
    return pltpu.roll(x, shift % x.shape[axis], axis)


def ring(x, shift, axis=0):
    shift %= x.shape[axis]
    cut = x.shape[axis] - shift
    return jnp.concatenate(
        [lax.slice_in_dim(x, cut, x.shape[axis], axis=axis), lax.slice_in_dim(x, 0, cut, axis=axis)], axis=axis
    )


def even(index, step):
    return jnp.bitwise_and(index, step) == 0


def partner(x, step, axis):
    index = lax.broadcasted_iota(jnp.int32, x.shape, axis)
    return jnp.where(even(index, step), roll(x, -step, axis), roll(x, step, axis))


def spread(x, step, axis):
    index = lax.broadcasted_iota(jnp.int32, x.shape, axis)
    low = even(index, step)
    return jnp.where(low, x, roll(x, step, axis)), jnp.where(low, roll(x, -step, axis), x)


def pack4(a, b, c, d):
    lane = lanes(a)
    return jnp.where(
        even(lane, 2), jnp.where(even(lane, 1), a, b), jnp.where(even(lane, 1), c, d)
    )


def unpack4(x):
    last = x.ndim - 1
    first, second = spread(x, 1, last)
    a, c = spread(first, 2, last)
    b, d = spread(second, 2, last)
    return a, b, c, d


def kernel(
    s_hbm, m_hbm, sol_ref, res_ref,
    s0, m0, w0, r0, v0_0, v0_1, v0_2, v0_3, v0_4, ht, hz, hy, wt, wz, wy,
    s1, m1, w1, weight_1, m2_own, v1_0, v1_1, v1_2, v1_3, v1_4, p2, s2, m2, w2, u2, v2, d2_own, d2_in, d3, w3, v3_0, v3_1, v3_2, v3_3, tmp, pairs, bytes_ref,
    load_sem, send_sem, recv_sem,
):
    ta, gz, gy = lax.axis_index("ta"), lax.axis_index("gz"), lax.axis_index("gy")
    nta, ngz, ngy = lax.axis_size("ta"), lax.axis_size("gz"), lax.axis_size("gy")

    v0, v1 = (v0_0, v0_1, v0_2, v0_3, v0_4), (v1_0, v1_1, v1_2, v1_3, v1_4)
    v3 = (v3_0, v3_1, v3_2, v3_3)
    load_m = pltpu.make_async_copy(m_hbm, m0, load_sem.at[0])
    load_s = pltpu.make_async_copy(s_hbm, s0, load_sem.at[1])
    load_m.start()
    load_s.start()

    def device(a, b, c):
        return (
            lax.rem(ta + (a + nta), nta),
            lax.rem(gz + (b + ngz), ngz),
            lax.rem(gy + c, ngy),
        )

    barrier = pltpu.get_barrier_semaphore()
    near = [(a, b, c) for a in (0, 1, -1) for b in range(4) for c in range(2)][1:]
    faces = [(1, 0, 0), (-1, 0, 0), (0, 1, 0), (0, -1, 0), (0, 0, 1)]
    for offset in faces:
        pl.semaphore_signal(barrier, inc=1, device_id=device(*offset), device_id_type=MESH)

    groups = []
    sends = [0, 0, 0]

    class Group:
        def __init__(self, sender=0):
            self.number, self.count, self.sender = len(groups), 0, sender
            groups.append(self)

        def send(self, src, dst, offset):
            size = 1
            for extent in dst.shape[:-1]:
                size *= extent
            self.count += size
            sends[self.sender] += size
            pltpu.make_async_remote_copy(
                src_ref=src,
                dst_ref=dst,
                send_sem=send_sem.at[self.sender],
                recv_sem=recv_sem.at[self.number],
                device_id=device(*offset),
                device_id_type=MESH,
            ).start()

        def arrived(self):
            whole = bytes_ref.at[pl.ds(0, self.count)]
            pltpu.make_async_copy(whole, whole, recv_sem.at[self.number]).wait()

    def all_sent(sender):
        whole = bytes_ref.at[pl.ds(0, sends[sender])]
        pltpu.make_async_copy(whole, whole, send_sem.at[sender]).wait()

    def loop(low, high, body):
        lax.fori_loop(low, high, lambda t, c: (body(t), c)[1], 0)

    t_all, y_all = pl.ds(1, 8), pl.ds(OFF, 16)
    z_all = t_all

    def swap0(slot, n, sender=0):
        buf = v0[slot]
        group = Group(sender)
        group.send(buf.at[t_all, 8, y_all], hz.at[n, 0], (0, 1, 0))
        group.send(buf.at[t_all, 1, y_all], hz.at[n, 1], (0, -1, 0))
        one = pl.ds(0, 1)
        whole = pl.ds(0, 8)
        group.send(buf.at[t_all, z_all, pl.ds(OFF + 15, 1)], hy.at[n, whole, whole, pl.ds(7, 1)], (0, 0, 1))
        group.send(buf.at[t_all, z_all, pl.ds(OFF, 1)], hy.at[n, whole, whole, one], (0, 0, 1))
        group.send(buf.at[8, z_all, y_all], ht.at[n, 0], (1, 0, 0))
        group.send(buf.at[1, z_all, y_all], ht.at[n, 1], (-1, 0, 0))
        return group

    def swap_weights():
        group = Group()
        whole = pl.ds(0, 8)
        group.send(w0.at[whole, 7], wz.at[0], (0, 1, 0))
        group.send(w0.at[whole, 0], wz.at[1], (0, -1, 0))
        group.send(w0.at[whole, whole, pl.ds(15, 1)], wy.at[whole, whole, pl.ds(7, 1)], (0, 0, 1))
        group.send(w0.at[whole, whole, pl.ds(0, 1)], wy.at[whole, whole, pl.ds(0, 1)], (0, 0, 1))
        group.send(w0.at[7], wt.at[0], (1, 0, 0))
        group.send(w0.at[0], wt.at[1], (-1, 0, 0))
        return group

    def around0(slot, t):
        buf = v0[slot]
        here = pl.ds(t + 1, GROUP)
        mid = buf[here, z_all, y_all, :]
        total = roll(mid, 1, 3) + roll(mid, -1, 3)
        total += buf[pl.ds(t, GROUP), z_all, y_all, :] + buf[pl.ds(t + 2, GROUP), z_all, y_all, :]
        total += buf[here, pl.ds(0, 8), y_all, :] + buf[here, pl.ds(2, 8), y_all, :]
        return mid, total + buf[here, z_all, pl.ds(OFF - 1, 16), :] + buf[here, z_all, pl.ds(OFF + 1, 16), :]

    def clear0(slot):
        zero = jnp.zeros((8, 16, 128), jnp.float32)
        v0[slot][0, z_all, y_all, :] = zero
        v0[slot][9, z_all, y_all, :] = zero
        rim = jnp.zeros((8, OFF, 128), jnp.float32)

        def body(t):
            v0[slot][t + 1, 0, y_all, :] = zero[0]
            v0[slot][t + 1, 9, y_all, :] = zero[0]
            v0[slot][t + 1, z_all, pl.ds(0, OFF), :] = rim
            v0[slot][t + 1, z_all, pl.ds(OFF + 16, OFF), :] = rim

        loop(0, 8, body)

    def sweep0(slot, out):
        def body(i):
            t = i * GROUP
            mid, total = around0(slot, t)
            here = pl.ds(t + 1, GROUP)
            old = (1.0 - DAMPING) * mid + v0[0][here, z_all, y_all, :]
            v0[out][here, z_all, y_all, :] = old + w0[pl.ds(t, GROUP)] * total

        loop(0, 8 // GROUP, body)

    def residual0(slot, t):
        mid, total = around0(slot, t)
        return s0[pl.ds(t, GROUP)] - ((8.0 + m0[pl.ds(t, GROUP)]) * mid - total)

    def halo_y(n, t):
        halo = hy[n, t]
        low = jnp.where(rows(halo) == 0, roll(halo, 1, 1), 0.0)
        high = jnp.where(rows(halo) == 7, roll(halo, -1, 1), 0.0)
        return jnp.concatenate([low, high], axis=1)

    def fix0(out, n):
        def body(t):
            v0[out][t + 1, z_all, y_all, :] = v0[out][t + 1, z_all, y_all, :] + w0[t] * halo_y(n, t)
            for side, z in ((0, 0), (1, 7)):
                v0[out][t + 1, z + 1, y_all, :] = v0[out][t + 1, z + 1, y_all, :] + w0[t, z] * hz[n, side, t]

        loop(0, 8, body)
        for side, t in ((0, 0), (1, 7)):
            v0[out][t + 1, z_all, y_all, :] = v0[out][t + 1, z_all, y_all, :] + w0[t] * ht[n, side]

    def add_halos(ref, n):
        def body(t):
            ref[t] = ref[t] + halo_y(n, t)
            for side, z in ((0, 0), (1, 7)):
                ref[t, z] = ref[t, z] + hz[n, side, t]

        loop(0, 8, body)
        for side, t in ((0, 0), (1, 7)):
            ref[t] = ref[t] + ht[n, side]

    def coarsen(a, step):
        nt, nz, ny, _ = a.shape
        a = a.reshape(nt // 2, 2, nz // 2, 2, ny, 128)
        a = a[:, 0] + a[:, 1]
        t, z = slice(0, nt // 2), slice(0, nz // 2)
        pairs[t, z, 0:ny, :] = a[:, :, 0] + a[:, :, 1]
        b = pairs[t, z, pl.ds(0, ny // 2, stride=2), :]
        b += pairs[t, z, pl.ds(1, ny // 2, stride=2), :]
        return (b + partner(b, step, 3)) * (1.0 / 16.0)

    def swap1(buf, into, widths, sender=0):
        def span(k, side):
            if side == 0:
                return pl.ds(3, 4), pl.ds(3, 4)
            if side == 1:
                return pl.ds(7 - k, k), pl.ds(3 - k, k)
            return pl.ds(3, k), pl.ds(7, k)

        group = Group(sender)
        offsets = [(a, b, c) for a in (0, 1, -1) for b in (0, 1, -1) for c in (0, 1, -1)][1:]
        for a, b, c in sorted(offsets, key=lambda o: -sum(map(abs, o))):
            k = widths[abs(a) + abs(b) + abs(c) - 1]
            if k < 1:
                continue
            (t_src, t_dst), (z_src, z_dst) = span(k, a), span(k, b)
            y = {0: pl.ds(0, 8), 1: pl.ds(8 - k, k), -1: pl.ds(0, k)}[c]
            y_dst = y if c == 0 else pl.ds(y.start + 8, y.size)
            group.send(buf.at[t_src, z_src, y], into.at[t_dst, z_dst, y_dst], (a, b, abs(c)))
        return group

    def around1(slot, t, count, radius):
        nz = 4 + 2 * radius
        z = 3 - radius
        buf = v1[slot]
        here = pl.ds(t, count)
        mid = buf[here, pl.ds(z, nz)]
        total = roll(mid, 2, 3) + roll(mid, -2, 3)
        total += buf[pl.ds(t - 1, count), pl.ds(z, nz)] + buf[pl.ds(t + 1, count), pl.ds(z, nz)]
        total += buf[here, pl.ds(z - 1, nz)] + buf[here, pl.ds(z + 1, nz)]
        return mid, total + roll(mid, 1, 2) + roll(mid, -1, 2)

    def sweep1(slot, out, radius, first, weight):
        z = pl.ds(3 - radius, 4 + 2 * radius)

        def body(i):
            t = 3 - radius + i * GROUP1
            mid, total = around1(slot, t, GROUP1, radius)
            here = pl.ds(t, GROUP1)
            v1[out][here, z] = (1.0 - DAMPING) * mid + first[here, z] + weight[here, z] * total

        loop(0, (4 + 2 * radius) // GROUP1, body)

    def pack2(kind, block):
        p2[1, 0, kind, 0:4, :] = pack4(block[0, 0], block[0, 1], block[1, 0], block[1, 1])

    def gather2():
        whole = pl.ds(0, 2)
        own = p2.at[1, 0, whole, pl.ds(0, 4)]
        group = Group()
        for a, b, c in sorted(near, key=lambda o: -(abs(o[0]) + (0, 1, 2, 1)[o[1]] + 2 * o[2])):
            group.send(own, p2.at[1 - a, (4 - b) % 4, whole, pl.ds(4 * c, 4)], (a, b, c))
        return group

    def unpack2(x, into, at):
        a, b, c, d = unpack4(x)
        into[at] = jnp.stack([a, b], axis=1).reshape(8, 8, 128)
        into[at + 1] = jnp.stack([c, d], axis=1).reshape(8, 8, 128)

    def image(buf, t, count, level):
        mid = buf[pl.ds(t, count)]
        step = 1 << level
        total = roll(mid, step, 3) + roll(mid, -step, 3)
        total += buf[pl.ds(t - 1, count)] + buf[pl.ds(t + 1, count)] + ring(mid, 1, 1) + ring(mid, -1, 1)
        step = level - 1
        return mid, total + roll(mid, step, 2) + roll(mid, -step, 2)

    def sweep_ring(buf, out, first, weight, low, high, level, count):
        def body(i):
            t = low + i * count
            mid, total = image(buf, t, count, level)
            span = pl.ds(t, count)
            out[span] = (1.0 - DAMPING) * mid + first[span] + weight[span] * total

        if high - low == count:
            body(0)
        else:
            loop(0, (high - low) // count, body)

    def coarsen_ring(first, second):
        a = (first + second).reshape(4, 2, 8, 128)
        a = a[:, 0] + a[:, 1]
        a += partner(a, 1, 1)
        return (a + partner(a, 4, 2)) * (1.0 / 16.0)

    def pack3(x):
        row, lane = rows(x[0]), lanes(x[0])
        return jnp.where(
            even(row, 1), jnp.where(even(lane, 1), x[0], x[2]), jnp.where(even(lane, 1), x[1], x[3])
        )

    def unpack3(x):
        first, second = spread(x, 1, 0)
        a, c = spread(first, 1, 1)
        b, d = spread(second, 1, 1)
        return jnp.stack([a, b, c, d])

    load_m.wait()
    load_s.wait()

    def first0(t):
        w = DAMPING / (8.0 + m0[t])
        w0[t] = w
        v0[0][t + 1, z_all, y_all, :] = w * s0[t]

    loop(0, 8, first0)
    pl.semaphore_wait(barrier, len(faces))
    halos = swap0(0, 0)

    own1 = pl.ds(3, 4)
    m1[...] = coarsen(m0[...], 1)
    w1[own1, own1, 0:8, :] = 0.5 * DAMPING / (4.0 + m1[...])
    m2_own[...] = coarsen(m1[...], 2)
    pack2(1, m2_own[...])
    for slot in (0, 1, 3, 4):
        clear0(slot)
    sweep0(0, 1)

    halos.arrived()
    fix0(1, 0)
    halos = swap0(1, 1)
    weights1_in = swap1(w1, w1, (1, 0, 0))

    def rest0(i):
        r0[pl.ds(i * GROUP, GROUP)] = residual0(1, i * GROUP)

    loop(0, 8 // GROUP, rest0)
    halos.arrived()
    add_halos(r0, 1)

    s1[...] = coarsen(r0[...], 1)
    v1[0][own1, own1, 0:8, :] = 2.0 * w1[own1, own1, 0:8, :] * s1[...]
    first1_in = swap1(v1[0], v1[0], (2, 1, 0))
    sweep0(1, 3)
    fix0(3, 1)
    halos = swap0(3, 2, 2)
    weights1_in.arrived()
    first1_in.arrived()
    sweep1(0, 1, 1, v1[0], w1)

    mid, total = around1(1, 3, 4, 0)
    mid1, total1 = mid, total = mid[:, :, 0:8], total[:, :, 0:8]
    d = 4.0 + m1[...]
    source2 = coarsen(s1[...] - (d * mid - 0.5 * total), 2)
    pack2(0, DAMPING * source2 / (2.0 + m2_own[...]))
    source2_in = gather2()
    v1[3][own1, own1, 0:8, :] = (
        (1.0 - DAMPING) * mid1 + v1[0][own1, own1, 0:8, :] + w1[own1, own1, 0:8, :] * total1
    )
    halo1_in = swap1(v1[3], v1[3], (2, 2, 1), 1)
    weight_1[own1, own1, 0:8, :] = w1[own1, own1, 0:8, :]
    weights_in = swap1(w1, weight_1, (2, 2, 1))
    source2_in.arrived()

    def first2(t):
        unpack2(p2[t, :, 0], u2, 2 + 2 * t)
        unpack2(p2[t, :, 1], m2, 2 + 2 * t)
        span = pl.ds(2 + 2 * t, 2)
        w2[span] = 0.25 * DAMPING / (2.0 + m2[span])

    for t in range(3):
        first2(t)
    sweep_ring(u2, v2, u2, w2, 3, 7, 2, 4)
    mid, total = image(v2, 4, 2, 2)
    remainder = (2.0 + m2[4:6]) * (u2[4:6] * (1.0 / DAMPING) - mid) + 0.25 * total
    weight3 = DAMPING / (1.0 + coarsen_ring(m2[4], m2[5]))
    d3[5, 0] = pack3(weight3 * coarsen_ring(remainder[0], remainder[1]))
    d3[5, 1] = pack3(0.125 * weight3)
    planes_in = Group()
    for k in range(5, 0, -1):
        for a in (k, -k):
            planes_in.send(d3.at[5], d3.at[5 - a], (a, 0, 0))
    d2_own[0] = p2[1, :, 0]
    for k, field in ((1, w2), (2, v2)):
        halves = field[4:6].reshape(2, 4, 2, 8, 128)
        d2_own[k] = pack4(halves[0, :, 0], halves[0, :, 1], halves[1, :, 0], halves[1, :, 1])
    halo2_in = Group()
    for a in (1, -1, 2, -2):
        halo2_in.send(d2_own, d2_in.at[2 - a], (a, 0, 0))
    weights0_in = swap_weights()
    halo2_in.arrived()
    for k, at in ((0, 0), (4, 8)):
        unpack2(d2_in[k, 0], u2, at)
        unpack2(d2_in[k, 1], w2, at)
    for k, at in ((0, 0), (1, 2), (3, 6), (4, 8)):
        unpack2(d2_in[k, 2], v2, at)

    planes_in.arrived()

    for t in range(11):
        v3[0][t] = unpack3(d3[t, 0])
        w3[t] = unpack3(d3[t, 1])
    for step in range(3):
        sweep_ring(v3[step], v3[step + 1], v3[0], w3, 1 + step, 10 - step, 3, 9 - 2 * step)

    def correct2(t):
        e = v3[3][3 + t]
        e = jnp.broadcast_to(e[:, None], (4, 2, 8, 128)).reshape(8, 8, 128)
        for k in range(2):
            v2[2 * t + k] = v2[2 * t + k] + e

    loop(0, 5, correct2)
    sweep_ring(v2, s2, u2, w2, 1, 9, 2, 4)
    sweep_ring(s2, v2, u2, w2, 2, 8, 2, 3)

    halo1_in.arrived()
    all_sent(1)

    def expand1(tc):
        for z in range(6):
            e = v2[2 + tc, (z - 2) % 8]
            tmp[z, pl.ds(0, 8, stride=2), :] = e
            tmp[z, pl.ds(1, 8, stride=2), :] = e
        e = tmp[0:6, 0:16, :]
        return jnp.broadcast_to(e[:, None], (6, 2, 16, 128)).reshape(12, 16, 128)[1:11]

    e = expand1(0)
    v1[2][0] = e

    def correct1(tc):
        e = expand1(tc)
        for k in range(2):
            v1[2][2 * tc + k - 1] = e

    loop(1, 5, correct1)
    e = expand1(5)
    v1[2][9] = e
    weights_in.arrived()
    sweep1(2, 3, 2, v1[3], weight_1)
    sweep1(3, 4, 1, v1[0], weight_1)

    def expand0(tc):
        e = v1[4][2 + tc, pl.ds(2, 6)]
        tmp[0:6, pl.ds(OFF, 8, stride=2), :] = e[:, 0:8]
        tmp[0:6, pl.ds(OFF + 1, 8, stride=2), :] = e[:, 0:8]
        tmp[0:6, OFF - 1 : OFF, :] = e[:, 15:16]
        tmp[0:6, OFF + 16 : OFF + 17, :] = e[:, 8:9]
        e = tmp[...]
        return jnp.broadcast_to(e[:, None], (6, 2, 32, 128)).reshape(12, 32, 128)[1:11]

    v0[2][0] = expand0(0)

    def correct0(tc):
        e = expand0(tc)
        for k in range(2):
            v0[2][2 * tc + k - 1] = e

    loop(1, 5, correct0)
    v0[2][9] = expand0(5)
    halos.arrived()
    weights0_in.arrived()
    all_sent(2)
    keep = 1.0 - DAMPING

    def add0(i):
        t = i * GROUP
        mid, total = around0(2, t)
        here = pl.ds(t + 1, GROUP)
        v0[3][here, z_all, y_all, :] = v0[3][here, z_all, y_all, :] + keep * mid + w0[pl.ds(t, GROUP)] * total

    loop(0, 8 // GROUP, add0)
    buf = v0[2]
    for side, t, inner in ((0, 0, 1), (1, 9, 8)):
        mid = buf[t, z_all, y_all, :]
        total = roll(mid, 1, 2) + roll(mid, -1, 2) + mid + buf[inner, z_all, y_all, :]
        total += buf[t, pl.ds(0, 8), y_all, :] + buf[t, pl.ds(2, 8), y_all, :]
        total += buf[t, z_all, pl.ds(OFF - 1, 16), :] + buf[t, z_all, pl.ds(OFF + 1, 16), :]
        ht[2, side] = ht[2, side] + keep * mid + wt[side] * total
    for side, z, inner in ((0, 0, 1), (1, 9, 8)):
        mid = buf[t_all, z, y_all, :]
        total = roll(mid, 1, 2) + roll(mid, -1, 2) + mid + buf[t_all, inner, y_all, :]
        total += buf[pl.ds(0, 8), z, y_all, :] + buf[pl.ds(2, 8), z, y_all, :]
        total += buf[t_all, z, pl.ds(OFF - 1, 16), :] + buf[t_all, z, pl.ds(OFF + 1, 16), :]
        hz[2, side] = hz[2, side] + keep * mid + wz[side] * total
    own, other = pl.ds(0, 8), pl.ds(8, 8)
    mid = v1[4][own1, own1, other, :]
    inner = v1[4][own1, own1, own, :]
    common = roll(mid, 1, 3) + roll(mid, -1, 3) + 3.0 * mid
    common += jnp.where(rows(inner) == 0, roll(inner, 1, 2), roll(inner, -1, 2))
    for a in range(2):
        for b in range(2):
            total = common + v1[4][pl.ds(2 + 2 * a, 4), own1, other, :] + v1[4][own1, pl.ds(2 + 2 * b, 4), other, :]
            for t in range(4):
                for z in range(4):
                    at = (2 * t + a, 2 * z + b)
                    hy[(2,) + at] = hy[(2,) + at] + keep * mid[t, z] + wy[at] * total[t, z]
    sweep0(3, 4)
    fix0(4, 2)
    halos = swap0(4, 3)

    def finish(i):
        here = pl.ds(i * GROUP, GROUP)
        res_ref[here] = residual0(4, i * GROUP)
        sol_ref[here] = v0[4][pl.ds(i * GROUP + 1, GROUP), z_all, y_all, :]

    loop(0, 8 // GROUP, finish)
    halos.arrived()
    add_halos(res_ref, 3)
    all_sent(0)


def per_device(right_side, mass_field):
    f32 = jnp.float32
    block = jax.ShapeDtypeStruct(right_side.shape, f32)
    vmem = pl.BlockSpec(memory_space=pltpu.VMEM)
    hbm = pl.BlockSpec(memory_space=pltpu.HBM)
    own, ring2, ring3 = (8, 8, 16, 128), (10, 8, 8, 128), (11, 4, 8, 128)
    shapes = [
        own, own, own, own, *[(10, 10, 32, 128)] * 5,
        (4, 2, 8, 16, 128), (4, 2, 8, 16, 128), (4, 8, 8, 8, 128),
        (2, 8, 16, 128), (2, 8, 16, 128), (8, 8, 8, 128),
        *[(4, 4, 8, 128)] * 2, *[(10, 10, 16, 128)] * 2, (2, 2, 4, 128), *[(10, 10, 16, 128)] * 5,
        (3, 4, 2, 8, 128), ring2, ring2, ring2, ring2, ring2, (3, 4, 8, 128), (5, 3, 4, 8, 128),
        (11, 2, 8, 128), *[ring3] * 5,
        (6, 32, 128), (4, 4, 16, 128), (ROWS, 128),
    ]
    scratch = [pltpu.VMEM(shape, f32) for shape in shapes]
    scratch += [pltpu.SemaphoreType.DMA((count,)) for count in (2, 3, 13)]
    return pl.pallas_call(
        kernel,
        out_shape=(block, block),
        in_specs=[hbm, hbm],
        out_specs=(vmem, vmem),
        scratch_shapes=scratch,
        compiler_params=pltpu.CompilerParams(
            collective_id=0, has_side_effects=True, vmem_limit_bytes=56 * 1024 * 1024
        ),
    )(right_side, mass_field)


def solution(mesh):
    placed = (P("ta", "gz", "gy", None), P("ta", "gz", "gy", None))
    return jax.shard_map(
        per_device, mesh=mesh, in_specs=placed, out_specs=placed, check_vma=False
    )
```

```python
import jax
import jax.numpy as jnp
from jax import lax
from jax.experimental import pallas as pl
from jax.experimental.pallas import tpu as pltpu
from jax.sharding import PartitionSpec as P

DAMPING = 0.7
OFF = 8
GROUP = 2
GROUP1 = 2
ROWS = 8192
MESH = pl.DeviceIdType.MESH


def lanes(like):
    return lax.broadcasted_iota(jnp.int32, like.shape, like.ndim - 1)


def rows(like):
    return lax.broadcasted_iota(jnp.int32, like.shape, like.ndim - 2)


def roll(x, shift, axis):
    return pltpu.roll(x, shift % x.shape[axis], axis)


def ring(x, shift, axis=0):
    shift %= x.shape[axis]
    cut = x.shape[axis] - shift
    return jnp.concatenate(
        [lax.slice_in_dim(x, cut, x.shape[axis], axis=axis), lax.slice_in_dim(x, 0, cut, axis=axis)], axis=axis
    )


def even(index, step):
    return jnp.bitwise_and(index, step) == 0


def partner(x, step, axis):
    index = lax.broadcasted_iota(jnp.int32, x.shape, axis)
    return jnp.where(even(index, step), roll(x, -step, axis), roll(x, step, axis))


def spread(x, step, axis):
    index = lax.broadcasted_iota(jnp.int32, x.shape, axis)
    low = even(index, step)
    return jnp.where(low, x, roll(x, step, axis)), jnp.where(low, roll(x, -step, axis), x)


def pack4(a, b, c, d):
    lane = lanes(a)
    return jnp.where(
        even(lane, 2), jnp.where(even(lane, 1), a, b), jnp.where(even(lane, 1), c, d)
    )


def unpack4(x):
    last = x.ndim - 1
    first, second = spread(x, 1, last)
    a, c = spread(first, 2, last)
    b, d = spread(second, 2, last)
    return a, b, c, d


def kernel(
    s_hbm, m_hbm, sol_ref, res_ref,
    s0, m0, w0, r0, v0_0, v0_1, v0_2, v0_3, v0_4, ht, hz, hy, wt, wz, wy,
    s1, m1, w1, weight_1, m2_own, v1_0, v1_1, v1_2, v1_3, v1_4, p2, s2, m2, w2, u2, v2, d2_own, d2_in, d3, w3, v3_0, v3_1, v3_2, v3_3, tmp, pairs, bytes_ref,
    load_sem, send_sem, recv_sem,
):
    ta, gz, gy = lax.axis_index("ta"), lax.axis_index("gz"), lax.axis_index("gy")
    nta, ngz, ngy = lax.axis_size("ta"), lax.axis_size("gz"), lax.axis_size("gy")

    v0, v1 = (v0_0, v0_1, v0_2, v0_3, v0_4), (v1_0, v1_1, v1_2, v1_3, v1_4)
    v3 = (v3_0, v3_1, v3_2, v3_3)
    load_m = pltpu.make_async_copy(m_hbm, m0, load_sem.at[0])
    load_s = pltpu.make_async_copy(s_hbm, s0, load_sem.at[1])
    load_m.start()
    load_s.start()

    def device(a, b, c):
        return (
            lax.rem(ta + (a + nta), nta),
            lax.rem(gz + (b + ngz), ngz),
            lax.rem(gy + c, ngy),
        )

    barrier = pltpu.get_barrier_semaphore()
    near = [(a, b, c) for a in (0, 1, -1) for b in range(4) for c in range(2)][1:]
    faces = [(1, 0, 0), (-1, 0, 0), (0, 1, 0), (0, -1, 0), (0, 0, 1)]
    for offset in faces:
        pl.semaphore_signal(barrier, inc=1, device_id=device(*offset), device_id_type=MESH)

    groups = []
    sends = [0, 0, 0]

    class Group:
        def __init__(self, sender=0):
            self.number, self.count, self.sender = len(groups), 0, sender
            groups.append(self)

        def send(self, src, dst, offset):
            size = 1
            for extent in dst.shape[:-1]:
                size *= extent
            self.count += size
            sends[self.sender] += size
            pltpu.make_async_remote_copy(
                src_ref=src,
                dst_ref=dst,
                send_sem=send_sem.at[self.sender],
                recv_sem=recv_sem.at[self.number],
                device_id=device(*offset),
                device_id_type=MESH,
            ).start()

        def arrived(self):
            whole = bytes_ref.at[pl.ds(0, self.count)]
            pltpu.make_async_copy(whole, whole, recv_sem.at[self.number]).wait()

    def all_sent(sender):
        whole = bytes_ref.at[pl.ds(0, sends[sender])]
        pltpu.make_async_copy(whole, whole, send_sem.at[sender]).wait()

    def loop(low, high, body):
        lax.fori_loop(low, high, lambda t, c: (body(t), c)[1], 0)

    t_all, y_all = pl.ds(1, 8), pl.ds(OFF, 16)
    z_all = t_all

    def swap0(slot, n, sender=0):
        buf = v0[slot]
        group = Group(sender)
        group.send(buf.at[t_all, 8, y_all], hz.at[n, 0], (0, 1, 0))
        group.send(buf.at[t_all, 1, y_all], hz.at[n, 1], (0, -1, 0))
        one = pl.ds(0, 1)
        whole = pl.ds(0, 8)
        group.send(buf.at[t_all, z_all, pl.ds(OFF + 15, 1)], hy.at[n, whole, whole, pl.ds(7, 1)], (0, 0, 1))
        group.send(buf.at[t_all, z_all, pl.ds(OFF, 1)], hy.at[n, whole, whole, one], (0, 0, 1))
        group.send(buf.at[8, z_all, y_all], ht.at[n, 0], (1, 0, 0))
        group.send(buf.at[1, z_all, y_all], ht.at[n, 1], (-1, 0, 0))
        return group

    def swap_weights():
        group = Group()
        whole = pl.ds(0, 8)
        group.send(w0.at[whole, 7], wz.at[0], (0, 1, 0))
        group.send(w0.at[whole, 0], wz.at[1], (0, -1, 0))
        group.send(w0.at[whole, whole, pl.ds(15, 1)], wy.at[whole, whole, pl.ds(7, 1)], (0, 0, 1))
        group.send(w0.at[whole, whole, pl.ds(0, 1)], wy.at[whole, whole, pl.ds(0, 1)], (0, 0, 1))
        group.send(w0.at[7], wt.at[0], (1, 0, 0))
        group.send(w0.at[0], wt.at[1], (-1, 0, 0))
        return group

    def around0(slot, t):
        buf = v0[slot]
        here = pl.ds(t + 1, GROUP)
        mid = buf[here, z_all, y_all, :]
        total = roll(mid, 1, 3) + roll(mid, -1, 3)
        total += buf[pl.ds(t, GROUP), z_all, y_all, :] + buf[pl.ds(t + 2, GROUP), z_all, y_all, :]
        total += buf[here, pl.ds(0, 8), y_all, :] + buf[here, pl.ds(2, 8), y_all, :]
        return mid, total + buf[here, z_all, pl.ds(OFF - 1, 16), :] + buf[here, z_all, pl.ds(OFF + 1, 16), :]

    def clear0(slot):
        zero = jnp.zeros((8, 16, 128), jnp.float32)
        v0[slot][0, z_all, y_all, :] = zero
        v0[slot][9, z_all, y_all, :] = zero
        rim = jnp.zeros((8, OFF, 128), jnp.float32)

        def body(t):
            v0[slot][t + 1, 0, y_all, :] = zero[0]
            v0[slot][t + 1, 9, y_all, :] = zero[0]
            v0[slot][t + 1, z_all, pl.ds(0, OFF), :] = rim
            v0[slot][t + 1, z_all, pl.ds(OFF + 16, OFF), :] = rim

        loop(0, 8, body)

    def sweep0(slot, out):
        def body(i):
            t = i * GROUP
            mid, total = around0(slot, t)
            here = pl.ds(t + 1, GROUP)
            old = (1.0 - DAMPING) * mid + v0[0][here, z_all, y_all, :]
            v0[out][here, z_all, y_all, :] = old + w0[pl.ds(t, GROUP)] * total

        loop(0, 8 // GROUP, body)

    def residual0(slot, t):
        mid, total = around0(slot, t)
        return s0[pl.ds(t, GROUP)] - ((8.0 + m0[pl.ds(t, GROUP)]) * mid - total)

    def halo_y(n, t):
        halo = hy[n, t]
        low = jnp.where(rows(halo) == 0, roll(halo, 1, 1), 0.0)
        high = jnp.where(rows(halo) == 7, roll(halo, -1, 1), 0.0)
        return jnp.concatenate([low, high], axis=1)

    def fix0(out, n):
        def body(t):
            v0[out][t + 1, z_all, y_all, :] = v0[out][t + 1, z_all, y_all, :] + w0[t] * halo_y(n, t)
            for side, z in ((0, 0), (1, 7)):
                v0[out][t + 1, z + 1, y_all, :] = v0[out][t + 1, z + 1, y_all, :] + w0[t, z] * hz[n, side, t]

        loop(0, 8, body)
        for side, t in ((0, 0), (1, 7)):
            v0[out][t + 1, z_all, y_all, :] = v0[out][t + 1, z_all, y_all, :] + w0[t] * ht[n, side]

    def add_halos(ref, n):
        def body(t):
            ref[t] = ref[t] + halo_y(n, t)
            for side, z in ((0, 0), (1, 7)):
                ref[t, z] = ref[t, z] + hz[n, side, t]

        loop(0, 8, body)
        for side, t in ((0, 0), (1, 7)):
            ref[t] = ref[t] + ht[n, side]

    def coarsen(a, step):
        nt, nz, ny, _ = a.shape
        a = a.reshape(nt // 2, 2, nz // 2, 2, ny, 128)
        a = a[:, 0] + a[:, 1]
        t, z = slice(0, nt // 2), slice(0, nz // 2)
        pairs[t, z, 0:ny, :] = a[:, :, 0] + a[:, :, 1]
        b = pairs[t, z, pl.ds(0, ny // 2, stride=2), :]
        b += pairs[t, z, pl.ds(1, ny // 2, stride=2), :]
        return (b + partner(b, step, 3)) * (1.0 / 16.0)

    def swap1(buf, into, widths, sender=0):
        def span(k, side):
            if side == 0:
                return pl.ds(3, 4), pl.ds(3, 4)
            if side == 1:
                return pl.ds(7 - k, k), pl.ds(3 - k, k)
            return pl.ds(3, k), pl.ds(7, k)

        group = Group(sender)
        offsets = [(a, b, c) for a in (0, 1, -1) for b in (0, 1, -1) for c in (0, 1, -1)][1:]
        for a, b, c in sorted(offsets, key=lambda o: -sum(map(abs, o))):
            k = widths[abs(a) + abs(b) + abs(c) - 1]
            if k < 1:
                continue
            (t_src, t_dst), (z_src, z_dst) = span(k, a), span(k, b)
            y = {0: pl.ds(0, 8), 1: pl.ds(8 - k, k), -1: pl.ds(0, k)}[c]
            y_dst = y if c == 0 else pl.ds(y.start + 8, y.size)
            group.send(buf.at[t_src, z_src, y], into.at[t_dst, z_dst, y_dst], (a, b, abs(c)))
        return group

    def around1(slot, t, count, radius):
        nz = 4 + 2 * radius
        z = 3 - radius
        buf = v1[slot]
        here = pl.ds(t, count)
        mid = buf[here, pl.ds(z, nz)]
        total = roll(mid, 2, 3) + roll(mid, -2, 3)
        total += buf[pl.ds(t - 1, count), pl.ds(z, nz)] + buf[pl.ds(t + 1, count), pl.ds(z, nz)]
        total += buf[here, pl.ds(z - 1, nz)] + buf[here, pl.ds(z + 1, nz)]
        return mid, total + roll(mid, 1, 2) + roll(mid, -1, 2)

    def sweep1(slot, out, radius, first, weight):
        z = pl.ds(3 - radius, 4 + 2 * radius)

        def body(i):
            t = 3 - radius + i * GROUP1
            mid, total = around1(slot, t, GROUP1, radius)
            here = pl.ds(t, GROUP1)
            v1[out][here, z] = (1.0 - DAMPING) * mid + first[here, z] + weight[here, z] * total

        loop(0, (4 + 2 * radius) // GROUP1, body)

    def pack2(kind, block):
        p2[1, 0, kind, 0:4, :] = pack4(block[0, 0], block[0, 1], block[1, 0], block[1, 1])

    def gather2():
        whole = pl.ds(0, 2)
        own = p2.at[1, 0, whole, pl.ds(0, 4)]
        group = Group()
        for a, b, c in sorted(near, key=lambda o: -(abs(o[0]) + (0, 1, 2, 1)[o[1]] + 2 * o[2])):
            group.send(own, p2.at[1 - a, (4 - b) % 4, whole, pl.ds(4 * c, 4)], (a, b, c))
        return group

    def unpack2(x, first, second):
        a, b, c, d = unpack4(x)
        first[0][first[1]] = jnp.stack([a, b], axis=1).reshape(8, 8, 128)
        second[0][second[1]] = jnp.stack([c, d], axis=1).reshape(8, 8, 128)

    def pack_planes(first, second):
        first, second = first.reshape(4, 2, 8, 128), second.reshape(4, 2, 8, 128)
        return pack4(first[:, 0], first[:, 1], second[:, 0], second[:, 1])

    def image(buf, t, count, level):
        mid = buf[pl.ds(t, count)]
        step = 1 << level
        total = roll(mid, step, 3) + roll(mid, -step, 3)
        total += buf[pl.ds(t - 1, count)] + buf[pl.ds(t + 1, count)] + ring(mid, 1, 1) + ring(mid, -1, 1)
        step = level - 1
        return mid, total + roll(mid, step, 2) + roll(mid, -step, 2)

    def sweep_ring(buf, out, first, weight, low, high, level, count):
        def body(i):
            t = low + i * count
            mid, total = image(buf, t, count, level)
            span = pl.ds(t, count)
            out[span] = (1.0 - DAMPING) * mid + first[span] + weight[span] * total

        if high - low == count:
            body(0)
        else:
            loop(0, (high - low) // count, body)

    def coarsen_ring(first, second):
        a = (first + second).reshape(4, 2, 8, 128)
        a = a[:, 0] + a[:, 1]
        a += partner(a, 1, 1)
        return (a + partner(a, 4, 2)) * (1.0 / 16.0)

    def pack3(x):
        row, lane = rows(x[0]), lanes(x[0])
        return jnp.where(
            even(row, 1), jnp.where(even(lane, 1), x[0], x[2]), jnp.where(even(lane, 1), x[1], x[3])
        )

    def unpack3(x):
        first, second = spread(x, 1, 0)
        a, c = spread(first, 1, 1)
        b, d = spread(second, 1, 1)
        return jnp.stack([a, b, c, d])

    load_m.wait()
    load_s.wait()

    def first0(t):
        w = DAMPING / (8.0 + m0[t])
        w0[t] = w
        v0[0][t + 1, z_all, y_all, :] = w * s0[t]

    loop(0, 8, first0)
    pl.semaphore_wait(barrier, len(faces))
    halos = swap0(0, 0)

    own1 = pl.ds(3, 4)
    m1[...] = coarsen(m0[...], 1)
    w1[own1, own1, 0:8, :] = 0.5 * DAMPING / (4.0 + m1[...])
    m2_own[...] = coarsen(m1[...], 2)
    pack2(1, m2_own[...])
    for slot in (0, 1, 3, 4):
        clear0(slot)
    sweep0(0, 1)

    halos.arrived()
    fix0(1, 0)
    halos = swap0(1, 1)
    weights1_in = swap1(w1, w1, (1, 0, 0))

    def rest0(i):
        r0[pl.ds(i * GROUP, GROUP)] = residual0(1, i * GROUP)

    loop(0, 8 // GROUP, rest0)
    halos.arrived()
    add_halos(r0, 1)

    s1[...] = coarsen(r0[...], 1)
    v1[0][own1, own1, 0:8, :] = 2.0 * w1[own1, own1, 0:8, :] * s1[...]
    first1_in = swap1(v1[0], v1[0], (2, 1, 0))
    sweep0(1, 3)
    fix0(3, 1)
    halos = swap0(3, 2, 2)
    weights1_in.arrived()
    first1_in.arrived()
    sweep1(0, 1, 1, v1[0], w1)

    mid, total = around1(1, 3, 4, 0)
    mid1, total1 = mid, total = mid[:, :, 0:8], total[:, :, 0:8]
    d = 4.0 + m1[...]
    source2 = coarsen(s1[...] - (d * mid - 0.5 * total), 2)
    pack2(0, DAMPING * source2 / (2.0 + m2_own[...]))
    source2_in = gather2()
    v1[3][own1, own1, 0:8, :] = (
        (1.0 - DAMPING) * mid1 + v1[0][own1, own1, 0:8, :] + w1[own1, own1, 0:8, :] * total1
    )
    halo1_in = swap1(v1[3], v1[3], (2, 2, 1), 1)
    weight_1[own1, own1, 0:8, :] = w1[own1, own1, 0:8, :]
    weights_in = swap1(w1, weight_1, (2, 2, 1))
    source2_in.arrived()

    def first2(t):
        unpack2(p2[t, :, 0], (u2, 2 + 2 * t), (u2, 3 + 2 * t))
        unpack2(p2[t, :, 1], (m2, 2 + 2 * t), (m2, 3 + 2 * t))
        span = pl.ds(2 + 2 * t, 2)
        w2[span] = 0.25 * DAMPING / (2.0 + m2[span])

    for t in range(3):
        first2(t)
    sweep_ring(u2, v2, u2, w2, 3, 7, 2, 4)
    mid, total = image(v2, 4, 2, 2)
    remainder = (2.0 + m2[4:6]) * (u2[4:6] * (1.0 / DAMPING) - mid) + 0.25 * total
    weight3 = DAMPING / (1.0 + coarsen_ring(m2[4], m2[5]))
    d3[5, 0] = pack3(weight3 * coarsen_ring(remainder[0], remainder[1]))
    d3[5, 1] = pack3(0.125 * weight3)
    planes_in = Group()
    for k in range(5, 0, -1):
        for a in (k, -k):
            planes_in.send(d3.at[5], d3.at[5 - a], (a, 0, 0))
    d2_own[0] = pack_planes(u2[5], w2[5])
    d2_own[1] = pack_planes(v2[4], v2[5])
    d2_own[2] = pack_planes(u2[4], w2[4])
    halo2_in = Group()
    for a, kind, count in ((2, 0, 2), (-2, 1, 2), (1, 1, 1), (-1, 1, 1)):
        halo2_in.send(d2_own.at[pl.ds(kind, count)], d2_in.at[2 - a, pl.ds(0, count)], (a, 0, 0))
    weights0_in = swap_weights()
    planes_in.arrived()

    for t in range(11):
        v3[0][t] = unpack3(d3[t, 0])
        w3[t] = unpack3(d3[t, 1])
    for step in range(3):
        sweep_ring(v3[step], v3[step + 1], v3[0], w3, 1 + step, 10 - step, 3, 9 - 2 * step)

    halo2_in.arrived()
    unpack2(d2_in[0, 0], (u2, 1), (w2, 1))
    unpack2(d2_in[4, 1], (u2, 8), (w2, 8))
    for k, kind, at in ((0, 1, 0), (1, 0, 2), (3, 0, 6), (4, 0, 8)):
        unpack2(d2_in[k, kind], (v2, at), (v2, at + 1))

    def correct2(t):
        e = v3[3][3 + t]
        e = jnp.broadcast_to(e[:, None], (4, 2, 8, 128)).reshape(8, 8, 128)
        for k in range(2):
            v2[2 * t + k] = v2[2 * t + k] + e

    loop(0, 5, correct2)
    sweep_ring(v2, s2, u2, w2, 1, 9, 2, 4)
    sweep_ring(s2, v2, u2, w2, 2, 8, 2, 3)

    halo1_in.arrived()
    all_sent(1)

    def expand1(tc):
        for z in range(6):
            e = v2[2 + tc, (z - 2) % 8]
            tmp[z, pl.ds(0, 8, stride=2), :] = e
            tmp[z, pl.ds(1, 8, stride=2), :] = e
        e = tmp[0:6, 0:16, :]
        return jnp.broadcast_to(e[:, None], (6, 2, 16, 128)).reshape(12, 16, 128)[1:11]

    e = expand1(0)
    v1[2][0] = e

    def correct1(tc):
        e = expand1(tc)
        for k in range(2):
            v1[2][2 * tc + k - 1] = e

    loop(1, 5, correct1)
    e = expand1(5)
    v1[2][9] = e
    weights_in.arrived()
    sweep1(2, 3, 2, v1[3], weight_1)
    sweep1(3, 4, 1, v1[0], weight_1)

    def expand0(tc):
        e = v1[4][2 + tc, pl.ds(2, 6)]
        tmp[0:6, pl.ds(OFF, 8, stride=2), :] = e[:, 0:8]
        tmp[0:6, pl.ds(OFF + 1, 8, stride=2), :] = e[:, 0:8]
        tmp[0:6, OFF - 1 : OFF, :] = e[:, 15:16]
        tmp[0:6, OFF + 16 : OFF + 17, :] = e[:, 8:9]
        e = tmp[...]
        return jnp.broadcast_to(e[:, None], (6, 2, 32, 128)).reshape(12, 32, 128)[1:11]

    v0[2][0] = expand0(0)

    def correct0(tc):
        e = expand0(tc)
        for k in range(2):
            v0[2][2 * tc + k - 1] = e

    loop(1, 5, correct0)
    v0[2][9] = expand0(5)
    halos.arrived()
    weights0_in.arrived()
    all_sent(2)
    keep = 1.0 - DAMPING

    def add0(i):
        t = i * GROUP
        mid, total = around0(2, t)
        here = pl.ds(t + 1, GROUP)
        v0[3][here, z_all, y_all, :] = v0[3][here, z_all, y_all, :] + keep * mid + w0[pl.ds(t, GROUP)] * total

    loop(0, 8 // GROUP, add0)
    buf = v0[2]
    for side, t, inner in ((0, 0, 1), (1, 9, 8)):
        mid = buf[t, z_all, y_all, :]
        total = roll(mid, 1, 2) + roll(mid, -1, 2) + mid + buf[inner, z_all, y_all, :]
        total += buf[t, pl.ds(0, 8), y_all, :] + buf[t, pl.ds(2, 8), y_all, :]
        total += buf[t, z_all, pl.ds(OFF - 1, 16), :] + buf[t, z_all, pl.ds(OFF + 1, 16), :]
        ht[2, side] = ht[2, side] + keep * mid + wt[side] * total
    for side, z, inner in ((0, 0, 1), (1, 9, 8)):
        mid = buf[t_all, z, y_all, :]
        total = roll(mid, 1, 2) + roll(mid, -1, 2) + mid + buf[t_all, inner, y_all, :]
        total += buf[pl.ds(0, 8), z, y_all, :] + buf[pl.ds(2, 8), z, y_all, :]
        total += buf[t_all, z, pl.ds(OFF - 1, 16), :] + buf[t_all, z, pl.ds(OFF + 1, 16), :]
        hz[2, side] = hz[2, side] + keep * mid + wz[side] * total
    own, other = pl.ds(0, 8), pl.ds(8, 8)
    mid = v1[4][own1, own1, other, :]
    inner = v1[4][own1, own1, own, :]
    common = roll(mid, 1, 3) + roll(mid, -1, 3) + 3.0 * mid
    common += jnp.where(rows(inner) == 0, roll(inner, 1, 2), roll(inner, -1, 2))
    for a in range(2):
        for b in range(2):
            total = common + v1[4][pl.ds(2 + 2 * a, 4), own1, other, :] + v1[4][own1, pl.ds(2 + 2 * b, 4), other, :]
            for t in range(4):
                for z in range(4):
                    at = (2 * t + a, 2 * z + b)
                    hy[(2,) + at] = hy[(2,) + at] + keep * mid[t, z] + wy[at] * total[t, z]
    sweep0(3, 4)
    fix0(4, 2)
    halos = swap0(4, 3)

    def finish(i):
        here = pl.ds(i * GROUP, GROUP)
        res_ref[here] = residual0(4, i * GROUP)
        sol_ref[here] = v0[4][pl.ds(i * GROUP + 1, GROUP), z_all, y_all, :]

    loop(0, 8 // GROUP, finish)
    halos.arrived()
    add_halos(res_ref, 3)
    all_sent(0)


def store(sol_ref, res_ref, sol_hbm, res_hbm, sem):
    copies = []
    for i, (src, dst) in enumerate(((sol_ref, sol_hbm), (res_ref, res_hbm))):
        for k in range(4):
            part = pl.ds(2 * k, 2)
            copies.append(pltpu.make_async_copy(src.at[part], dst.at[part], sem.at[4 * i + k]))
    for copy in copies:
        copy.start()
    for copy in copies:
        copy.wait()


def per_device(right_side, mass_field):
    f32 = jnp.float32
    block = jax.ShapeDtypeStruct(right_side.shape, f32)
    vmem = pl.BlockSpec(memory_space=pltpu.VMEM)
    hbm = pl.BlockSpec(memory_space=pltpu.HBM)
    own, ring2, ring3 = (8, 8, 16, 128), (10, 8, 8, 128), (11, 4, 8, 128)
    shapes = [
        own, own, own, own, *[(10, 10, 32, 128)] * 5,
        (4, 2, 8, 16, 128), (4, 2, 8, 16, 128), (4, 8, 8, 8, 128),
        (2, 8, 16, 128), (2, 8, 16, 128), (8, 8, 8, 128),
        *[(4, 4, 8, 128)] * 2, *[(10, 10, 16, 128)] * 2, (2, 2, 4, 128), *[(10, 10, 16, 128)] * 5,
        (3, 4, 2, 8, 128), ring2, ring2, ring2, ring2, ring2, (3, 4, 8, 128), (5, 2, 4, 8, 128),
        (11, 2, 8, 128), *[ring3] * 5,
        (6, 32, 128), (4, 4, 16, 128), (ROWS, 128),
    ]
    scratch = [pltpu.VMEM(shape, f32) for shape in shapes]
    scratch += [pltpu.SemaphoreType.DMA((count,)) for count in (2, 3, 13)]
    outs = pl.pallas_call(
        kernel,
        out_shape=(block, block),
        in_specs=[hbm, hbm],
        out_specs=(vmem, vmem),
        scratch_shapes=scratch,
        compiler_params=pltpu.CompilerParams(
            collective_id=0, has_side_effects=True, vmem_limit_bytes=56 * 1024 * 1024
        ),
    )(right_side, mass_field)
    return pl.pallas_call(
        store,
        out_shape=(block, block),
        in_specs=[vmem, vmem],
        out_specs=(hbm, hbm),
        scratch_shapes=[pltpu.SemaphoreType.DMA((8,))],
    )(*outs)


def solution(mesh):
    placed = (P("ta", "gz", "gy", None), P("ta", "gz", "gy", None))
    return jax.shard_map(
        per_device, mesh=mesh, in_specs=placed, out_specs=placed, check_vma=False
    )
```

```python
import jax
import jax.numpy as jnp
from jax import lax
from jax.experimental import pallas as pl
from jax.experimental.pallas import tpu as pltpu
from jax.sharding import PartitionSpec as P

DAMPING = 0.7
OFF = 8
GROUP = 4
GROUP1 = 2
ROWS = 8192
MESH = pl.DeviceIdType.MESH


def lanes(like):
    return lax.broadcasted_iota(jnp.int32, like.shape, like.ndim - 1)


def rows(like):
    return lax.broadcasted_iota(jnp.int32, like.shape, like.ndim - 2)


def roll(x, shift, axis):
    return pltpu.roll(x, shift % x.shape[axis], axis)


def ring(x, shift, axis=0):
    shift %= x.shape[axis]
    cut = x.shape[axis] - shift
    return jnp.concatenate(
        [lax.slice_in_dim(x, cut, x.shape[axis], axis=axis), lax.slice_in_dim(x, 0, cut, axis=axis)], axis=axis
    )


def even(index, step):
    return jnp.bitwise_and(index, step) == 0


def partner(x, step, axis):
    index = lax.broadcasted_iota(jnp.int32, x.shape, axis)
    return jnp.where(even(index, step), roll(x, -step, axis), roll(x, step, axis))


def spread(x, step, axis):
    index = lax.broadcasted_iota(jnp.int32, x.shape, axis)
    low = even(index, step)
    return jnp.where(low, x, roll(x, step, axis)), jnp.where(low, roll(x, -step, axis), x)


def pack4(a, b, c, d):
    lane = lanes(a)
    return jnp.where(
        even(lane, 2), jnp.where(even(lane, 1), a, b), jnp.where(even(lane, 1), c, d)
    )


def unpack4(x):
    last = x.ndim - 1
    first, second = spread(x, 1, last)
    a, c = spread(first, 2, last)
    b, d = spread(second, 2, last)
    return a, b, c, d


def kernel(
    s_hbm, m_hbm, sol_ref, res_ref,
    s0, m0, w0, r0, v0_0, v0_1, v0_2, v0_3, v0_4, ht, hz, hy, wt, wz, wy,
    s1, m1, w1, weight_1, m2_own, v1_0, v1_1, v1_2, v1_3, v1_4, p2, s2, m2, w2, u2, v2, d2_own, d2_in, d3, w3, v3_0, v3_1, v3_2, v3_3, tmp, pairs, bytes_ref,
    load_sem, send_sem, recv_sem,
):
    ta, gz, gy = lax.axis_index("ta"), lax.axis_index("gz"), lax.axis_index("gy")
    nta, ngz, ngy = lax.axis_size("ta"), lax.axis_size("gz"), lax.axis_size("gy")

    v0, v1 = (v0_0, v0_1, v0_2, v0_3, v0_4), (v1_0, v1_1, v1_2, v1_3, v1_4)
    v3 = (v3_0, v3_1, v3_2, v3_3)
    load_m = pltpu.make_async_copy(m_hbm, m0, load_sem.at[0])
    load_s = pltpu.make_async_copy(s_hbm, s0, load_sem.at[1])
    load_m.start()
    load_s.start()

    def device(a, b, c):
        return (
            lax.rem(ta + (a + nta), nta),
            lax.rem(gz + (b + ngz), ngz),
            lax.rem(gy + c, ngy),
        )

    barrier = pltpu.get_barrier_semaphore()
    near = [(a, b, c) for a in (0, 1, -1) for b in range(4) for c in range(2)][1:]
    faces = [(1, 0, 0), (-1, 0, 0), (0, 1, 0), (0, -1, 0), (0, 0, 1)]
    for offset in faces:
        pl.semaphore_signal(barrier, inc=1, device_id=device(*offset), device_id_type=MESH)

    groups = []
    sends = [0, 0, 0]

    class Group:
        def __init__(self, sender=0):
            self.number, self.count, self.sender = len(groups), 0, sender
            groups.append(self)

        def send(self, src, dst, offset):
            size = 1
            for extent in dst.shape[:-1]:
                size *= extent
            self.count += size
            sends[self.sender] += size
            pltpu.make_async_remote_copy(
                src_ref=src,
                dst_ref=dst,
                send_sem=send_sem.at[self.sender],
                recv_sem=recv_sem.at[self.number],
                device_id=device(*offset),
                device_id_type=MESH,
            ).start()

        def arrived(self):
            whole = bytes_ref.at[pl.ds(0, self.count)]
            pltpu.make_async_copy(whole, whole, recv_sem.at[self.number]).wait()

    def all_sent(sender):
        whole = bytes_ref.at[pl.ds(0, sends[sender])]
        pltpu.make_async_copy(whole, whole, send_sem.at[sender]).wait()

    def loop(low, high, body):
        lax.fori_loop(low, high, lambda t, c: (body(t), c)[1], 0)

    t_all, y_all = pl.ds(1, 8), pl.ds(OFF, 16)
    z_all = t_all

    def swap0(slot, n, sender=0):
        buf = v0[slot]
        group = Group(sender)
        group.send(buf.at[t_all, 8, y_all], hz.at[n, 0], (0, 1, 0))
        group.send(buf.at[t_all, 1, y_all], hz.at[n, 1], (0, -1, 0))
        one = pl.ds(0, 1)
        whole = pl.ds(0, 8)
        group.send(buf.at[t_all, z_all, pl.ds(OFF + 15, 1)], hy.at[n, whole, whole, pl.ds(7, 1)], (0, 0, 1))
        group.send(buf.at[t_all, z_all, pl.ds(OFF, 1)], hy.at[n, whole, whole, one], (0, 0, 1))
        group.send(buf.at[8, z_all, y_all], ht.at[n, 0], (1, 0, 0))
        group.send(buf.at[1, z_all, y_all], ht.at[n, 1], (-1, 0, 0))
        return group

    def swap_weights():
        group = Group()
        whole = pl.ds(0, 8)
        group.send(w0.at[whole, 7], wz.at[0], (0, 1, 0))
        group.send(w0.at[whole, 0], wz.at[1], (0, -1, 0))
        group.send(w0.at[whole, whole, pl.ds(15, 1)], wy.at[whole, whole, pl.ds(7, 1)], (0, 0, 1))
        group.send(w0.at[whole, whole, pl.ds(0, 1)], wy.at[whole, whole, pl.ds(0, 1)], (0, 0, 1))
        group.send(w0.at[7], wt.at[0], (1, 0, 0))
        group.send(w0.at[0], wt.at[1], (-1, 0, 0))
        return group

    def around0(slot, t):
        buf = v0[slot]
        here = pl.ds(t + 1, GROUP)
        mid = buf[here, z_all, y_all, :]
        total = roll(mid, 1, 3) + roll(mid, -1, 3)
        total += buf[pl.ds(t, GROUP), z_all, y_all, :] + buf[pl.ds(t + 2, GROUP), z_all, y_all, :]
        total += buf[here, pl.ds(0, 8), y_all, :] + buf[here, pl.ds(2, 8), y_all, :]
        return mid, total + buf[here, z_all, pl.ds(OFF - 1, 16), :] + buf[here, z_all, pl.ds(OFF + 1, 16), :]

    def clear0(slot):
        zero = jnp.zeros((8, 16, 128), jnp.float32)
        v0[slot][0, z_all, y_all, :] = zero
        v0[slot][9, z_all, y_all, :] = zero
        rim = jnp.zeros((8, OFF, 128), jnp.float32)

        def body(t):
            v0[slot][t + 1, 0, y_all, :] = zero[0]
            v0[slot][t + 1, 9, y_all, :] = zero[0]
            v0[slot][t + 1, z_all, pl.ds(0, OFF), :] = rim
            v0[slot][t + 1, z_all, pl.ds(OFF + 16, OFF), :] = rim

        loop(0, 8, body)

    def sweep0(slot, out):
        def body(i):
            t = i * GROUP
            mid, total = around0(slot, t)
            here = pl.ds(t + 1, GROUP)
            old = (1.0 - DAMPING) * mid + v0[0][here, z_all, y_all, :]
            v0[out][here, z_all, y_all, :] = old + w0[pl.ds(t, GROUP)] * total

        loop(0, 8 // GROUP, body)

    def residual0(slot, t):
        mid, total = around0(slot, t)
        return s0[pl.ds(t, GROUP)] - ((8.0 + m0[pl.ds(t, GROUP)]) * mid - total)

    def halo_y(n, t):
        halo = hy[n, t]
        low = jnp.where(rows(halo) == 0, roll(halo, 1, 1), 0.0)
        high = jnp.where(rows(halo) == 7, roll(halo, -1, 1), 0.0)
        return jnp.concatenate([low, high], axis=1)

    def fix0(out, n):
        def body(t):
            v0[out][t + 1, z_all, y_all, :] = v0[out][t + 1, z_all, y_all, :] + w0[t] * halo_y(n, t)
            for side, z in ((0, 0), (1, 7)):
                v0[out][t + 1, z + 1, y_all, :] = v0[out][t + 1, z + 1, y_all, :] + w0[t, z] * hz[n, side, t]

        loop(0, 8, body)
        for side, t in ((0, 0), (1, 7)):
            v0[out][t + 1, z_all, y_all, :] = v0[out][t + 1, z_all, y_all, :] + w0[t] * ht[n, side]

    def add_halos(ref, n):
        def body(t):
            ref[t] = ref[t] + halo_y(n, t)
            for side, z in ((0, 0), (1, 7)):
                ref[t, z] = ref[t, z] + hz[n, side, t]

        loop(0, 8, body)
        for side, t in ((0, 0), (1, 7)):
            ref[t] = ref[t] + ht[n, side]

    def coarsen(a, step):
        nt, nz, ny, _ = a.shape
        a = a.reshape(nt // 2, 2, nz // 2, 2, ny, 128)
        a = a[:, 0] + a[:, 1]
        t, z = slice(0, nt // 2), slice(0, nz // 2)
        pairs[t, z, 0:ny, :] = a[:, :, 0] + a[:, :, 1]
        b = pairs[t, z, pl.ds(0, ny // 2, stride=2), :]
        b += pairs[t, z, pl.ds(1, ny // 2, stride=2), :]
        return (b + partner(b, step, 3)) * (1.0 / 16.0)

    def swap1(buf, into, widths, sender=0):
        def span(k, side):
            if side == 0:
                return pl.ds(3, 4), pl.ds(3, 4)
            if side == 1:
                return pl.ds(7 - k, k), pl.ds(3 - k, k)
            return pl.ds(3, k), pl.ds(7, k)

        group = Group(sender)
        offsets = [(a, b, c) for a in (0, 1, -1) for b in (0, 1, -1) for c in (0, 1, -1)][1:]
        for a, b, c in sorted(offsets, key=lambda o: -sum(map(abs, o))):
            k = widths[abs(a) + abs(b) + abs(c) - 1]
            if k < 1:
                continue
            (t_src, t_dst), (z_src, z_dst) = span(k, a), span(k, b)
            y = {0: pl.ds(0, 8), 1: pl.ds(8 - k, k), -1: pl.ds(0, k)}[c]
            y_dst = y if c == 0 else pl.ds(y.start + 8, y.size)
            group.send(buf.at[t_src, z_src, y], into.at[t_dst, z_dst, y_dst], (a, b, abs(c)))
        return group

    def around1(slot, t, count, radius):
        nz = 4 + 2 * radius
        z = 3 - radius
        buf = v1[slot]
        here = pl.ds(t, count)
        mid = buf[here, pl.ds(z, nz)]
        total = roll(mid, 2, 3) + roll(mid, -2, 3)
        total += buf[pl.ds(t - 1, count), pl.ds(z, nz)] + buf[pl.ds(t + 1, count), pl.ds(z, nz)]
        total += buf[here, pl.ds(z - 1, nz)] + buf[here, pl.ds(z + 1, nz)]
        return mid, total + roll(mid, 1, 2) + roll(mid, -1, 2)

    def sweep1(slot, out, radius, first, weight):
        z = pl.ds(3 - radius, 4 + 2 * radius)

        def body(i):
            t = 3 - radius + i * GROUP1
            mid, total = around1(slot, t, GROUP1, radius)
            here = pl.ds(t, GROUP1)
            v1[out][here, z] = (1.0 - DAMPING) * mid + first[here, z] + weight[here, z] * total

        loop(0, (4 + 2 * radius) // GROUP1, body)

    def pack2(kind, block):
        p2[1, 0, kind, 0:4, :] = pack4(block[0, 0], block[0, 1], block[1, 0], block[1, 1])

    def gather2():
        whole = pl.ds(0, 2)
        own = p2.at[1, 0, whole, pl.ds(0, 4)]
        group = Group()
        for a, b, c in sorted(near, key=lambda o: -(abs(o[0]) + (0, 1, 2, 1)[o[1]] + 2 * o[2])):
            group.send(own, p2.at[1 - a, (4 - b) % 4, whole, pl.ds(4 * c, 4)], (a, b, c))
        return group

    def unpack2(x, first, second):
        a, b, c, d = unpack4(x)
        first[0][first[1]] = jnp.stack([a, b], axis=1).reshape(8, 8, 128)
        second[0][second[1]] = jnp.stack([c, d], axis=1).reshape(8, 8, 128)

    def pack_planes(first, second):
        first, second = first.reshape(4, 2, 8, 128), second.reshape(4, 2, 8, 128)
        return pack4(first[:, 0], first[:, 1], second[:, 0], second[:, 1])

    def image(buf, t, count, level):
        mid = buf[pl.ds(t, count)]
        step = 1 << level
        total = roll(mid, step, 3) + roll(mid, -step, 3)
        total += buf[pl.ds(t - 1, count)] + buf[pl.ds(t + 1, count)] + ring(mid, 1, 1) + ring(mid, -1, 1)
        step = level - 1
        return mid, total + roll(mid, step, 2) + roll(mid, -step, 2)

    def sweep_ring(buf, out, first, weight, low, high, level, count):
        def body(i):
            t = low + i * count
            mid, total = image(buf, t, count, level)
            span = pl.ds(t, count)
            out[span] = (1.0 - DAMPING) * mid + first[span] + weight[span] * total

        if high - low == count:
            body(0)
        else:
            loop(0, (high - low) // count, body)

    def coarsen_ring(first, second):
        a = (first + second).reshape(4, 2, 8, 128)
        a = a[:, 0] + a[:, 1]
        a += partner(a, 1, 1)
        return (a + partner(a, 4, 2)) * (1.0 / 16.0)

    def pack3(x):
        row, lane = rows(x[0]), lanes(x[0])
        return jnp.where(
            even(row, 1), jnp.where(even(lane, 1), x[0], x[2]), jnp.where(even(lane, 1), x[1], x[3])
        )

    def unpack3(x):
        first, second = spread(x, 1, 0)
        a, c = spread(first, 1, 1)
        b, d = spread(second, 1, 1)
        return jnp.stack([a, b, c, d])

    load_m.wait()
    load_s.wait()

    def first0(t):
        w = DAMPING / (8.0 + m0[t])
        w0[t] = w
        v0[0][t + 1, z_all, y_all, :] = w * s0[t]

    loop(0, 8, first0)
    pl.semaphore_wait(barrier, len(faces))
    halos = swap0(0, 0)

    own1 = pl.ds(3, 4)
    m1[...] = coarsen(m0[...], 1)
    w1[own1, own1, 0:8, :] = 0.5 * DAMPING / (4.0 + m1[...])
    m2_own[...] = coarsen(m1[...], 2)
    pack2(1, m2_own[...])
    for slot in (0, 1, 3, 4):
        clear0(slot)
    sweep0(0, 1)

    halos.arrived()
    fix0(1, 0)
    halos = swap0(1, 1)
    weights1_in = swap1(w1, w1, (1, 0, 0))

    def rest0(i):
        r0[pl.ds(i * GROUP, GROUP)] = residual0(1, i * GROUP)

    loop(0, 8 // GROUP, rest0)
    halos.arrived()
    add_halos(r0, 1)

    s1[...] = coarsen(r0[...], 1)
    v1[0][own1, own1, 0:8, :] = 2.0 * w1[own1, own1, 0:8, :] * s1[...]
    first1_in = swap1(v1[0], v1[0], (2, 1, 0))
    sweep0(1, 3)
    fix0(3, 1)
    halos = swap0(3, 2, 2)
    weights1_in.arrived()
    first1_in.arrived()
    sweep1(0, 1, 1, v1[0], w1)

    mid, total = around1(1, 3, 4, 0)
    mid1, total1 = mid, total = mid[:, :, 0:8], total[:, :, 0:8]
    d = 4.0 + m1[...]
    source2 = coarsen(s1[...] - (d * mid - 0.5 * total), 2)
    pack2(0, DAMPING * source2 / (2.0 + m2_own[...]))
    source2_in = gather2()
    v1[3][own1, own1, 0:8, :] = (
        (1.0 - DAMPING) * mid1 + v1[0][own1, own1, 0:8, :] + w1[own1, own1, 0:8, :] * total1
    )
    halo1_in = swap1(v1[3], v1[3], (2, 2, 1), 1)
    weight_1[own1, own1, 0:8, :] = w1[own1, own1, 0:8, :]
    weights_in = swap1(w1, weight_1, (2, 2, 1))
    source2_in.arrived()

    def first2(t):
        unpack2(p2[t, :, 0], (u2, 2 + 2 * t), (u2, 3 + 2 * t))
        unpack2(p2[t, :, 1], (m2, 2 + 2 * t), (m2, 3 + 2 * t))
        span = pl.ds(2 + 2 * t, 2)
        w2[span] = 0.25 * DAMPING / (2.0 + m2[span])

    for t in range(3):
        first2(t)
    sweep_ring(u2, v2, u2, w2, 3, 7, 2, 4)
    mid, total = image(v2, 4, 2, 2)
    remainder = (2.0 + m2[4:6]) * (u2[4:6] * (1.0 / DAMPING) - mid) + 0.25 * total
    weight3 = DAMPING / (1.0 + coarsen_ring(m2[4], m2[5]))
    d3[5, 0] = pack3(weight3 * coarsen_ring(remainder[0], remainder[1]))
    d3[5, 1] = pack3(0.125 * weight3)
    planes_in = Group()
    for k in range(5, 0, -1):
        for a in (k, -k):
            planes_in.send(d3.at[5], d3.at[5 - a], (a, 0, 0))
    d2_own[0] = pack_planes(u2[5], w2[5])
    d2_own[1] = pack_planes(v2[4], v2[5])
    d2_own[2] = pack_planes(u2[4], w2[4])
    halo2_in = Group()
    for a, kind, count in ((2, 0, 2), (-2, 1, 2), (1, 1, 1), (-1, 1, 1)):
        halo2_in.send(d2_own.at[pl.ds(kind, count)], d2_in.at[2 - a, pl.ds(0, count)], (a, 0, 0))
    weights0_in = swap_weights()
    planes_in.arrived()

    for t in range(11):
        v3[0][t] = unpack3(d3[t, 0])
        w3[t] = unpack3(d3[t, 1])
    for step in range(3):
        sweep_ring(v3[step], v3[step + 1], v3[0], w3, 1 + step, 10 - step, 3, 9 - 2 * step)

    halo2_in.arrived()
    unpack2(d2_in[0, 0], (u2, 1), (w2, 1))
    unpack2(d2_in[4, 1], (u2, 8), (w2, 8))
    for k, kind, at in ((0, 1, 0), (1, 0, 2), (3, 0, 6), (4, 0, 8)):
        unpack2(d2_in[k, kind], (v2, at), (v2, at + 1))

    def correct2(t):
        e = v3[3][3 + t]
        e = jnp.broadcast_to(e[:, None], (4, 2, 8, 128)).reshape(8, 8, 128)
        for k in range(2):
            v2[2 * t + k] = v2[2 * t + k] + e

    loop(0, 5, correct2)
    sweep_ring(v2, s2, u2, w2, 1, 9, 2, 4)
    sweep_ring(s2, v2, u2, w2, 2, 8, 2, 3)

    halo1_in.arrived()
    all_sent(1)

    def expand1(tc):
        for z in range(6):
            e = v2[2 + tc, (z - 2) % 8]
            tmp[z, pl.ds(0, 8, stride=2), :] = e
            tmp[z, pl.ds(1, 8, stride=2), :] = e
        e = tmp[0:6, 0:16, :]
        return jnp.broadcast_to(e[:, None], (6, 2, 16, 128)).reshape(12, 16, 128)[1:11]

    e = expand1(0)
    v1[2][0] = e

    def correct1(tc):
        e = expand1(tc)
        for k in range(2):
            v1[2][2 * tc + k - 1] = e

    loop(1, 5, correct1)
    e = expand1(5)
    v1[2][9] = e
    weights_in.arrived()
    sweep1(2, 3, 2, v1[3], weight_1)
    sweep1(3, 4, 1, v1[0], weight_1)

    def expand0(tc):
        e = v1[4][2 + tc, pl.ds(2, 6)]
        tmp[0:6, pl.ds(OFF, 8, stride=2), :] = e[:, 0:8]
        tmp[0:6, pl.ds(OFF + 1, 8, stride=2), :] = e[:, 0:8]
        tmp[0:6, OFF - 1 : OFF, :] = e[:, 15:16]
        tmp[0:6, OFF + 16 : OFF + 17, :] = e[:, 8:9]
        e = tmp[...]
        return jnp.broadcast_to(e[:, None], (6, 2, 32, 128)).reshape(12, 32, 128)[1:11]

    v0[2][0] = expand0(0)

    def correct0(tc):
        e = expand0(tc)
        for k in range(2):
            v0[2][2 * tc + k - 1] = e

    loop(1, 5, correct0)
    v0[2][9] = expand0(5)
    halos.arrived()
    weights0_in.arrived()
    all_sent(2)
    keep = 1.0 - DAMPING

    def add0(i):
        t = i * GROUP
        mid, total = around0(2, t)
        here = pl.ds(t + 1, GROUP)
        v0[3][here, z_all, y_all, :] = v0[3][here, z_all, y_all, :] + keep * mid + w0[pl.ds(t, GROUP)] * total

    loop(0, 8 // GROUP, add0)
    buf = v0[2]
    for side, t, inner in ((0, 0, 1), (1, 9, 8)):
        mid = buf[t, z_all, y_all, :]
        total = roll(mid, 1, 2) + roll(mid, -1, 2) + mid + buf[inner, z_all, y_all, :]
        total += buf[t, pl.ds(0, 8), y_all, :] + buf[t, pl.ds(2, 8), y_all, :]
        total += buf[t, z_all, pl.ds(OFF - 1, 16), :] + buf[t, z_all, pl.ds(OFF + 1, 16), :]
        ht[2, side] = ht[2, side] + keep * mid + wt[side] * total
    for side, z, inner in ((0, 0, 1), (1, 9, 8)):
        mid = buf[t_all, z, y_all, :]
        total = roll(mid, 1, 2) + roll(mid, -1, 2) + mid + buf[t_all, inner, y_all, :]
        total += buf[pl.ds(0, 8), z, y_all, :] + buf[pl.ds(2, 8), z, y_all, :]
        total += buf[t_all, z, pl.ds(OFF - 1, 16), :] + buf[t_all, z, pl.ds(OFF + 1, 16), :]
        hz[2, side] = hz[2, side] + keep * mid + wz[side] * total
    own, other = pl.ds(0, 8), pl.ds(8, 8)
    mid = v1[4][own1, own1, other, :]
    inner = v1[4][own1, own1, own, :]
    common = roll(mid, 1, 3) + roll(mid, -1, 3) + 3.0 * mid
    common += jnp.where(rows(inner) == 0, roll(inner, 1, 2), roll(inner, -1, 2))
    for a in range(2):
        for b in range(2):
            total = common + v1[4][pl.ds(2 + 2 * a, 4), own1, other, :] + v1[4][own1, pl.ds(2 + 2 * b, 4), other, :]
            for t in range(4):
                for z in range(4):
                    at = (2 * t + a, 2 * z + b)
                    hy[(2,) + at] = hy[(2,) + at] + keep * mid[t, z] + wy[at] * total[t, z]
    sweep0(3, 4)
    fix0(4, 2)
    halos = swap0(4, 3)

    def finish(i):
        here = pl.ds(i * GROUP, GROUP)
        res_ref[here] = residual0(4, i * GROUP)
        sol_ref[here] = v0[4][pl.ds(i * GROUP + 1, GROUP), z_all, y_all, :]

    loop(0, 8 // GROUP, finish)
    halos.arrived()
    add_halos(res_ref, 3)
    all_sent(0)


def store(sol_ref, res_ref, sol_hbm, res_hbm, sem):
    copies = []
    for i, (src, dst) in enumerate(((sol_ref, sol_hbm), (res_ref, res_hbm))):
        for k in range(4):
            part = pl.ds(2 * k, 2)
            copies.append(pltpu.make_async_copy(src.at[part], dst.at[part], sem.at[4 * i + k]))
    for copy in copies:
        copy.start()
    for copy in copies:
        copy.wait()


def per_device(right_side, mass_field):
    f32 = jnp.float32
    block = jax.ShapeDtypeStruct(right_side.shape, f32)
    vmem = pl.BlockSpec(memory_space=pltpu.VMEM)
    hbm = pl.BlockSpec(memory_space=pltpu.HBM)
    own, ring2, ring3 = (8, 8, 16, 128), (10, 8, 8, 128), (11, 4, 8, 128)
    shapes = [
        own, own, own, own, *[(10, 10, 32, 128)] * 5,
        (4, 2, 8, 16, 128), (4, 2, 8, 16, 128), (4, 8, 8, 8, 128),
        (2, 8, 16, 128), (2, 8, 16, 128), (8, 8, 8, 128),
        *[(4, 4, 8, 128)] * 2, *[(10, 10, 16, 128)] * 2, (2, 2, 4, 128), *[(10, 10, 16, 128)] * 5,
        (3, 4, 2, 8, 128), ring2, ring2, ring2, ring2, ring2, (3, 4, 8, 128), (5, 2, 4, 8, 128),
        (11, 2, 8, 128), *[ring3] * 5,
        (6, 32, 128), (4, 4, 16, 128), (ROWS, 128),
    ]
    scratch = [pltpu.VMEM(shape, f32) for shape in shapes]
    scratch += [pltpu.SemaphoreType.DMA((count,)) for count in (2, 3, 13)]
    outs = pl.pallas_call(
        kernel,
        out_shape=(block, block),
        in_specs=[hbm, hbm],
        out_specs=(vmem, vmem),
        scratch_shapes=scratch,
        compiler_params=pltpu.CompilerParams(
            collective_id=0, has_side_effects=True, vmem_limit_bytes=56 * 1024 * 1024
        ),
    )(right_side, mass_field)
    return pl.pallas_call(
        store,
        out_shape=(block, block),
        in_specs=[vmem, vmem],
        out_specs=(hbm, hbm),
        scratch_shapes=[pltpu.SemaphoreType.DMA((8,))],
    )(*outs)


def solution(mesh):
    placed = (P("ta", "gz", "gy", None), P("ta", "gz", "gy", None))
    return jax.shard_map(
        per_device, mesh=mesh, in_specs=placed, out_specs=placed, check_vma=False
    )
```

```python
import jax
import jax.numpy as jnp
from jax import lax
from jax.experimental import pallas as pl
from jax.experimental.pallas import tpu as pltpu
from jax.sharding import PartitionSpec as P

DAMPING = 0.7
OFF = 8
GROUP = 4
ROWS = 8192
MESH = pl.DeviceIdType.MESH


def lanes(like):
    return lax.broadcasted_iota(jnp.int32, like.shape, like.ndim - 1)


def rows(like):
    return lax.broadcasted_iota(jnp.int32, like.shape, like.ndim - 2)


def roll(x, shift, axis):
    return pltpu.roll(x, shift % x.shape[axis], axis)


def ring(x, shift, axis=0):
    shift %= x.shape[axis]
    cut = x.shape[axis] - shift
    return jnp.concatenate(
        [lax.slice_in_dim(x, cut, x.shape[axis], axis=axis), lax.slice_in_dim(x, 0, cut, axis=axis)], axis=axis
    )


def even(index, step):
    return jnp.bitwise_and(index, step) == 0


def partner(x, step, axis):
    index = lax.broadcasted_iota(jnp.int32, x.shape, axis)
    return jnp.where(even(index, step), roll(x, -step, axis), roll(x, step, axis))


def spread(x, step, axis):
    index = lax.broadcasted_iota(jnp.int32, x.shape, axis)
    low = even(index, step)
    return jnp.where(low, x, roll(x, step, axis)), jnp.where(low, roll(x, -step, axis), x)


def pack4(a, b, c, d):
    lane = lanes(a)
    return jnp.where(
        even(lane, 2), jnp.where(even(lane, 1), a, b), jnp.where(even(lane, 1), c, d)
    )


def unpack4(x):
    last = x.ndim - 1
    first, second = spread(x, 1, last)
    a, c = spread(first, 2, last)
    b, d = spread(second, 2, last)
    return a, b, c, d


def kernel(
    s_hbm, m_hbm, sol_ref, res_ref,
    s0, m0, w0, r0, v0_0, v0_1, v0_2, v0_3, v0_4, ht, hz, hy, wt, wz, wy,
    s1, m1, w1, weight_1, m2_own, v1_0, v1_1, v1_2, v1_3, v1_4, p2, s2, m2, w2, u2, v2, d2_own, d2_in, d3, w3, v3_0, v3_1, v3_2, v3_3, tmp, pairs, bytes_ref,
    load_sem, send_sem, recv_sem,
):
    ta, gz, gy = lax.axis_index("ta"), lax.axis_index("gz"), lax.axis_index("gy")
    nta, ngz, ngy = lax.axis_size("ta"), lax.axis_size("gz"), lax.axis_size("gy")

    v0, v1 = (v0_0, v0_1, v0_2, v0_3, v0_4), (v1_0, v1_1, v1_2, v1_3, v1_4)
    v3 = (v3_0, v3_1, v3_2, v3_3)
    load_m = pltpu.make_async_copy(m_hbm, m0, load_sem.at[0])
    load_s = pltpu.make_async_copy(s_hbm, s0, load_sem.at[1])
    load_m.start()
    load_s.start()

    def device(a, b, c):
        return (
            lax.rem(ta + (a + nta), nta),
            lax.rem(gz + (b + ngz), ngz),
            lax.rem(gy + c, ngy),
        )

    barrier = pltpu.get_barrier_semaphore()
    near = [(a, b, c) for a in (0, 1, -1) for b in range(4) for c in range(2)][1:]
    faces = [(1, 0, 0), (-1, 0, 0), (0, 1, 0), (0, -1, 0), (0, 0, 1)]
    for offset in faces:
        pl.semaphore_signal(barrier, inc=1, device_id=device(*offset), device_id_type=MESH)

    groups = []
    sends = [0, 0, 0]

    class Group:
        def __init__(self, sender=0):
            self.number, self.count, self.sender = len(groups), 0, sender
            groups.append(self)

        def send(self, src, dst, offset):
            size = 1
            for extent in dst.shape[:-1]:
                size *= extent
            self.count += size
            sends[self.sender] += size
            pltpu.make_async_remote_copy(
                src_ref=src,
                dst_ref=dst,
                send_sem=send_sem.at[self.sender],
                recv_sem=recv_sem.at[self.number],
                device_id=device(*offset),
                device_id_type=MESH,
            ).start()

        def arrived(self):
            whole = bytes_ref.at[pl.ds(0, self.count)]
            pltpu.make_async_copy(whole, whole, recv_sem.at[self.number]).wait()

    def all_sent(sender):
        whole = bytes_ref.at[pl.ds(0, sends[sender])]
        pltpu.make_async_copy(whole, whole, send_sem.at[sender]).wait()

    def loop(low, high, body):
        lax.fori_loop(low, high, lambda t, c: (body(t), c)[1], 0)

    t_all, y_all = pl.ds(1, 8), pl.ds(OFF, 16)
    z_all = t_all

    def swap0(slot, n, sender=0):
        buf = v0[slot]
        group = Group(sender)
        group.send(buf.at[t_all, 8, y_all], hz.at[n, 0], (0, 1, 0))
        group.send(buf.at[t_all, 1, y_all], hz.at[n, 1], (0, -1, 0))
        one = pl.ds(0, 1)
        whole = pl.ds(0, 8)
        group.send(buf.at[t_all, z_all, pl.ds(OFF + 15, 1)], hy.at[n, whole, whole, pl.ds(7, 1)], (0, 0, 1))
        group.send(buf.at[t_all, z_all, pl.ds(OFF, 1)], hy.at[n, whole, whole, one], (0, 0, 1))
        group.send(buf.at[8, z_all, y_all], ht.at[n, 0], (1, 0, 0))
        group.send(buf.at[1, z_all, y_all], ht.at[n, 1], (-1, 0, 0))
        return group

    def swap_weights():
        group = Group()
        whole = pl.ds(0, 8)
        group.send(w0.at[whole, 7], wz.at[0], (0, 1, 0))
        group.send(w0.at[whole, 0], wz.at[1], (0, -1, 0))
        group.send(w0.at[whole, whole, pl.ds(15, 1)], wy.at[whole, whole, pl.ds(7, 1)], (0, 0, 1))
        group.send(w0.at[whole, whole, pl.ds(0, 1)], wy.at[whole, whole, pl.ds(0, 1)], (0, 0, 1))
        group.send(w0.at[7], wt.at[0], (1, 0, 0))
        group.send(w0.at[0], wt.at[1], (-1, 0, 0))
        return group

    def around0(slot, t):
        buf = v0[slot]
        here = pl.ds(t + 1, GROUP)
        mid = buf[here, z_all, y_all, :]
        total = roll(mid, 1, 3) + roll(mid, -1, 3)
        total += buf[pl.ds(t, GROUP), z_all, y_all, :] + buf[pl.ds(t + 2, GROUP), z_all, y_all, :]
        total += buf[here, pl.ds(0, 8), y_all, :] + buf[here, pl.ds(2, 8), y_all, :]
        return mid, total + buf[here, z_all, pl.ds(OFF - 1, 16), :] + buf[here, z_all, pl.ds(OFF + 1, 16), :]

    def clear0(slot):
        zero = jnp.zeros((8, 16, 128), jnp.float32)
        v0[slot][0, z_all, y_all, :] = zero
        v0[slot][9, z_all, y_all, :] = zero
        rim = jnp.zeros((8, OFF, 128), jnp.float32)

        def body(t):
            v0[slot][t + 1, 0, y_all, :] = zero[0]
            v0[slot][t + 1, 9, y_all, :] = zero[0]
            v0[slot][t + 1, z_all, pl.ds(0, OFF), :] = rim
            v0[slot][t + 1, z_all, pl.ds(OFF + 16, OFF), :] = rim

        loop(0, 8, body)

    def sweep0(slot, out):
        def body(i):
            t = i * GROUP
            mid, total = around0(slot, t)
            here = pl.ds(t + 1, GROUP)
            old = (1.0 - DAMPING) * mid + v0[0][here, z_all, y_all, :]
            v0[out][here, z_all, y_all, :] = old + w0[pl.ds(t, GROUP)] * total

        loop(0, 8 // GROUP, body)

    def residual0(slot, t):
        mid, total = around0(slot, t)
        return s0[pl.ds(t, GROUP)] - ((8.0 + m0[pl.ds(t, GROUP)]) * mid - total)

    def halo_y(n, t):
        halo = hy[n, t]
        low = jnp.where(rows(halo) == 0, roll(halo, 1, 1), 0.0)
        high = jnp.where(rows(halo) == 7, roll(halo, -1, 1), 0.0)
        return jnp.concatenate([low, high], axis=1)

    def fix0(out, n):
        def body(t):
            v0[out][t + 1, z_all, y_all, :] = v0[out][t + 1, z_all, y_all, :] + w0[t] * halo_y(n, t)
            for side, z in ((0, 0), (1, 7)):
                v0[out][t + 1, z + 1, y_all, :] = v0[out][t + 1, z + 1, y_all, :] + w0[t, z] * hz[n, side, t]

        loop(0, 8, body)
        for side, t in ((0, 0), (1, 7)):
            v0[out][t + 1, z_all, y_all, :] = v0[out][t + 1, z_all, y_all, :] + w0[t] * ht[n, side]

    def add_halos(ref, n):
        def body(t):
            ref[t] = ref[t] + halo_y(n, t)
            for side, z in ((0, 0), (1, 7)):
                ref[t, z] = ref[t, z] + hz[n, side, t]

        loop(0, 8, body)
        for side, t in ((0, 0), (1, 7)):
            ref[t] = ref[t] + ht[n, side]

    def coarsen(a, step):
        nt, nz, ny, _ = a.shape
        a = a.reshape(nt // 2, 2, nz // 2, 2, ny, 128)
        a = a[:, 0] + a[:, 1]
        t, z = slice(0, nt // 2), slice(0, nz // 2)
        pairs[t, z, 0:ny, :] = a[:, :, 0] + a[:, :, 1]
        b = pairs[t, z, pl.ds(0, ny // 2, stride=2), :]
        b += pairs[t, z, pl.ds(1, ny // 2, stride=2), :]
        return (b + partner(b, step, 3)) * (1.0 / 16.0)

    def swap1(buf, into, widths, sender=0):
        def span(k, side):
            if side == 0:
                return pl.ds(3, 4), pl.ds(3, 4)
            if side == 1:
                return pl.ds(7 - k, k), pl.ds(3 - k, k)
            return pl.ds(3, k), pl.ds(7, k)

        group = Group(sender)
        offsets = [(a, b, c) for a in (0, 1, -1) for b in (0, 1, -1) for c in (0, 1, -1)][1:]
        for a, b, c in sorted(offsets, key=lambda o: -sum(map(abs, o))):
            k = widths[abs(a) + abs(b) + abs(c) - 1]
            if k < 1:
                continue
            (t_src, t_dst), (z_src, z_dst) = span(k, a), span(k, b)
            y = {0: pl.ds(0, 8), 1: pl.ds(8 - k, k), -1: pl.ds(0, k)}[c]
            y_dst = y if c == 0 else pl.ds(y.start + 8, y.size)
            group.send(buf.at[t_src, z_src, y], into.at[t_dst, z_dst, y_dst], (a, b, abs(c)))
        return group

    def around1(slot, t, count, radius):
        nz = 4 + 2 * radius
        z = 3 - radius
        buf = v1[slot]
        here = pl.ds(t, count)
        mid = buf[here, pl.ds(z, nz)]
        total = roll(mid, 2, 3) + roll(mid, -2, 3)
        total += buf[pl.ds(t - 1, count), pl.ds(z, nz)] + buf[pl.ds(t + 1, count), pl.ds(z, nz)]
        total += buf[here, pl.ds(z - 1, nz)] + buf[here, pl.ds(z + 1, nz)]
        return mid, total + roll(mid, 1, 2) + roll(mid, -1, 2)

    def sweep1(slot, out, radius, first, weight):
        z = pl.ds(3 - radius, 4 + 2 * radius)

        count = 2 + radius

        def body(i):
            t = 3 - radius + i * count
            mid, total = around1(slot, t, count, radius)
            here = pl.ds(t, count)
            v1[out][here, z] = (1.0 - DAMPING) * mid + first[here, z] + weight[here, z] * total

        loop(0, 2, body)

    def pack2(kind, block):
        p2[1, 0, kind, 0:4, :] = pack4(block[0, 0], block[0, 1], block[1, 0], block[1, 1])

    def gather2():
        whole = pl.ds(0, 2)
        own = p2.at[1, 0, whole, pl.ds(0, 4)]
        group = Group()
        for a, b, c in sorted(near, key=lambda o: -(abs(o[0]) + (0, 1, 2, 1)[o[1]] + 2 * o[2])):
            group.send(own, p2.at[1 - a, (4 - b) % 4, whole, pl.ds(4 * c, 4)], (a, b, c))
        return group

    def unpack2(x, first, second):
        a, b, c, d = unpack4(x)
        first[0][first[1]] = jnp.stack([a, b], axis=1).reshape(8, 8, 128)
        second[0][second[1]] = jnp.stack([c, d], axis=1).reshape(8, 8, 128)

    def pack_planes(first, second):
        first, second = first.reshape(4, 2, 8, 128), second.reshape(4, 2, 8, 128)
        return pack4(first[:, 0], first[:, 1], second[:, 0], second[:, 1])

    def image(buf, t, count, level):
        mid = buf[pl.ds(t, count)]
        step = 1 << level
        total = roll(mid, step, 3) + roll(mid, -step, 3)
        total += buf[pl.ds(t - 1, count)] + buf[pl.ds(t + 1, count)] + ring(mid, 1, 1) + ring(mid, -1, 1)
        step = level - 1
        return mid, total + roll(mid, step, 2) + roll(mid, -step, 2)

    def sweep_ring(buf, out, first, weight, low, high, level, count):
        def body(i):
            t = low + i * count
            mid, total = image(buf, t, count, level)
            span = pl.ds(t, count)
            out[span] = (1.0 - DAMPING) * mid + first[span] + weight[span] * total

        if high - low == count:
            body(0)
        else:
            loop(0, (high - low) // count, body)

    def coarsen_ring(first, second):
        a = (first + second).reshape(4, 2, 8, 128)
        a = a[:, 0] + a[:, 1]
        a += partner(a, 1, 1)
        return (a + partner(a, 4, 2)) * (1.0 / 16.0)

    def pack3(x):
        row, lane = rows(x[0]), lanes(x[0])
        return jnp.where(
            even(row, 1), jnp.where(even(lane, 1), x[0], x[2]), jnp.where(even(lane, 1), x[1], x[3])
        )

    def unpack3(x):
        first, second = spread(x, 1, 0)
        a, c = spread(first, 1, 1)
        b, d = spread(second, 1, 1)
        return jnp.stack([a, b, c, d])

    load_m.wait()
    load_s.wait()

    def first0(t):
        w = DAMPING / (8.0 + m0[t])
        w0[t] = w
        v0[0][t + 1, z_all, y_all, :] = w * s0[t]

    loop(0, 8, first0)
    pl.semaphore_wait(barrier, len(faces))
    halos = swap0(0, 0)

    own1 = pl.ds(3, 4)
    m1[...] = coarsen(m0[...], 1)
    w1[own1, own1, 0:8, :] = 0.5 * DAMPING / (4.0 + m1[...])
    m2_own[...] = coarsen(m1[...], 2)
    pack2(1, m2_own[...])
    for slot in (0, 1, 3, 4):
        clear0(slot)
    sweep0(0, 1)

    halos.arrived()
    fix0(1, 0)
    halos = swap0(1, 1)
    weights1_in = swap1(w1, w1, (1, 0, 0))

    def rest0(i):
        r0[pl.ds(i * GROUP, GROUP)] = residual0(1, i * GROUP)

    loop(0, 8 // GROUP, rest0)
    halos.arrived()
    add_halos(r0, 1)

    s1[...] = coarsen(r0[...], 1)
    v1[0][own1, own1, 0:8, :] = 2.0 * w1[own1, own1, 0:8, :] * s1[...]
    first1_in = swap1(v1[0], v1[0], (2, 1, 0))
    sweep0(1, 3)
    fix0(3, 1)
    halos = swap0(3, 2, 2)
    weights1_in.arrived()
    first1_in.arrived()
    sweep1(0, 1, 1, v1[0], w1)

    mid, total = around1(1, 3, 4, 0)
    mid1, total1 = mid, total = mid[:, :, 0:8], total[:, :, 0:8]
    d = 4.0 + m1[...]
    source2 = coarsen(s1[...] - (d * mid - 0.5 * total), 2)
    pack2(0, DAMPING * source2 / (2.0 + m2_own[...]))
    source2_in = gather2()
    v1[3][own1, own1, 0:8, :] = (
        (1.0 - DAMPING) * mid1 + v1[0][own1, own1, 0:8, :] + w1[own1, own1, 0:8, :] * total1
    )
    halo1_in = swap1(v1[3], v1[3], (2, 2, 1), 1)
    weight_1[own1, own1, 0:8, :] = w1[own1, own1, 0:8, :]
    weights_in = swap1(w1, weight_1, (2, 2, 1))
    source2_in.arrived()

    def first2(t):
        unpack2(p2[t, :, 0], (u2, 2 + 2 * t), (u2, 3 + 2 * t))
        unpack2(p2[t, :, 1], (m2, 2 + 2 * t), (m2, 3 + 2 * t))
        span = pl.ds(2 + 2 * t, 2)
        w2[span] = 0.25 * DAMPING / (2.0 + m2[span])

    for t in range(3):
        first2(t)
    sweep_ring(u2, v2, u2, w2, 3, 7, 2, 4)
    mid, total = image(v2, 4, 2, 2)
    remainder = (2.0 + m2[4:6]) * (u2[4:6] * (1.0 / DAMPING) - mid) + 0.25 * total
    weight3 = DAMPING / (1.0 + coarsen_ring(m2[4], m2[5]))
    d3[5, 0] = pack3(weight3 * coarsen_ring(remainder[0], remainder[1]))
    d3[5, 1] = pack3(0.125 * weight3)
    planes_in = Group()
    for k in range(5, 0, -1):
        for a in (k, -k):
            planes_in.send(d3.at[5], d3.at[5 - a], (a, 0, 0))
    d2_own[0] = pack_planes(u2[5], w2[5])
    d2_own[1] = pack_planes(v2[4], v2[5])
    d2_own[2] = pack_planes(u2[4], w2[4])
    halo2_in = Group()
    for a, kind, count in ((2, 0, 2), (-2, 1, 2), (1, 1, 1), (-1, 1, 1)):
        halo2_in.send(d2_own.at[pl.ds(kind, count)], d2_in.at[2 - a, pl.ds(0, count)], (a, 0, 0))
    weights0_in = swap_weights()
    planes_in.arrived()

    for t in range(11):
        v3[0][t] = unpack3(d3[t, 0])
        w3[t] = unpack3(d3[t, 1])
    for step in range(3):
        sweep_ring(v3[step], v3[step + 1], v3[0], w3, 1 + step, 10 - step, 3, 9 - 2 * step)

    halo2_in.arrived()
    unpack2(d2_in[0, 0], (u2, 1), (w2, 1))
    unpack2(d2_in[4, 1], (u2, 8), (w2, 8))
    for k, kind, at in ((0, 1, 0), (1, 0, 2), (3, 0, 6), (4, 0, 8)):
        unpack2(d2_in[k, kind], (v2, at), (v2, at + 1))

    def correct2(t):
        e = v3[3][3 + t]
        e = jnp.broadcast_to(e[:, None], (4, 2, 8, 128)).reshape(8, 8, 128)
        for k in range(2):
            v2[2 * t + k] = v2[2 * t + k] + e

    loop(0, 5, correct2)
    sweep_ring(v2, s2, u2, w2, 1, 9, 2, 4)
    sweep_ring(s2, v2, u2, w2, 2, 8, 2, 3)

    halo1_in.arrived()
    all_sent(1)

    def expand1(tc):
        for z in range(6):
            e = v2[2 + tc, (z - 2) % 8]
            tmp[z, pl.ds(0, 8, stride=2), :] = e
            tmp[z, pl.ds(1, 8, stride=2), :] = e
        e = tmp[0:6, 0:16, :]
        return jnp.broadcast_to(e[:, None], (6, 2, 16, 128)).reshape(12, 16, 128)[1:11]

    e = expand1(0)
    v1[2][0] = e

    def correct1(tc):
        e = expand1(tc)
        for k in range(2):
            v1[2][2 * tc + k - 1] = e

    loop(1, 5, correct1)
    e = expand1(5)
    v1[2][9] = e
    weights_in.arrived()
    sweep1(2, 3, 2, v1[3], weight_1)
    sweep1(3, 4, 1, v1[0], weight_1)

    def expand0(tc):
        e = v1[4][2 + tc, pl.ds(2, 6)]
        tmp[0:6, pl.ds(OFF, 8, stride=2), :] = e[:, 0:8]
        tmp[0:6, pl.ds(OFF + 1, 8, stride=2), :] = e[:, 0:8]
        tmp[0:6, OFF - 1 : OFF, :] = e[:, 15:16]
        tmp[0:6, OFF + 16 : OFF + 17, :] = e[:, 8:9]
        e = tmp[...]
        return jnp.broadcast_to(e[:, None], (6, 2, 32, 128)).reshape(12, 32, 128)[1:11]

    v0[2][0] = expand0(0)

    def correct0(tc):
        e = expand0(tc)
        for k in range(2):
            v0[2][2 * tc + k - 1] = e

    loop(1, 5, correct0)
    v0[2][9] = expand0(5)
    halos.arrived()
    weights0_in.arrived()
    all_sent(2)
    keep = 1.0 - DAMPING

    def add0(i):
        t = i * GROUP
        mid, total = around0(2, t)
        here = pl.ds(t + 1, GROUP)
        v0[3][here, z_all, y_all, :] = v0[3][here, z_all, y_all, :] + keep * mid + w0[pl.ds(t, GROUP)] * total

    loop(0, 8 // GROUP, add0)
    buf = v0[2]
    for side, t, inner in ((0, 0, 1), (1, 9, 8)):
        mid = buf[t, z_all, y_all, :]
        total = roll(mid, 1, 2) + roll(mid, -1, 2) + mid + buf[inner, z_all, y_all, :]
        total += buf[t, pl.ds(0, 8), y_all, :] + buf[t, pl.ds(2, 8), y_all, :]
        total += buf[t, z_all, pl.ds(OFF - 1, 16), :] + buf[t, z_all, pl.ds(OFF + 1, 16), :]
        ht[2, side] = ht[2, side] + keep * mid + wt[side] * total
    for side, z, inner in ((0, 0, 1), (1, 9, 8)):
        mid = buf[t_all, z, y_all, :]
        total = roll(mid, 1, 2) + roll(mid, -1, 2) + mid + buf[t_all, inner, y_all, :]
        total += buf[pl.ds(0, 8), z, y_all, :] + buf[pl.ds(2, 8), z, y_all, :]
        total += buf[t_all, z, pl.ds(OFF - 1, 16), :] + buf[t_all, z, pl.ds(OFF + 1, 16), :]
        hz[2, side] = hz[2, side] + keep * mid + wz[side] * total
    own, other = pl.ds(0, 8), pl.ds(8, 8)
    mid = v1[4][own1, own1, other, :]
    inner = v1[4][own1, own1, own, :]
    common = roll(mid, 1, 3) + roll(mid, -1, 3) + 3.0 * mid
    common += jnp.where(rows(inner) == 0, roll(inner, 1, 2), roll(inner, -1, 2))
    for a in range(2):
        for b in range(2):
            total = common + v1[4][pl.ds(2 + 2 * a, 4), own1, other, :] + v1[4][own1, pl.ds(2 + 2 * b, 4), other, :]
            for t in range(4):
                for z in range(4):
                    at = (2 * t + a, 2 * z + b)
                    hy[(2,) + at] = hy[(2,) + at] + keep * mid[t, z] + wy[at] * total[t, z]
    sweep0(3, 4)
    fix0(4, 2)
    halos = swap0(4, 3)

    def finish(i):
        here = pl.ds(i * GROUP, GROUP)
        res_ref[here] = residual0(4, i * GROUP)
        sol_ref[here] = v0[4][pl.ds(i * GROUP + 1, GROUP), z_all, y_all, :]

    loop(0, 8 // GROUP, finish)
    halos.arrived()
    add_halos(res_ref, 3)
    all_sent(0)


def store(sol_ref, res_ref, sol_hbm, res_hbm, sem):
    copies = []
    for i, (src, dst) in enumerate(((sol_ref, sol_hbm), (res_ref, res_hbm))):
        for k in range(4):
            part = pl.ds(2 * k, 2)
            copies.append(pltpu.make_async_copy(src.at[part], dst.at[part], sem.at[4 * i + k]))
    for copy in copies:
        copy.start()
    for copy in copies:
        copy.wait()


def per_device(right_side, mass_field):
    f32 = jnp.float32
    block = jax.ShapeDtypeStruct(right_side.shape, f32)
    vmem = pl.BlockSpec(memory_space=pltpu.VMEM)
    hbm = pl.BlockSpec(memory_space=pltpu.HBM)
    own, ring2, ring3 = (8, 8, 16, 128), (10, 8, 8, 128), (11, 4, 8, 128)
    shapes = [
        own, own, own, own, *[(10, 10, 32, 128)] * 5,
        (4, 2, 8, 16, 128), (4, 2, 8, 16, 128), (4, 8, 8, 8, 128),
        (2, 8, 16, 128), (2, 8, 16, 128), (8, 8, 8, 128),
        *[(4, 4, 8, 128)] * 2, *[(10, 10, 16, 128)] * 2, (2, 2, 4, 128), *[(10, 10, 16, 128)] * 5,
        (3, 4, 2, 8, 128), ring2, ring2, ring2, ring2, ring2, (3, 4, 8, 128), (5, 2, 4, 8, 128),
        (11, 2, 8, 128), *[ring3] * 5,
        (6, 32, 128), (4, 4, 16, 128), (ROWS, 128),
    ]
    scratch = [pltpu.VMEM(shape, f32) for shape in shapes]
    scratch += [pltpu.SemaphoreType.DMA((count,)) for count in (2, 3, 13)]
    outs = pl.pallas_call(
        kernel,
        out_shape=(block, block),
        in_specs=[hbm, hbm],
        out_specs=(vmem, vmem),
        scratch_shapes=scratch,
        compiler_params=pltpu.CompilerParams(
            collective_id=0, has_side_effects=True, vmem_limit_bytes=56 * 1024 * 1024
        ),
    )(right_side, mass_field)
    return pl.pallas_call(
        store,
        out_shape=(block, block),
        in_specs=[vmem, vmem],
        out_specs=(hbm, hbm),
        scratch_shapes=[pltpu.SemaphoreType.DMA((8,))],
    )(*outs)


def solution(mesh):
    placed = (P("ta", "gz", "gy", None), P("ta", "gz", "gy", None))
    return jax.shard_map(
        per_device, mesh=mesh, in_specs=placed, out_specs=placed, check_vma=False
    )
```
